32 devices in a mesh: grp: 4 (over x, core), lat: 8 (over z, y).
Axes of the slice: x: 2, y: 2, z: 4, core: 2. Of those that a mesh axis runs over, the one named last changes fastest.
Arguments:
- grid_state: bfloat16 [16, 192, 384, 128], P('grp', 'lat'), may hold values from -6 to 6
- noise_field: bfloat16 [16, 192, 384, 128], P('grp', 'lat'), may hold values from -6 to 6
- legendre: bfloat16 [192, 128, 128], P('lat'), may hold values from -0.4375 to 0.4375
- diffusion: float32 [128], replicated, may hold values from 0.1 to 10
- input_weight: bfloat16 [128, 256], replicated, may hold values from -0.5 to 0.5
- noise_weight: bfloat16 [128, 256], replicated, may hold values from -0.5 to 0.5
- input_bias: float32 [256], replicated, may hold values from -4 to 4
- middle_weight: bfloat16 [256, 256], replicated, may hold values from -0.375 to 0.375
- output_weight: bfloat16 [256, 128], replicated, may hold values from -0.375 to 0.375
Outputs:
- new_state: bfloat16 [16, 192, 384, 128], P('grp', 'lat')
- ens_mean: float32 [192, 384, 128], P('lat')
- ens_var: float32 [192, 384, 128], P('lat')
The draws below stay inside these ranges and needn't reach their ends.
All inputs are finite; a program needn't handle non-finite values.
Results may differ from the reference program's by a relative error of at most 0.012.
Values may be sent and summed in bfloat16 or wider, within the bound.
A program may use at most 192 MiB of HBM per device.

```python
import math
import jax
import jax.numpy as jnp
from jax import lax

CHAN = 128
NLON = 384
NLAT = 192
WAVES = 128
NOISE = 128
HIDDEN_SIZE = 256
MEMBERS = 16


def levels(key, extent, shards, low, largest):
    loudness = 1.0
    for dim, blocks in shards:
        draws = jax.random.uniform(jax.random.fold_in(jax.random.fold_in(key, 6), dim), (blocks,), jnp.float32, low / len(shards), largest / len(shards))
        loudness = loudness * jnp.repeat(jnp.exp(draws), extent[dim] // blocks).reshape((-1,) + (1,) * (len(extent) - 1 - dim))
    return loudness


def gaussian(own_key, shape, deviation, most, pieces=(), held_as=jnp.bfloat16):
    result = jax.random.normal(own_key, shape, jnp.float32) * deviation
    if len(pieces) > 0:
        result = levels(own_key, shape, pieces, -0.22, 0.18) * result
    return jnp.clip(result, min=-most, max=most).astype(held_as)


def setup_inputs(seed: int = 0) -> dict:
    arg_keys = jax.random.split(jax.random.key(seed), 10)
    grid_state = gaussian(arg_keys[0], (MEMBERS, NLAT, NLON, CHAN), 1.0, 6.0, ((0, 4), (1, 8)))
    noise_field = gaussian(arg_keys[1], (MEMBERS, NLAT, NLON, NOISE), 1.0, 6.0, ((0, 4), (1, 8)))
    legendre = gaussian(arg_keys[2], (NLAT, WAVES, WAVES), NLAT ** -0.5, 0.4375, ((0, 8),))
    diffusion = jnp.clip(jnp.exp(jax.random.uniform(arg_keys[3], (CHAN,), jnp.float32, math.log(0.1), math.log(10.0))), 0.1, 10.0)
    input_weight = gaussian(arg_keys[4], (CHAN, HIDDEN_SIZE), CHAN ** -0.5, 0.5)
    noise_weight = gaussian(arg_keys[5], (NOISE, HIDDEN_SIZE), NOISE ** -0.5, 0.5)
    input_bias = gaussian(arg_keys[6], (HIDDEN_SIZE,), 1.0, 4.0, (), jnp.float32)
    middle_weight = gaussian(arg_keys[7], (HIDDEN_SIZE, HIDDEN_SIZE), HIDDEN_SIZE ** -0.5, 0.375)
    output_weight = gaussian(arg_keys[8], (HIDDEN_SIZE, CHAN), HIDDEN_SIZE ** -0.5, 0.375)
    return {"grid_state": grid_state, "noise_field": noise_field, "legendre": legendre, "diffusion": diffusion, "input_weight": input_weight, "noise_weight": noise_weight, "input_bias": input_bias, "middle_weight": middle_weight, "output_weight": output_weight}


def wave_table(lon_count, wave_count):
    lon_ids = jnp.arange(lon_count, dtype=jnp.int32)[:, None]
    wave_ids = jnp.arange(wave_count, dtype=jnp.int32)[None, :]
    phase = (lon_ids * wave_ids % lon_count).astype(jnp.float32) * (2.0 * math.pi / lon_count)
    factor = math.sqrt(2.0 / lon_count)
    joined = jnp.concatenate([jnp.cos(phase), -jnp.sin(phase)], axis=1) * factor
    return joined.astype(jnp.bfloat16)

def damping_filter(diffusion, wave_count):
    degree = jnp.arange(wave_count, dtype=jnp.int32).astype(jnp.float32)
    ratio = degree * (degree + 1.0) / float((wave_count - 1) * wave_count)
    return 1.0 / (1.0 + diffusion[None, :] * (ratio * ratio)[:, None])

def reference(grid_state, noise_field, legendre, diffusion, input_weight, noise_weight, input_bias, middle_weight, output_weight):
    transform = wave_table(NLON, WAVES).astype(jnp.float32)
    legendre_values = legendre.astype(jnp.float32)
    wave_ids = jnp.arange(WAVES, dtype=jnp.int32)
    triangle = (wave_ids[None, :] >= wave_ids[:, None]).astype(jnp.float32)
    damping = damping_filter(diffusion, WAVES)

    def advance(pair):
        member_state, member_noise = pair
        fourier = jnp.einsum('lxc,xk->lkc', member_state.astype(jnp.float32), transform).astype(jnp.bfloat16)
        fourier = fourier.reshape(NLAT, 2, WAVES, CHAN).astype(jnp.float32)
        spectrum = jnp.einsum('lmn,lrmc->rmnc', legendre_values, fourier) * triangle[None, :, :, None]
        filtered = (spectrum * damping[None, None, :, :]).astype(jnp.bfloat16)
        grid_fourier = jnp.einsum('lmn,rmnc->lrmc', legendre_values, filtered.astype(jnp.float32)).astype(jnp.bfloat16)
        grid_fourier = grid_fourier.reshape(NLAT, 2 * WAVES, CHAN).astype(jnp.float32)
        smoothed = jnp.einsum('lkc,xk->lxc', grid_fourier, transform)
        flat_fields = smoothed.reshape(-1, CHAN)
        smoothed_in = flat_fields.astype(jnp.bfloat16)
        pre_act = jnp.dot(smoothed_in, input_weight, preferred_element_type=jnp.float32)
        pre_act = pre_act + jnp.dot(member_noise.reshape(-1, NOISE), noise_weight, preferred_element_type=jnp.float32)
        hidden_one = jax.nn.silu(pre_act + input_bias).astype(jnp.bfloat16)
        hidden_two = jax.nn.silu(jnp.dot(hidden_one, middle_weight, preferred_element_type=jnp.float32)).astype(jnp.bfloat16)
        tendency = jnp.dot(hidden_two, output_weight, preferred_element_type=jnp.float32)
        return (flat_fields + tendency).astype(jnp.bfloat16).reshape(NLAT, NLON, CHAN)
    new_state = lax.map(advance, (grid_state, noise_field))
    member_values = new_state.astype(jnp.float32)
    ens_mean = lax.optimization_barrier(jnp.mean(member_values, axis=0))
    ens_var = lax.optimization_barrier(jnp.sum(jnp.square(member_values - ens_mean), axis=0)) / (MEMBERS - 1)
    return (new_state, ens_mean, ens_var)
```

```python
import functools
import math

import jax
import jax.numpy as jnp
from jax import lax
from jax.experimental import pallas as pl
from jax.experimental.pallas import tpu as pltpu
from jax.sharding import PartitionSpec as P

BF16 = jnp.bfloat16
F32 = jnp.float32


def wave_table(lon_count, wave_count):
    lon_ids = jnp.arange(lon_count, dtype=jnp.int32)[:, None]
    wave_ids = jnp.arange(wave_count, dtype=jnp.int32)[None, :]
    phase = (lon_ids * wave_ids % lon_count).astype(jnp.float32) * (2.0 * math.pi / lon_count)
    factor = math.sqrt(2.0 / lon_count)
    joined = jnp.concatenate([jnp.cos(phase), -jnp.sin(phase)], axis=1) * factor
    return joined.astype(jnp.bfloat16)


def damping_filter(diffusion, wave_count):
    degree = jnp.arange(wave_count, dtype=jnp.int32).astype(jnp.float32)
    ratio = degree * (degree + 1.0) / float((wave_count - 1) * wave_count)
    return 1.0 / (1.0 + diffusion[None, :] * (ratio * ratio)[:, None])


def analysis_body(table_ref, grid_ref, out_ref):
    bands, _, rows, width, channels = out_ref.shape
    for row in range(0, rows, 2):
        pair = jnp.concatenate([grid_ref[0, row], grid_ref[0, row + 1]], axis=1)
        waves = jnp.dot(table_ref[...], pair, preferred_element_type=F32).astype(BF16)
        for k in range(2):
            out_ref[:, 0, row + k] = waves[:, k * channels:(k + 1) * channels].reshape(
                bands, width, channels
            )


def analyse(grid_state, table, first, count, bands):
    _, lat_rows, lon_count, channels = grid_state.shape
    width = table.shape[0] // bands
    rows = 6
    return pl.pallas_call(
        analysis_body,
        grid=(count, lat_rows // rows),
        in_specs=[
            pl.BlockSpec(table.shape, lambda b, i: (0, 0)),
            pl.BlockSpec((1, rows, lon_count, channels), lambda b, i: (b + first, i, 0, 0)),
        ],
        out_specs=pl.BlockSpec((bands, 1, rows, width, channels), lambda b, i: (0, b, i, 0, 0)),
        out_shape=jax.ShapeDtypeStruct((bands, count, lat_rows, width, channels), BF16),
        cost_estimate=pl.CostEstimate(
            flops=2 * count * lat_rows * lon_count * channels * table.shape[0],
            bytes_accessed=4 * count * lat_rows * lon_count * channels,
            transcendentals=0,
        ),
    )(table, grid_state)


def spectral_body(parts, in_ref, basis_ref, flipped_ref, damping_ref, *rest):
    outs, (fin, fout) = rest[:parts], rest[parts:]
    bands, _, lat_rows, width, channels = in_ref.shape
    waves = basis_ref.shape[0]
    lats = bands * lat_rows
    span = lat_rows * width
    for s in range(bands):
        fin[pl.ds(s * span, span), :] = in_ref[s, 0].astype(F32).reshape(span, channels)
    damping = jnp.concatenate([damping_ref[...]] * 2, axis=1)
    for m in range(waves):
        values = jnp.concatenate(
            [fin[pl.ds(r * waves + m, lats, stride=width), :] for r in range(2)], axis=1
        ).astype(BF16)
        spectrum = jnp.dot(flipped_ref[m], values, preferred_element_type=F32)
        filtered = (spectrum * damping).astype(BF16)
        grid = jnp.dot(basis_ref[m], filtered, preferred_element_type=F32)
        for r in range(2):
            fout[pl.ds(r * waves + m, lats, stride=width), :] = grid[
                :, r * channels:(r + 1) * channels
            ]
    part_rows = lat_rows // parts
    for q in range(parts):
        for s in range(bands):
            start = (s * lat_rows + q * part_rows) * width
            outs[q][s, 0] = (
                fout[pl.ds(start, part_rows * width), :]
                .reshape(part_rows, width, channels)
                .astype(BF16)
            )


def spectral(received, basis, flipped, damping, parts):
    bands, count, lat_rows, width, channels = received.shape
    part_rows = lat_rows // parts
    whole = lambda a: pl.BlockSpec(a.shape, lambda b: (0,) * a.ndim)
    return pl.pallas_call(
        functools.partial(spectral_body, parts),
        grid=(count,),
        in_specs=[
            pl.BlockSpec((bands, 1, lat_rows, width, channels), lambda b: (0, b, 0, 0, 0)),
            whole(basis),
            whole(flipped),
            whole(damping),
        ],
        out_specs=[
            pl.BlockSpec((bands, 1, part_rows, width, channels), lambda b: (0, b, 0, 0, 0))
        ] * parts,
        out_shape=[
            jax.ShapeDtypeStruct((bands, count, part_rows, width, channels), BF16)
        ] * parts,
        scratch_shapes=[pltpu.VMEM((bands * lat_rows * width, channels), F32)] * 2,
        cost_estimate=pl.CostEstimate(
            flops=8 * count * basis.size * channels,
            bytes_accessed=4 * received.size,
            transcendentals=0,
        ),
    )(received, basis, flipped, damping)


def silu(value):
    half = 0.5 * value
    return half + half * jnp.tanh(half)


def physics_body(groups, *refs):
    fields = refs[:groups]
    noise_ref, table_ref, first_ref, bias_ref, middle_ref, last_ref = refs[groups:groups + 6]
    state_ref, stats_ref = refs[-2:]
    members, _, lon_count, channels = noise_ref.shape
    states = []
    for ref in fields:
        count = ref.shape[1]
        waves = jnp.concatenate(
            [ref[:, k, 0].reshape(-1, channels) for k in range(count)], axis=1
        )
        smoothed = jnp.dot(table_ref[...], waves, preferred_element_type=F32)
        for k in range(count):
            flat = smoothed[:, k * channels:(k + 1) * channels]
            b = len(states)
            joined = jnp.concatenate([flat.astype(BF16), noise_ref[b, 0]], axis=1)
            pre = jnp.dot(joined, first_ref[...], preferred_element_type=F32)
            one = silu(pre + bias_ref[...]).astype(BF16)
            two = silu(jnp.dot(one, middle_ref[...], preferred_element_type=F32)).astype(BF16)
            tendency = jnp.dot(two, last_ref[...], preferred_element_type=F32)
            state = (flat + tendency).astype(BF16)
            state_ref[b, 0] = state
            states.append(state)
    values = [s.astype(F32) for s in states]
    total = functools.reduce(jnp.add, values)
    mean = total * (1.0 / members)
    spread = functools.reduce(jnp.add, [jnp.square(v - mean) for v in values])
    half = lon_count // 2
    for h in range(2):
        stats_ref[h, 0, 0] = total[h * half:(h + 1) * half].astype(BF16)
        stats_ref[h, 1, 0] = spread[h * half:(h + 1) * half].astype(BF16)


def physics(fields, noise, table, first, bias, middle, last, part, previous):
    bands, _, part_rows, width, channels = fields[0].shape
    members, lat_rows, lon_count, noise_channels = noise.shape
    whole = lambda a: pl.BlockSpec(a.shape, lambda i: (0,) * a.ndim)
    at = part * part_rows
    specs = [
        pl.BlockSpec((bands, f.shape[1], 1, width, channels), lambda i: (0, 0, i, 0, 0))
        for f in fields
    ]
    specs.append(
        pl.BlockSpec((members, 1, lon_count, noise_channels), lambda i: (0, i + at, 0, 0))
    )
    params = [table, first, bias, middle, last]
    specs += [whole(a) for a in params]
    operands = [*fields, noise, *params]
    aliases = {}
    if previous is not None:
        aliases = {len(operands): 0}
        operands.append(previous)
        specs.append(pl.BlockSpec(memory_space=pl.ANY))
    columns = members * part_rows * lon_count
    hidden = middle.shape[0]
    return pl.pallas_call(
        functools.partial(physics_body, len(fields)),
        grid=(part_rows,),
        in_specs=specs,
        out_specs=[
            pl.BlockSpec((members, 1, lon_count, channels), lambda i: (0, i + at, 0, 0)),
            pl.BlockSpec((2, 2, 1, lon_count // 2, channels), lambda i: (0, 0, i, 0, 0)),
        ],
        out_shape=[
            jax.ShapeDtypeStruct((members, lat_rows, lon_count, channels), BF16),
            jax.ShapeDtypeStruct((2, 2, part_rows, lon_count // 2, channels), BF16),
        ],
        input_output_aliases=aliases,
        cost_estimate=pl.CostEstimate(
            flops=2 * columns * (first.size + middle.size + last.size + 256 * channels),
            bytes_accessed=8 * columns * channels,
            transcendentals=2 * columns * hidden,
        ),
    )(*operands)


def swap(value, bit):
    groups = lax.axis_size("grp")
    return lax.ppermute(value, "grp", [(g, g ^ bit) for g in range(groups)])


def join(a, b, count):
    a, b = a.astype(F32), b.astype(F32)
    total = a[0] + b[0]
    spread = (a[1] + b[1]) + jnp.square(a[0] - b[0]) * (0.5 / count)
    return jnp.stack([total, spread])


def pair_moments(stats, members):
    core = lax.axis_index("grp") % 2
    own = lax.dynamic_index_in_dim(stats, core, 0, keepdims=False)
    other = lax.dynamic_index_in_dim(stats, 1 - core, 0, keepdims=False)
    return join(own, swap(other, 1), members).astype(BF16)


def ensemble_moments(held, members):
    groups = lax.axis_size("grp")
    core = lax.axis_index("grp") % 2
    bit, count = 2, 2 * members
    while bit < groups:
        held = join(held.astype(BF16), swap(held.astype(BF16), bit), count)
        bit, count = 2 * bit, 2 * count
    scale = jnp.array([1.0 / count, 1.0 / (count - 1)], F32)
    held = (held * scale[:, None, None, None]).astype(BF16)
    partner = swap(held, 1)
    low = jnp.where(core == 0, held, partner)
    high = jnp.where(core == 0, partner, held)
    return low, high


def direct_plan(
    grid_state,
    noise_field,
    legendre,
    diffusion,
    input_weight,
    noise_weight,
    input_bias,
    middle_weight,
    output_weight,
):
    members, lat_rows, lon_count, channels = grid_state.shape
    wave_count = legendre.shape[1]
    bands = lax.axis_size("lat")
    local_waves = wave_count // bands
    chunk = 2
    parts = 2
    transform = wave_table(lon_count, wave_count)
    table = (
        transform.reshape(lon_count, 2, bands, local_waves)
        .transpose(0, 2, 1, 3)
        .reshape(lon_count, 2 * wave_count)
    )
    table_t = table.T
    exchange = lambda v: lax.all_to_all(v, "lat", split_axis=0, concat_axis=0, tiled=True)
    damping = damping_filter(diffusion, wave_count)

    sent = [
        analyse(grid_state, table_t, b, chunk, bands) for b in range(0, members, chunk)
    ]
    groups = lax.axis_size("grp")
    turned = legendre.transpose(1, 0, 2).reshape(bands, local_waves * lat_rows, wave_count)
    share = local_waves * lat_rows // groups
    own = lax.dynamic_slice_in_dim(turned, lax.axis_index("grp") * share, share, axis=1)
    basis = lax.all_gather(exchange(own), "grp", axis=1, tiled=True)
    basis = basis.reshape(bands, local_waves, lat_rows, wave_count).transpose(1, 0, 2, 3)
    basis = basis.reshape(local_waves, bands * lat_rows, wave_count)
    zonal_ids = lax.axis_index("lat") * local_waves + jnp.arange(local_waves, dtype=jnp.int32)
    total_ids = jnp.arange(wave_count, dtype=jnp.int32)
    triangle = total_ids[None, :] >= zonal_ids[:, None]
    basis = jnp.where(triangle[:, None], basis, jnp.zeros_like(basis))
    flipped = basis.transpose(0, 2, 1)
    received = [exchange(s) for s in sent]
    banded = [spectral(r, basis, flipped, damping, parts) for r in received]

    first = jnp.concatenate([input_weight, noise_weight], axis=0)
    new_state = None
    moments = []
    for q in range(parts):
        fields = [exchange(g[q]) for g in banded]
        if moments:
            fields, moments[-1] = lax.optimization_barrier((fields, moments[-1]))
        new_state, stats = physics(
            fields, noise_field, table, first, input_bias[None], middle_weight,
            output_weight, q, new_state,
        )
        moments.append(ensemble_moments(pair_moments(stats, members), members))
    joined = [jnp.concatenate([low, high], axis=2) for low, high in moments]
    ens_mean = jnp.concatenate([j[0] for j in joined], axis=0).astype(F32)
    ens_var = jnp.concatenate([j[1] for j in joined], axis=0).astype(F32)
    return (new_state, ens_mean, ens_var)


GROUP = 8


def slot_table(lon_count, wave_count, share, lane_y, lanes):
    offset = jnp.arange(lanes, dtype=jnp.int32)[:, None, None, None]
    p = jnp.arange(2, dtype=jnp.int32)[None, :, None, None]
    part = jnp.arange(2, dtype=jnp.int32)[None, None, :, None]
    unit = (lane_y - offset) % lanes * share + jnp.arange(share, dtype=jnp.int32)[None, None, None, :]
    wave = jnp.where(p == 0, unit, wave_count - unit)
    wave = jnp.where(unit == 0, jnp.where(part == 0, 0, wave_count // 2), wave)
    imaginary = jnp.where(unit == 0, p, part) == 1
    lon_ids = jnp.arange(lon_count, dtype=jnp.int32)
    turn = (wave.reshape(-1, 1) * lon_ids[None, :]) % lon_count
    phase = turn.astype(F32) * (2.0 * math.pi / lon_count)
    factor = math.sqrt(2.0 / lon_count)
    flag = jnp.broadcast_to(imaginary, wave.shape).reshape(-1, 1)
    return (jnp.where(flag, -jnp.sin(phase), jnp.cos(phase)) * factor).astype(BF16)


def forward_body(lanes, table_ref, grid_ref, *rest):
    outs, scratch = rest[:lanes], rest[lanes:]
    _, share, rows, _ = outs[0].shape
    _, group, _, channels = grid_ref.shape
    pitch = scratch[0].shape[0] // share
    for k in range(0, group, 2):
        pair = jnp.concatenate([grid_ref[0, k], grid_ref[0, k + 1]], axis=1)
        waves = jnp.dot(table_ref[...], pair, preferred_element_type=F32)
        at = 0
        for dy in range(lanes):
            for p in range(2):
                for part in range(2):
                    for t in range(2):
                        scratch[2 * dy + part][pl.ds(p * group + k + t, share, stride=pitch), :] = (
                            waves[at:at + share, t * channels:(t + 1) * channels]
                        )
                    at += share
    for dy in range(lanes):
        for i in range(share):
            both = [scratch[2 * dy + part][i * pitch:i * pitch + rows, :] for part in range(2)]
            outs[dy][0, i] = jnp.concatenate(both, axis=1).astype(BF16)


def forward(grid_state, table, first, count, lanes, share):
    _, lat_rows, lon_count, channels = grid_state.shape
    rows, pitch = 2 * GROUP, 3 * GROUP
    groups = lat_rows // GROUP
    return pl.pallas_call(
        functools.partial(forward_body, lanes),
        grid=(count, groups),
        in_specs=[
            pl.BlockSpec(table.shape, lambda b, g: (0, 0)),
            pl.BlockSpec((1, GROUP, lon_count, channels), lambda b, g: (b + first, g, 0, 0)),
        ],
        out_specs=[
            pl.BlockSpec((1, share, rows, 2 * channels), lambda b, g: (b, 0, g, 0))
        ] * lanes,
        out_shape=[
            jax.ShapeDtypeStruct((count, share, groups * rows, 2 * channels), BF16)
        ] * lanes,
        scratch_shapes=[pltpu.VMEM((share * pitch, channels), F32)] * (2 * lanes),
        cost_estimate=pl.CostEstimate(
            flops=2 * count * lat_rows * lon_count * channels * table.shape[0],
            bytes_accessed=4 * count * lat_rows * lon_count * channels,
            transcendentals=0,
        ),
    )(table, grid_state)


def basis_body(start_ref, waves_ref, out_ref):
    lanes, entries, rows, totals = out_ref.shape
    count, lat_rows, _ = waves_ref.shape
    groups = lat_rows // GROUP
    row = lax.broadcasted_iota(jnp.int32, (lat_rows, totals), 1)
    flip = lax.broadcasted_iota(jnp.int32, (totals, totals), 0)
    flip = flip + lax.broadcasted_iota(jnp.int32, (totals, totals), 1) == totals - 1
    flip = flip.astype(F32).astype(BF16)
    for dy in range(lanes):
        def step(i, carry):
            unit = start_ref[dy * entries + i]
            low = waves_ref[jnp.minimum(unit, count - 1)].astype(F32)
            high = jnp.dot(
                waves_ref[jnp.clip(count - unit, 0, count - 1)], flip, preferred_element_type=F32
            )
            low = jnp.where(row >= unit, low, 0.0).reshape(groups, 1, GROUP, totals)
            high = jnp.where(row < unit, high, 0.0).reshape(groups, 1, GROUP, totals)
            both = jnp.concatenate([low, high], axis=1).reshape(rows, totals)
            out_ref[dy, i] = both.astype(BF16)
            return carry
        lax.fori_loop(0, entries, step, 0)


def basis_blocks(units, turned):
    lanes, entries = units.shape
    count, lat_rows, totals = turned.shape
    whole = lambda a: pl.BlockSpec(a.shape, lambda: (0,) * a.ndim)
    shape = (lanes, entries, 2 * lat_rows, totals)
    return pl.pallas_call(
        basis_body,
        in_specs=[pl.BlockSpec(memory_space=pltpu.SMEM), whole(turned)],
        out_specs=pl.BlockSpec(shape, lambda: (0,) * 4),
        out_shape=jax.ShapeDtypeStruct(shape, BF16),
        cost_estimate=pl.CostEstimate(
            flops=2 * lanes * entries * lat_rows * totals * totals,
            bytes_accessed=4 * lanes * entries * lat_rows * totals,
            transcendentals=0,
        ),
    )(units.reshape(-1), turned)


def partial_body(blocks, extra_ref, flipped_ref, *rest):
    ins, out_ref = rest[:blocks], rest[blocks]
    channels = out_ref.shape[-1] // 2
    first = pl.program_id(1) == 0
    for j in range(out_ref.shape[1]):
        values = jnp.concatenate([ref[0, j] for ref in ins], axis=0)
        if j == 0:
            second = jnp.where(first, extra_ref[0], flipped_ref[0])
            sums = jnp.concatenate([
                jnp.dot(flipped_ref[0], values[:, :channels], preferred_element_type=F32),
                jnp.dot(second, values[:, channels:], preferred_element_type=F32),
            ], axis=1)
        else:
            sums = jnp.dot(flipped_ref[j], values, preferred_element_type=F32)
        out_ref[0, j] = sums.astype(BF16)


def partial_spectra(fields, flipped, steps):
    count, share, rows, width = fields[0].shape
    totals, depth = flipped.shape[1:]
    per = share // steps
    return pl.pallas_call(
        functools.partial(partial_body, len(fields)),
        grid=(count, steps),
        in_specs=[
            pl.BlockSpec((1, totals, depth), lambda b, s: (share, 0, 0)),
            pl.BlockSpec((per, totals, depth), lambda b, s: (s, 0, 0)),
        ] + [pl.BlockSpec((1, per, rows, width), lambda b, s: (b, s, 0, 0))] * len(fields),
        out_specs=pl.BlockSpec((1, per, totals, width), lambda b, s: (b, s, 0, 0)),
        out_shape=jax.ShapeDtypeStruct((count, share, totals, width), BF16),
        cost_estimate=pl.CostEstimate(
            flops=2 * count * share * totals * depth * width,
            bytes_accessed=2 * count * share * (totals + depth) * width,
            transcendentals=0,
        ),
    )(flipped, flipped, *fields)


def synthesis_body(blocks, parts, half_wave, start_ref, damping_ref, mirrored_ref, extra_ref, basis_ref,
                   own_ref, other_ref, *outs):
    per, totals, width = own_ref.shape[1:]
    channels = width // 2
    step = pl.program_id(1)
    row = lax.broadcasted_iota(jnp.int32, (totals, channels), 0)
    rows = basis_ref.shape[1] // blocks // parts
    for j in range(per):
        total = own_ref[0, j].astype(F32) + other_ref[0, j].astype(F32)
        unit = start_ref[0] + step * per + j
        marks = [unit, jnp.where(unit == 0, half_wave, unit)]
        damping = jnp.concatenate(
            [jnp.where(row < u, mirrored_ref[...], damping_ref[...]) for u in marks], axis=1
        )
        filtered = (total * damping).astype(BF16)
        if j == 0:
            second = jnp.where(step == 0, extra_ref[0], basis_ref[0])
            grid = jnp.concatenate([
                jnp.dot(basis_ref[0], filtered[:, :channels], preferred_element_type=F32),
                jnp.dot(second, filtered[:, channels:], preferred_element_type=F32),
            ], axis=1).astype(BF16)
        else:
            grid = jnp.dot(basis_ref[j], filtered, preferred_element_type=F32).astype(BF16)
        for k in range(blocks * parts):
            outs[k][0, j] = grid[k * rows:(k + 1) * rows]


def synthesis(own, other, basis, damping, start, blocks, parts, steps):
    count, share, totals, width = own.shape
    depth = basis.shape[1]
    rows = depth // blocks // parts
    per = share // steps
    whole = lambda a: pl.BlockSpec(a.shape, lambda b, s: (0,) * a.ndim)
    block = pl.BlockSpec((1, per, totals, width), lambda b, s: (b, s, 0, 0))
    outs = pl.pallas_call(
        functools.partial(synthesis_body, blocks, parts, totals // 2),
        grid=(count, steps),
        in_specs=[
            pl.BlockSpec(memory_space=pltpu.SMEM),
            whole(damping),
            whole(damping),
            pl.BlockSpec((1, depth, totals), lambda b, s: (share, 0, 0)),
            pl.BlockSpec((per, depth, totals), lambda b, s: (s, 0, 0)),
            block,
            block,
        ],
        out_specs=[pl.BlockSpec((1, per, rows, width), lambda b, s: (b, s, 0, 0))] * (blocks * parts),
        out_shape=[jax.ShapeDtypeStruct((count, share, rows, width), BF16)] * (blocks * parts),
        cost_estimate=pl.CostEstimate(
            flops=2 * count * share * totals * depth * width,
            bytes_accessed=2 * count * share * (2 * totals + depth) * width,
            transcendentals=0,
        ),
    )(start, damping, damping[::-1], basis, basis, own, other)
    return [outs[k * parts:(k + 1) * parts] for k in range(blocks)]


def column_body(lanes, far, last, *refs):
    dist_ref, fields = refs[0], refs[1:1 + lanes * far]
    noise_ref, table_ref, first_ref, bias_ref, middle_ref, last_ref = refs[1 + lanes * far:7 + lanes * far]
    scratch = refs[-2 * lanes:]
    outs = refs[-2 * lanes - (2 if last else 1):-2 * lanes]
    state_ref = outs[0]
    _, lats, lon_count, channels = noise_ref.shape
    _, share, rows, _ = fields[0].shape
    group = rows // 2
    pitch = scratch[0].shape[0] // share
    inner = pl.program_id(1)

    @pl.when(inner == 0)
    def _():
        for dy in range(lanes):
            for i in range(share):
                value = fields[dy * far][0, i]
                for d in range(1, far):
                    value = jnp.where(dist_ref[0] == d, fields[dy * far + d][0, i], value)
                value = value.astype(F32)
                for part in range(2):
                    scratch[2 * dy + part][i * pitch:i * pitch + rows, :] = (
                        value[:, part * channels:(part + 1) * channels]
                    )

    waves = []
    for k in range(lats):
        at = inner * lats + k
        waves.append(jnp.concatenate([
            scratch[2 * dy + part][pl.ds(p * group + at, share, stride=pitch), :]
            for dy in range(lanes) for p in range(2) for part in range(2)
        ], axis=0).astype(BF16))
    smoothed = jnp.dot(table_ref[...], jnp.concatenate(waves, axis=1), preferred_element_type=F32)
    for k in range(lats):
        flat = smoothed[:, k * channels:(k + 1) * channels]
        joined = jnp.concatenate([flat.astype(BF16), noise_ref[0, k]], axis=1)
        pre = jnp.dot(joined, first_ref[...], preferred_element_type=F32)
        one = silu(pre + bias_ref[...]).astype(BF16)
        two = silu(jnp.dot(one, middle_ref[...], preferred_element_type=F32)).astype(BF16)
        tendency = jnp.dot(two, last_ref[...], preferred_element_type=F32)
        state = (flat + tendency).astype(BF16)
        state_ref[0, k] = state
        if last:
            held_ref, stats_ref = refs[7 + lanes * far], outs[1]
            members = held_ref.shape[0] + 1
            values = [held_ref[b, k].astype(F32) for b in range(members - 1)] + [state.astype(F32)]
            total = functools.reduce(jnp.add, values)
            mean = total * (1.0 / members)
            spread = functools.reduce(jnp.add, [jnp.square(v - mean) for v in values])
            half = lon_count // 2
            for h in range(2):
                stats_ref[h, 0, k] = total[h * half:(h + 1) * half].astype(BF16)
                stats_ref[h, 1, k] = spread[h * half:(h + 1) * half].astype(BF16)


def columns(fields, dist, noise, table, first, bias, middle, output, member, part, previous):
    lanes, far = len(fields), len(fields[0])
    members, lat_rows, lon_count, channels = noise.shape
    _, share, depth, width = fields[0][0].shape
    rows = 2 * GROUP
    groups = depth // rows
    lats = 2
    inner = GROUP // lats
    at = 0 if part is None else part
    last = part is not None
    whole = lambda a: pl.BlockSpec(a.shape, lambda g, i: (0,) * a.ndim)
    params = [table, first, bias, middle, output]
    operands = [dist, *[f for each in fields for f in each], noise, *params]
    row_block = lambda g, i: (member, (g + at) * inner + i, 0, 0)
    specs = [pl.BlockSpec(memory_space=pltpu.SMEM)]
    specs += [pl.BlockSpec((1, share, rows, width), lambda g, i: (0, 0, g, 0))] * (lanes * far)
    specs.append(pl.BlockSpec((1, lats, lon_count, channels), row_block))
    specs += [whole(a) for a in params]
    aliases = {}
    if previous is not None:
        aliases = {len(operands): 0}
        operands.append(previous)
        if last:
            specs.append(pl.BlockSpec(
                (members - 1, lats, lon_count, channels), lambda g, i: (0, (g + at) * inner + i, 0, 0)
            ))
        else:
            specs.append(pl.BlockSpec(memory_space=pl.ANY))
    out_specs = [pl.BlockSpec((1, lats, lon_count, channels), row_block)]
    out_shape = [jax.ShapeDtypeStruct(noise.shape, BF16)]
    if last:
        half = lon_count // 2
        out_specs.append(
            pl.BlockSpec((2, 2, lats, half, channels), lambda g, i: (0, 0, g * inner + i, 0, 0))
        )
        out_shape.append(jax.ShapeDtypeStruct((2, 2, groups * GROUP, half, channels), BF16))
    points = groups * GROUP * lon_count
    hidden = middle.shape[0]
    return pl.pallas_call(
        functools.partial(column_body, lanes, far, last),
        grid=(groups, inner),
        in_specs=specs,
        out_specs=out_specs,
        out_shape=out_shape,
        input_output_aliases=aliases,
        scratch_shapes=[pltpu.VMEM((share * 3 * GROUP, channels), F32)] * (2 * lanes),
        cost_estimate=pl.CostEstimate(
            flops=2 * points * (first.size + middle.size + output.size + 256 * channels),
            bytes_accessed=8 * points * channels,
            transcendentals=2 * points * hidden,
        ),
    )(*operands)


def hub_plan(
    lanes,
    grid_state,
    noise_field,
    legendre,
    diffusion,
    input_weight,
    noise_weight,
    input_bias,
    middle_weight,
    output_weight,
):
    members, lat_rows, lon_count, channels = grid_state.shape
    wave_count = legendre.shape[1]
    places = lax.axis_size("lat") // lanes
    far = places // 2
    share = wave_count // 2 // lanes
    parts = lat_rows // GROUP
    steps = 4
    index = lax.axis_index("lat")
    place, lane = index // lanes, index % lanes
    dist = jnp.where(place < far, far - 1 - place, place - far)[None].astype(jnp.int32)
    hubs = (far - 1, far)
    routes = {}
    for d in range(far):
        for dy in range(lanes):
            ends = [((hubs[0] - d) * lanes, hubs[0] * lanes), ((hubs[1] + d) * lanes, hubs[1] * lanes)]
            routes[d, dy] = [(s + v, t + (v - dy) % lanes) for s, t in ends for v in range(lanes)]
    across = [(hubs[s] * lanes + v, hubs[1 - s] * lanes + v) for s in range(2) for v in range(lanes)]
    order = [(d, dy) for d in range(far) for dy in range(lanes)]

    def gather(values):
        return [
            values[dy] if (d, dy) == (0, 0) else lax.ppermute(values[dy], "lat", routes[d, dy])
            for d, dy in order
        ]

    def scatter(values):
        back = {}
        for (d, dy), value in zip(order, values):
            pairs = [(t, s) for s, t in routes[d, dy]]
            back[d, dy] = value if (d, dy) == (0, 0) else lax.ppermute(value, "lat", pairs)
        return [[back[d, dy] for d in range(far)] for dy in range(lanes)]

    table_t = slot_table(lon_count, wave_count, share, lane, lanes)
    table = table_t.T
    damping = damping_filter(diffusion, wave_count)
    fields = [forward(grid_state, table_t, b, 1, lanes, share) for b in range(members)]

    core = lax.axis_index("grp") % 2
    entries = share + 4
    local = jnp.arange(entries, dtype=jnp.int32)[None, :]
    owner = (lane - jnp.arange(lanes, dtype=jnp.int32)[:, None]) % lanes * share
    extra = jnp.where(owner == 0, wave_count // 2, owner)
    units = jnp.where(local < share, owner + local, extra)
    units = lax.dynamic_slice_in_dim(units, core * (entries // 2), entries // 2, axis=1)
    blocks = basis_blocks(units, legendre.transpose(1, 0, 2))
    basis = jnp.concatenate(gather([blocks[dy] for dy in range(lanes)]), axis=1)
    partner = swap(basis, 1)
    basis = jnp.concatenate(
        [jnp.where(core == 0, basis, partner), jnp.where(core == 0, partner, basis)], axis=0
    )
    flipped = basis.transpose(0, 2, 1)
    start = (lane * share)[None].astype(jnp.int32)

    first = jnp.concatenate([input_weight, noise_weight], axis=0)
    common = (noise_field, table, first, input_bias[None], middle_weight, output_weight)
    new_state = None
    moments = []
    for b in range(members):
        own = partial_spectra(gather(fields[b]), flipped, steps)
        other = lax.ppermute(own, "lat", across)
        last = b == members - 1
        grids = synthesis(own, other, basis, damping, start, len(order), parts if last else 1, steps)
        if not last:
            found = scatter([g[0] for g in grids])
            (new_state,) = columns(found, dist, *common, b, None, new_state)
            continue
        for q in range(parts):
            found = scatter([g[q] for g in grids])
            new_state, stats = columns(found, dist, *common, b, q, new_state)
            moments.append(ensemble_moments(pair_moments(stats, members), members))
    joined = [jnp.concatenate([low, high], axis=2) for low, high in moments]
    ens_mean = jnp.concatenate([j[0] for j in joined], axis=0).astype(F32)
    ens_var = jnp.concatenate([j[1] for j in joined], axis=0).astype(F32)
    return (new_state, ens_mean, ens_var)


def lane_count(mesh):
    line = [getattr(d, "coords", None) for d in mesh.devices.reshape(-1, mesh.shape["lat"])[0]]
    if len(line) < 2 or line[0] is None:
        return 2
    axis = [a != b for a, b in zip(line[0], line[1])].index(True)
    return len({c[axis] for c in line})


def per_device(lanes, *args):
    grid_state, legendre = args[0], args[2]
    members, lat_rows = grid_state.shape[:2]
    units = legendre.shape[1] // 2
    fits = (
        lax.axis_size("lat") % (2 * lanes) == 0
        and units % (4 * lanes) == 0
        and lat_rows % GROUP == 0
        and members > 1
    )
    return hub_plan(lanes, *args) if fits else direct_plan(*args)


def solution(mesh):
    in_specs = (
        P("grp", "lat", None, None),
        P("grp", "lat", None, None),
        P("lat", None, None),
        P(),
        P(),
        P(),
        P(),
        P(),
        P(),
    )
    out_specs = (P("grp", "lat", None, None), P("lat", None, None), P("lat", None, None))
    return jax.shard_map(
        functools.partial(per_device, lane_count(mesh)), mesh=mesh, in_specs=in_specs, out_specs=out_specs, check_vma=False
    )
```

```python
import functools
import math

import jax
import jax.numpy as jnp
from jax import lax
from jax.experimental import pallas as pl
from jax.experimental.pallas import tpu as pltpu
from jax.sharding import PartitionSpec as P

BF16 = jnp.bfloat16
F32 = jnp.float32


def wave_table(lon_count, wave_count):
    lon_ids = jnp.arange(lon_count, dtype=jnp.int32)[:, None]
    wave_ids = jnp.arange(wave_count, dtype=jnp.int32)[None, :]
    phase = (lon_ids * wave_ids % lon_count).astype(jnp.float32) * (2.0 * math.pi / lon_count)
    factor = math.sqrt(2.0 / lon_count)
    joined = jnp.concatenate([jnp.cos(phase), -jnp.sin(phase)], axis=1) * factor
    return joined.astype(jnp.bfloat16)


def damping_filter(diffusion, wave_count):
    degree = jnp.arange(wave_count, dtype=jnp.int32).astype(jnp.float32)
    ratio = degree * (degree + 1.0) / float((wave_count - 1) * wave_count)
    return 1.0 / (1.0 + diffusion[None, :] * (ratio * ratio)[:, None])


def analysis_body(table_ref, grid_ref, out_ref):
    bands, _, rows, width, channels = out_ref.shape
    for row in range(0, rows, 2):
        pair = jnp.concatenate([grid_ref[0, row], grid_ref[0, row + 1]], axis=1)
        waves = jnp.dot(table_ref[...], pair, preferred_element_type=F32).astype(BF16)
        for k in range(2):
            out_ref[:, 0, row + k] = waves[:, k * channels:(k + 1) * channels].reshape(
                bands, width, channels
            )


def analyse(grid_state, table, first, count, bands):
    _, lat_rows, lon_count, channels = grid_state.shape
    width = table.shape[0] // bands
    rows = 6
    return pl.pallas_call(
        analysis_body,
        grid=(count, lat_rows // rows),
        in_specs=[
            pl.BlockSpec(table.shape, lambda b, i: (0, 0)),
            pl.BlockSpec((1, rows, lon_count, channels), lambda b, i: (b + first, i, 0, 0)),
        ],
        out_specs=pl.BlockSpec((bands, 1, rows, width, channels), lambda b, i: (0, b, i, 0, 0)),
        out_shape=jax.ShapeDtypeStruct((bands, count, lat_rows, width, channels), BF16),
        cost_estimate=pl.CostEstimate(
            flops=2 * count * lat_rows * lon_count * channels * table.shape[0],
            bytes_accessed=4 * count * lat_rows * lon_count * channels,
            transcendentals=0,
        ),
    )(table, grid_state)


def spectral_body(parts, in_ref, basis_ref, flipped_ref, damping_ref, *rest):
    outs, (fin, fout) = rest[:parts], rest[parts:]
    bands, _, lat_rows, width, channels = in_ref.shape
    waves = basis_ref.shape[0]
    lats = bands * lat_rows
    span = lat_rows * width
    for s in range(bands):
        fin[pl.ds(s * span, span), :] = in_ref[s, 0].astype(F32).reshape(span, channels)
    damping = jnp.concatenate([damping_ref[...]] * 2, axis=1)
    for m in range(waves):
        values = jnp.concatenate(
            [fin[pl.ds(r * waves + m, lats, stride=width), :] for r in range(2)], axis=1
        ).astype(BF16)
        spectrum = jnp.dot(flipped_ref[m], values, preferred_element_type=F32)
        filtered = (spectrum * damping).astype(BF16)
        grid = jnp.dot(basis_ref[m], filtered, preferred_element_type=F32)
        for r in range(2):
            fout[pl.ds(r * waves + m, lats, stride=width), :] = grid[
                :, r * channels:(r + 1) * channels
            ]
    part_rows = lat_rows // parts
    for q in range(parts):
        for s in range(bands):
            start = (s * lat_rows + q * part_rows) * width
            outs[q][s, 0] = (
                fout[pl.ds(start, part_rows * width), :]
                .reshape(part_rows, width, channels)
                .astype(BF16)
            )


def spectral(received, basis, flipped, damping, parts):
    bands, count, lat_rows, width, channels = received.shape
    part_rows = lat_rows // parts
    whole = lambda a: pl.BlockSpec(a.shape, lambda b: (0,) * a.ndim)
    return pl.pallas_call(
        functools.partial(spectral_body, parts),
        grid=(count,),
        in_specs=[
            pl.BlockSpec((bands, 1, lat_rows, width, channels), lambda b: (0, b, 0, 0, 0)),
            whole(basis),
            whole(flipped),
            whole(damping),
        ],
        out_specs=[
            pl.BlockSpec((bands, 1, part_rows, width, channels), lambda b: (0, b, 0, 0, 0))
        ] * parts,
        out_shape=[
            jax.ShapeDtypeStruct((bands, count, part_rows, width, channels), BF16)
        ] * parts,
        scratch_shapes=[pltpu.VMEM((bands * lat_rows * width, channels), F32)] * 2,
        cost_estimate=pl.CostEstimate(
            flops=8 * count * basis.size * channels,
            bytes_accessed=4 * received.size,
            transcendentals=0,
        ),
    )(received, basis, flipped, damping)


def silu(value):
    half = 0.5 * value
    return half + half * jnp.tanh(half)


def physics_body(groups, *refs):
    fields = refs[:groups]
    noise_ref, table_ref, first_ref, bias_ref, middle_ref, last_ref = refs[groups:groups + 6]
    state_ref, stats_ref = refs[-2:]
    members, _, lon_count, channels = noise_ref.shape
    states = []
    for ref in fields:
        count = ref.shape[1]
        waves = jnp.concatenate(
            [ref[:, k, 0].reshape(-1, channels) for k in range(count)], axis=1
        )
        smoothed = jnp.dot(table_ref[...], waves, preferred_element_type=F32)
        for k in range(count):
            flat = smoothed[:, k * channels:(k + 1) * channels]
            b = len(states)
            joined = jnp.concatenate([flat.astype(BF16), noise_ref[b, 0]], axis=1)
            pre = jnp.dot(joined, first_ref[...], preferred_element_type=F32)
            one = silu(pre + bias_ref[...]).astype(BF16)
            two = silu(jnp.dot(one, middle_ref[...], preferred_element_type=F32)).astype(BF16)
            tendency = jnp.dot(two, last_ref[...], preferred_element_type=F32)
            state = (flat + tendency).astype(BF16)
            state_ref[b, 0] = state
            states.append(state)
    values = [s.astype(F32) for s in states]
    total = functools.reduce(jnp.add, values)
    mean = total * (1.0 / members)
    spread = functools.reduce(jnp.add, [jnp.square(v - mean) for v in values])
    half = lon_count // 2
    for h in range(2):
        stats_ref[h, 0, 0] = total[h * half:(h + 1) * half].astype(BF16)
        stats_ref[h, 1, 0] = spread[h * half:(h + 1) * half].astype(BF16)


def physics(fields, noise, table, first, bias, middle, last, part, previous):
    bands, _, part_rows, width, channels = fields[0].shape
    members, lat_rows, lon_count, noise_channels = noise.shape
    whole = lambda a: pl.BlockSpec(a.shape, lambda i: (0,) * a.ndim)
    at = part * part_rows
    specs = [
        pl.BlockSpec((bands, f.shape[1], 1, width, channels), lambda i: (0, 0, i, 0, 0))
        for f in fields
    ]
    specs.append(
        pl.BlockSpec((members, 1, lon_count, noise_channels), lambda i: (0, i + at, 0, 0))
    )
    params = [table, first, bias, middle, last]
    specs += [whole(a) for a in params]
    operands = [*fields, noise, *params]
    aliases = {}
    if previous is not None:
        aliases = {len(operands): 0}
        operands.append(previous)
        specs.append(pl.BlockSpec(memory_space=pl.ANY))
    columns = members * part_rows * lon_count
    hidden = middle.shape[0]
    return pl.pallas_call(
        functools.partial(physics_body, len(fields)),
        grid=(part_rows,),
        in_specs=specs,
        out_specs=[
            pl.BlockSpec((members, 1, lon_count, channels), lambda i: (0, i + at, 0, 0)),
            pl.BlockSpec((2, 2, 1, lon_count // 2, channels), lambda i: (0, 0, i, 0, 0)),
        ],
        out_shape=[
            jax.ShapeDtypeStruct((members, lat_rows, lon_count, channels), BF16),
            jax.ShapeDtypeStruct((2, 2, part_rows, lon_count // 2, channels), BF16),
        ],
        input_output_aliases=aliases,
        cost_estimate=pl.CostEstimate(
            flops=2 * columns * (first.size + middle.size + last.size + 256 * channels),
            bytes_accessed=8 * columns * channels,
            transcendentals=2 * columns * hidden,
        ),
    )(*operands)


def swap(value, bit):
    groups = lax.axis_size("grp")
    return lax.ppermute(value, "grp", [(g, g ^ bit) for g in range(groups)])


def join(a, b, count):
    a, b = a.astype(F32), b.astype(F32)
    total = a[0] + b[0]
    spread = (a[1] + b[1]) + jnp.square(a[0] - b[0]) * (0.5 / count)
    return jnp.stack([total, spread])


def pair_moments(stats, members):
    core = lax.axis_index("grp") % 2
    own = lax.dynamic_index_in_dim(stats, core, 0, keepdims=False)
    other = lax.dynamic_index_in_dim(stats, 1 - core, 0, keepdims=False)
    return join(own, swap(other, 1), members).astype(BF16)


def ensemble_moments(held, members):
    groups = lax.axis_size("grp")
    core = lax.axis_index("grp") % 2
    bit, count = 2, 2 * members
    while bit < groups:
        held = join(held.astype(BF16), swap(held.astype(BF16), bit), count)
        bit, count = 2 * bit, 2 * count
    scale = jnp.array([1.0 / count, 1.0 / (count - 1)], F32)
    held = (held * scale[:, None, None, None]).astype(BF16)
    partner = swap(held, 1)
    low = jnp.where(core == 0, held, partner)
    high = jnp.where(core == 0, partner, held)
    return low, high


def direct_plan(
    grid_state,
    noise_field,
    legendre,
    diffusion,
    input_weight,
    noise_weight,
    input_bias,
    middle_weight,
    output_weight,
):
    members, lat_rows, lon_count, channels = grid_state.shape
    wave_count = legendre.shape[1]
    bands = lax.axis_size("lat")
    local_waves = wave_count // bands
    chunk = 2
    parts = 2
    transform = wave_table(lon_count, wave_count)
    table = (
        transform.reshape(lon_count, 2, bands, local_waves)
        .transpose(0, 2, 1, 3)
        .reshape(lon_count, 2 * wave_count)
    )
    table_t = table.T
    exchange = lambda v: lax.all_to_all(v, "lat", split_axis=0, concat_axis=0, tiled=True)
    damping = damping_filter(diffusion, wave_count)

    sent = [
        analyse(grid_state, table_t, b, chunk, bands) for b in range(0, members, chunk)
    ]
    groups = lax.axis_size("grp")
    turned = legendre.transpose(1, 0, 2).reshape(bands, local_waves * lat_rows, wave_count)
    share = local_waves * lat_rows // groups
    own = lax.dynamic_slice_in_dim(turned, lax.axis_index("grp") * share, share, axis=1)
    basis = lax.all_gather(exchange(own), "grp", axis=1, tiled=True)
    basis = basis.reshape(bands, local_waves, lat_rows, wave_count).transpose(1, 0, 2, 3)
    basis = basis.reshape(local_waves, bands * lat_rows, wave_count)
    zonal_ids = lax.axis_index("lat") * local_waves + jnp.arange(local_waves, dtype=jnp.int32)
    total_ids = jnp.arange(wave_count, dtype=jnp.int32)
    triangle = total_ids[None, :] >= zonal_ids[:, None]
    basis = jnp.where(triangle[:, None], basis, jnp.zeros_like(basis))
    flipped = basis.transpose(0, 2, 1)
    received = [exchange(s) for s in sent]
    banded = [spectral(r, basis, flipped, damping, parts) for r in received]

    first = jnp.concatenate([input_weight, noise_weight], axis=0)
    new_state = None
    moments = []
    for q in range(parts):
        fields = [exchange(g[q]) for g in banded]
        if moments:
            fields, moments[-1] = lax.optimization_barrier((fields, moments[-1]))
        new_state, stats = physics(
            fields, noise_field, table, first, input_bias[None], middle_weight,
            output_weight, q, new_state,
        )
        moments.append(ensemble_moments(pair_moments(stats, members), members))
    joined = [jnp.concatenate([low, high], axis=2) for low, high in moments]
    ens_mean = jnp.concatenate([j[0] for j in joined], axis=0).astype(F32)
    ens_var = jnp.concatenate([j[1] for j in joined], axis=0).astype(F32)
    return (new_state, ens_mean, ens_var)


GROUP = 8


def slot_table(lon_count, wave_count, share, lane_y, lanes):
    offset = jnp.arange(lanes, dtype=jnp.int32)[:, None, None, None]
    p = jnp.arange(2, dtype=jnp.int32)[None, :, None, None]
    part = jnp.arange(2, dtype=jnp.int32)[None, None, :, None]
    unit = (lane_y - offset) % lanes * share + jnp.arange(share, dtype=jnp.int32)[None, None, None, :]
    wave = jnp.where(p == 0, unit, wave_count - unit)
    wave = jnp.where(unit == 0, jnp.where(part == 0, 0, wave_count // 2), wave)
    wave, unit, p, part = jnp.broadcast_arrays(wave, unit, p, part)
    quarter = jnp.where(unit == 0, p, part) * lon_count
    lon_ids = jnp.arange(lon_count, dtype=jnp.int32)
    turn = (4 * (wave.reshape(-1, 1) * lon_ids[None, :]) + quarter.reshape(-1, 1)) % (4 * lon_count)
    phase = turn.astype(F32) * (0.5 * math.pi / lon_count)
    return (jnp.cos(phase) * math.sqrt(2.0 / lon_count)).astype(BF16)


WAIT = pl.BlockSpec(memory_space=pl.ANY)
MESH = pl.DeviceIdType.MESH


def basis_body(start_ref, waves_ref, out_ref):
    lanes, entries, rows, totals = out_ref.shape
    count, lat_rows, _ = waves_ref.shape
    groups = lat_rows // GROUP
    row = lax.broadcasted_iota(jnp.int32, (lat_rows, totals), 1)
    flip = lax.broadcasted_iota(jnp.int32, (totals, totals), 0)
    flip = flip + lax.broadcasted_iota(jnp.int32, (totals, totals), 1) == totals - 1
    flip = flip.astype(F32).astype(BF16)
    for dy in range(lanes):
        def step(i, carry):
            unit = start_ref[dy * entries + i]
            low = waves_ref[jnp.minimum(unit, count - 1)].astype(F32)
            high = jnp.dot(
                waves_ref[jnp.clip(count - unit, 0, count - 1)], flip, preferred_element_type=F32
            )
            low = jnp.where(row >= unit, low, 0.0).reshape(groups, 1, GROUP, totals)
            high = jnp.where(row < unit, high, 0.0).reshape(groups, 1, GROUP, totals)
            both = jnp.concatenate([low, high], axis=1).reshape(rows, totals)
            out_ref[dy, i] = both.astype(BF16)
            return carry
        lax.fori_loop(0, entries, step, 0, unroll=6)


def basis_blocks(units, turned):
    lanes, entries = units.shape
    count, lat_rows, totals = turned.shape
    whole = lambda a: pl.BlockSpec(a.shape, lambda: (0,) * a.ndim)
    shape = (lanes, entries, 2 * lat_rows, totals)
    return pl.pallas_call(
        basis_body,
        in_specs=[pl.BlockSpec(memory_space=pltpu.SMEM), whole(turned)],
        out_specs=pl.BlockSpec(shape, lambda: (0,) * 4),
        out_shape=jax.ShapeDtypeStruct(shape, BF16),
        cost_estimate=pl.CostEstimate(
            flops=2 * lanes * entries * lat_rows * totals * totals,
            bytes_accessed=4 * lanes * entries * lat_rows * totals,
            transcendentals=0,
        ),
    )(units.reshape(-1), turned)


def pipeline_body(lanes, far, cuts, grid_ref, noise_ref, table_t_ref, table_ref, blocks_ref, damping_ref, mirrored_ref,
                  first_ref, bias_ref, middle_ref, last_ref, state_ref, fields_ref, kept, sent, own, other, back,
                  basis, flipped, rows_in, rows_out, *rest):
    scratch = rest[:2 * lanes]
    (row_sem, out_sem, field_sem, basis_send, basis_recv, kept_send, kept_recv, own_send, own_recv, back_send,
     back_recv) = rest[2 * lanes:]
    members, lat_rows, lon_count, channels = grid_ref.shape
    blocks, share, depth = kept.shape[1:4]
    slots, per, totals, width = own.shape
    ahead = slots // 2
    entries = blocks_ref.shape[1]
    groups = lat_rows // GROUP
    rows = 2 * GROUP
    pitch = scratch[0].shape[0] // share
    chunks = members * cuts
    index, team = lax.axis_index("lat"), lax.axis_index("grp")
    place, lane = index // lanes, index % lanes
    half = place // far
    dist = (1 - half) * (far - 1 - place) + half * (place - far)
    hub_place = far - 1 + half
    opposite = (far - half) * lanes + lane
    core = team % 2
    partner = team + 1 - 2 * core
    hub, leaf = dist == 0, dist > 0
    start = lane * share
    ranges = [pl.ds(q * per, per) for q in range(cuts)]

    def remote(src, dst, send, recv, **target):
        return pltpu.make_async_remote_copy(
            src_ref=src, dst_ref=dst, send_sem=send, recv_sem=recv, device_id=target, device_id_type=MESH
        )

    def hub_lane(dy):
        return hub_place * lanes + (lane + lanes - dy) % lanes

    def source_lane(k):
        return (hub_place + (2 * half - 1) * (k // lanes)) * lanes + (lane + k % lanes) % lanes

    def basis_copy(dy):
        at = pl.multiple_of((dist * lanes + dy) * depth, depth)
        return remote(
            blocks_ref.at[dy], basis.at[pl.ds(core * entries, entries), pl.ds(at, depth)],
            basis_send.at[dy], basis_recv.at[dist * lanes + dy], lat=hub_lane(dy),
        )

    def basis_own():
        return pltpu.make_async_copy(
            blocks_ref.at[0], basis.at[pl.ds(core * entries, entries), pl.ds(0, depth)], basis_recv.at[0]
        )

    def basis_swap():
        part = basis.at[pl.ds(core * entries, entries)]
        return remote(part, part, basis_send.at[lanes], basis_recv.at[blocks], grp=partner)

    def lane_copy(b, q, dy):
        return remote(
            sent.at[b, dy - 1, ranges[q]], kept.at[b, dy, ranges[q]], kept_send.at[b, q, dy - 1],
            kept_recv.at[b, q, dy], lat=place * lanes + (lane + lanes - dy) % lanes,
        )

    def kept_copy(b, q, dy):
        k = dist * lanes + dy
        return remote(
            kept.at[b, dy, ranges[q]], kept.at[b, k, ranges[q]], kept_send.at[b, q, lanes - 1 + dy],
            kept_recv.at[b, q, k], lat=hub_lane(0),
        )

    def kept_arrival(b, q, k):
        part = kept.at[b, k, pl.ds(q * per, per)]
        return remote(part, part, kept_send.at[b, q, 0], kept_recv.at[b, q, k], lat=opposite)

    def own_copy(c):
        return remote(own.at[c % slots], other.at[c], own_send.at[c], own_recv.at[c], lat=opposite)

    def back_copy(b, q, k):
        units = pl.ds(q * per, per)
        return remote(
            kept.at[b, k, units], back.at[b, k % lanes, units], back_send.at[b, q, k - 1],
            back_recv.at[b, q, k % lanes], lat=source_lane(k),
        )

    def back_arrival(b, q, dy):
        part = back.at[b, dy, pl.ds(q * per, per)]
        return remote(part, part, back_send.at[b, q, 0], back_recv.at[b, q, dy], lat=opposite)

    def load(ref, n):
        at = pl.multiple_of(n % groups * GROUP, GROUP)
        return pltpu.make_async_copy(
            ref.at[n // groups, pl.ds(at, GROUP)], rows_in.at[n % 2], row_sem.at[n % 2]
        )

    def store(n):
        at = pl.multiple_of(n % groups * GROUP, GROUP)
        return pltpu.make_async_copy(
            rows_out.at[n % 2], state_ref.at[n // groups, pl.ds(at, GROUP)], out_sem.at[n % 2]
        )

    def analyse_group(n, carry):
        b = n // groups
        at = pl.multiple_of(n % groups * rows, rows)

        @pl.when(n + 1 < members * groups)
        def _():
            load(grid_ref, n + 1).start()

        load(grid_ref, n).wait()
        for k in range(0, GROUP, 2):
            pair = jnp.concatenate([rows_in[n % 2, k], rows_in[n % 2, k + 1]], axis=1)
            waves = jnp.dot(table_t_ref[...], pair, preferred_element_type=F32)
            row = 0
            for dy in range(lanes):
                for p in range(2):
                    for part in range(2):
                        for t in range(2):
                            scratch[2 * dy + part][pl.ds(p * GROUP + k + t, share, stride=pitch), :] = (
                                waves[row:row + share, t * channels:(t + 1) * channels]
                            )
                        row += share
        for dy in range(lanes):
            for part in range(2):
                value = scratch[2 * dy + part][...].reshape(share, pitch, channels)[:, :rows].astype(BF16)
                side = slice(part * channels, (part + 1) * channels)
                if dy == 0:
                    kept[b, 0, :, pl.ds(at, rows), side] = value
                else:
                    sent[b, dy - 1, :, pl.ds(at, rows), side] = value
        return carry

    def partial(c):
        b, q = c // cuts, c % cuts
        for k in range(1, blocks):
            kept_arrival(b, q, k).wait_recv()

        @pl.when(c >= slots)
        def _():
            own_copy(c - slots).wait_send()

        def unit(j, carry):
            values = jnp.concatenate([kept[b, k, q * per + j] for k in range(blocks)], axis=0)
            sums = jnp.dot(flipped[q * per + j], values, preferred_element_type=F32)
            own[c % slots, j] = sums.astype(BF16)
            return carry

        lax.fori_loop(0, per, unit, 0, unroll=True)

        @pl.when(q == 0)
        def _():
            values = jnp.concatenate([kept[b, k, 0, :, channels:] for k in range(blocks)], axis=0)
            sums = jnp.dot(flipped[share], values, preferred_element_type=F32)
            own[c % slots, 0, :, channels:] = sums.astype(BF16)

        own_copy(c).start()

    def synthesise(c):
        b, q = c // cuts, c % cuts
        own_copy(c).wait_recv()
        row = lax.broadcasted_iota(jnp.int32, (totals, channels), 0)

        def damped(j, mark, side):
            total = own[c % slots, j, :, side].astype(F32) + other[c, j, :, side].astype(F32)
            return (total * jnp.where(row < mark, mirrored_ref[...], damping_ref[...])).astype(BF16)

        def put(i, grid, side):
            back[b, 0, i, :, side] = grid[:depth]
            for k in range(1, blocks):
                kept[b, k, i, :, side] = grid[k * depth:(k + 1) * depth]

        def unit(j, carry):
            mark = start + q * per + j
            value = jnp.concatenate(
                [damped(j, mark, slice(r * channels, (r + 1) * channels)) for r in range(2)], axis=1
            )
            grid = jnp.dot(basis[q * per + j], value, preferred_element_type=F32).astype(BF16)
            put(q * per + j, grid, slice(None))
            return carry

        lax.fori_loop(0, per, unit, 0, unroll=True)

        @pl.when(q == 0)
        def _():
            mark = jnp.where(start == 0, totals // 2, start)
            side = slice(channels, 2 * channels)
            grid = jnp.dot(basis[share], damped(0, mark, side), preferred_element_type=F32).astype(BF16)
            put(0, grid, side)

        for k in range(1, blocks):
            back_copy(b, q, k).start()

    def column_group(b, g):
        n = b * groups + g
        at = pl.multiple_of(g * rows, rows)

        @pl.when(n + 1 < (members - 1) * groups)
        def _():
            load(noise_ref, n + 1).start()

        @pl.when(g == 0)
        def _():
            for q in range(cuts):
                for dy in range(lanes):
                    if dy > 0:
                        back_arrival(b, q, dy).wait_recv()
                    else:
                        @pl.when(leaf)
                        def _():
                            back_arrival(b, q, dy).wait_recv()

        for dy in range(lanes):
            for part in range(2):
                side = slice(part * channels, (part + 1) * channels)
                value = back[b, dy, :, pl.ds(at, rows), side].astype(F32)
                space = jnp.zeros((share, pitch - rows, channels), F32)
                scratch[2 * dy + part][...] = jnp.concatenate([value, space], axis=1).reshape(-1, channels)
        load(noise_ref, n).wait()

        @pl.when(n >= 2)
        def _():
            store(n - 2).wait()

        def pair(i, carry):
            waves = []
            for t in range(2):
                waves.append(jnp.concatenate([
                    scratch[2 * dy + part][pl.ds(p * GROUP + 2 * i + t, share, stride=pitch), :]
                    for dy in range(lanes) for p in range(2) for part in range(2)
                ], axis=0).astype(BF16))
            smoothed = jnp.dot(table_ref[...], jnp.concatenate(waves, axis=1), preferred_element_type=F32)
            for t in range(2):
                flat = smoothed[:, t * channels:(t + 1) * channels]
                joined = jnp.concatenate([flat.astype(BF16), rows_in[n % 2, 2 * i + t]], axis=1)
                pre = jnp.dot(joined, first_ref[...], preferred_element_type=F32)
                one = silu(pre + bias_ref[...]).astype(BF16)
                two = silu(jnp.dot(one, middle_ref[...], preferred_element_type=F32)).astype(BF16)
                tendency = jnp.dot(two, last_ref[...], preferred_element_type=F32)
                rows_out[n % 2, 2 * i + t] = (flat + tendency).astype(BF16)
            return carry

        lax.fori_loop(0, GROUP // 2, pair, 0)
        store(n).start()

    for dy in range(1, lanes):
        basis_copy(dy).start()

    @pl.when(leaf)
    def _():
        basis_copy(0).start()

    @pl.when(hub)
    def _():
        basis_own().start()

    load(grid_ref, 0).start()

    def member(b, carry):
        lax.fori_loop(b * groups, (b + 1) * groups, analyse_group, 0)
        for q in range(cuts):
            for dy in range(1, lanes):
                lane_copy(b, q, dy).start()

        @pl.when(leaf)
        def _():
            kept_copy(b, 0, 0).start()
            for q in range(cuts):
                if q + 1 < cuts:
                    kept_copy(b, q + 1, 0).start()
                for dy in range(1, lanes):
                    kept_arrival(b, q, dy).wait_recv()
                    kept_copy(b, q, dy).start()
        return carry

    lax.fori_loop(0, members, member, 0)
    load(noise_ref, 0).start()

    @pl.when(hub)
    def _():
        basis_own().wait()
        for k in range(1, blocks):
            part = basis.at[pl.ds(core * entries, entries), pl.ds(k * depth, depth)]
            remote(part, part, basis_send.at[0], basis_recv.at[k], lat=opposite).wait_recv()
        basis_swap().start()
        basis_swap().wait_recv()

        def turn(i, carry):
            flipped[i] = basis[i].T
            return carry

        lax.fori_loop(0, share + 1, turn, 0, unroll=3)

    def tick(t, carry):
        @pl.when(hub)
        def _():
            @pl.when(t < chunks)
            def _():
                partial(t)

            @pl.when(t >= ahead)
            def _():
                synthesise(t - ahead)

        late = t - cuts - ahead
        g = (late + cuts) % cuts

        @pl.when((late >= 0) & (g < groups))
        def _():
            column_group(late // cuts, g)
        return carry

    lax.fori_loop(0, chunks + ahead, tick, 0)

    last = members - 1
    for q in range(cuts):
        for dy in range(lanes):
            if dy > 0:
                back_arrival(last, q, dy).wait_recv()
            else:
                @pl.when(leaf)
                def _():
                    back_arrival(last, q, dy).wait_recv()
    final = pltpu.make_async_copy(back.at[last], fields_ref, field_sem)
    final.start()
    for n in ((members - 1) * groups - 2, (members - 1) * groups - 1):
        store(n).wait()

    def drain(b, carry):
        for q in range(cuts):
            for dy in range(1, lanes):
                lane_copy(b, q, dy).wait_send()

            @pl.when(leaf)
            def _():
                for dy in range(lanes):
                    kept_copy(b, q, dy).wait_send()

            @pl.when(hub)
            def _():
                for k in range(1, blocks):
                    back_copy(b, q, k).wait_send()
        return carry

    lax.fori_loop(0, members, drain, 0)

    @pl.when(hub)
    def _():
        basis_swap().wait_send()
        for c in range(chunks - slots, chunks):
            own_copy(c).wait_send()

    @pl.when(leaf)
    def _():
        basis_copy(0).wait_send()

    for dy in range(1, lanes):
        basis_copy(dy).wait_send()
    final.wait()


def pipeline(lanes, far, cuts, grid_state, noise, table_t, table, blocks, damping, first, bias, middle, output):
    members, lat_rows, lon_count, channels = grid_state.shape
    wave_count = damping.shape[0]
    share = wave_count // 2 // lanes
    entries = blocks.shape[1]
    depth = 2 * lat_rows
    count = far * lanes
    per = share // cuts
    slots = 4
    vmem = pl.BlockSpec(memory_space=pltpu.VMEM)
    dma = pltpu.SemaphoreType.DMA
    return pl.pallas_call(
        functools.partial(pipeline_body, lanes, far, cuts),
        in_specs=[WAIT, WAIT, vmem, vmem, WAIT, vmem, vmem, vmem, vmem, vmem, vmem],
        out_specs=[WAIT, WAIT],
        out_shape=[
            jax.ShapeDtypeStruct(grid_state.shape, BF16),
            jax.ShapeDtypeStruct((lanes, share, depth, 2 * channels), BF16),
        ],
        scratch_shapes=[
            pltpu.VMEM((members, count, share, depth, 2 * channels), BF16),
            pltpu.VMEM((members, lanes - 1, share, depth, 2 * channels), BF16),
            pltpu.VMEM((slots, per, wave_count, 2 * channels), BF16),
            pltpu.VMEM((members * cuts, per, wave_count, 2 * channels), BF16),
            pltpu.VMEM((members, lanes, share, depth, 2 * channels), BF16),
            pltpu.VMEM((2 * entries, count * depth, wave_count), BF16),
            pltpu.VMEM((share + 1, wave_count, count * depth), BF16),
            pltpu.VMEM((2, GROUP, lon_count, channels), BF16),
            pltpu.VMEM((2, GROUP, lon_count, channels), BF16),
        ] + [pltpu.VMEM((share * 3 * GROUP, channels), F32)] * (2 * lanes) + [
            dma((2,)),
            dma((2,)),
            dma,
            dma((lanes + 1,)),
            dma((count + 1,)),
            dma((members, cuts, 2 * lanes - 1)),
            dma((members, cuts, count)),
            dma((members * cuts,)),
            dma((members * cuts,)),
            dma((members, cuts, count - 1)),
            dma((members, cuts, lanes)),
        ],
        compiler_params=pltpu.CompilerParams(
            has_side_effects=True, vmem_limit_bytes=64000 * 1024
        ),
    )(grid_state, noise, table_t, table, blocks, damping, damping[::-1], first, bias, middle, output)


def column_body(lanes, far, last, *refs):
    dist_ref, fields = refs[0], refs[1:1 + lanes * far]
    noise_ref, table_ref, first_ref, bias_ref, middle_ref, last_ref = refs[1 + lanes * far:7 + lanes * far]
    scratch = refs[-2 * lanes:]
    outs = refs[-2 * lanes - (2 if last else 1):-2 * lanes]
    state_ref = outs[0]
    _, lats, lon_count, channels = noise_ref.shape
    _, share, rows, _ = fields[0].shape
    group = rows // 2
    pitch = scratch[0].shape[0] // share
    inner = pl.program_id(1)

    @pl.when(inner == 0)
    def _():
        for dy in range(lanes):
            for i in range(share):
                value = fields[dy * far][0, i]
                for d in range(1, far):
                    value = jnp.where(dist_ref[0] == d, fields[dy * far + d][0, i], value)
                value = value.astype(F32)
                for part in range(2):
                    scratch[2 * dy + part][i * pitch:i * pitch + rows, :] = (
                        value[:, part * channels:(part + 1) * channels]
                    )

    waves = []
    for k in range(lats):
        at = inner * lats + k
        waves.append(jnp.concatenate([
            scratch[2 * dy + part][pl.ds(p * group + at, share, stride=pitch), :]
            for dy in range(lanes) for p in range(2) for part in range(2)
        ], axis=0).astype(BF16))
    smoothed = jnp.dot(table_ref[...], jnp.concatenate(waves, axis=1), preferred_element_type=F32)
    for k in range(lats):
        flat = smoothed[:, k * channels:(k + 1) * channels]
        joined = jnp.concatenate([flat.astype(BF16), noise_ref[0, k]], axis=1)
        pre = jnp.dot(joined, first_ref[...], preferred_element_type=F32)
        one = silu(pre + bias_ref[...]).astype(BF16)
        two = silu(jnp.dot(one, middle_ref[...], preferred_element_type=F32)).astype(BF16)
        tendency = jnp.dot(two, last_ref[...], preferred_element_type=F32)
        state = (flat + tendency).astype(BF16)
        state_ref[0, k] = state
        if last:
            held_ref, stats_ref = refs[7 + lanes * far], outs[1]
            members = held_ref.shape[0] + 1
            values = [held_ref[b, k].astype(F32) for b in range(members - 1)] + [state.astype(F32)]
            total = functools.reduce(jnp.add, values)
            mean = total * (1.0 / members)
            spread = functools.reduce(jnp.add, [jnp.square(v - mean) for v in values])
            half = lon_count // 2
            for h in range(2):
                stats_ref[h, 0, k] = total[h * half:(h + 1) * half].astype(BF16)
                stats_ref[h, 1, k] = spread[h * half:(h + 1) * half].astype(BF16)


def columns(fields, dist, noise, table, first, bias, middle, output, member, part, previous):
    lanes, far = len(fields), len(fields[0])
    members, lat_rows, lon_count, channels = noise.shape
    _, share, depth, width = fields[0][0].shape
    rows = 2 * GROUP
    groups = 1 if part is not None else depth // rows
    lats = 2
    inner = GROUP // lats
    at = 0 if part is None else part
    last = part is not None
    whole = lambda a: pl.BlockSpec(a.shape, lambda g, i: (0,) * a.ndim)
    params = [table, first, bias, middle, output]
    operands = [dist, *[f for each in fields for f in each], noise, *params]
    row_block = lambda g, i: (member, (g + at) * inner + i, 0, 0)
    specs = [pl.BlockSpec(memory_space=pltpu.SMEM)]
    specs += [pl.BlockSpec((1, share, rows, width), lambda g, i: (0, 0, g + at, 0))] * (lanes * far)
    specs.append(pl.BlockSpec((1, lats, lon_count, channels), row_block))
    specs += [whole(a) for a in params]
    aliases = {}
    if previous is not None:
        aliases = {len(operands): 0}
        operands.append(previous)
        if last:
            specs.append(pl.BlockSpec(
                (members - 1, lats, lon_count, channels), lambda g, i: (0, (g + at) * inner + i, 0, 0)
            ))
        else:
            specs.append(pl.BlockSpec(memory_space=pl.ANY))
    out_specs = [pl.BlockSpec((1, lats, lon_count, channels), row_block)]
    out_shape = [jax.ShapeDtypeStruct(noise.shape, BF16)]
    if last:
        half = lon_count // 2
        out_specs.append(
            pl.BlockSpec((2, 2, lats, half, channels), lambda g, i: (0, 0, g * inner + i, 0, 0))
        )
        out_shape.append(jax.ShapeDtypeStruct((2, 2, groups * GROUP, half, channels), BF16))
    points = groups * GROUP * lon_count
    hidden = middle.shape[0]
    return pl.pallas_call(
        functools.partial(column_body, lanes, far, last),
        grid=(groups, inner),
        in_specs=specs,
        out_specs=out_specs,
        out_shape=out_shape,
        input_output_aliases=aliases,
        scratch_shapes=[pltpu.VMEM((share * 3 * GROUP, channels), F32)] * (2 * lanes),
        cost_estimate=pl.CostEstimate(
            flops=2 * points * (first.size + middle.size + output.size + 256 * channels),
            bytes_accessed=8 * points * channels,
            transcendentals=2 * points * hidden,
        ),
    )(*operands)


def hub_plan(
    lanes,
    grid_state,
    noise_field,
    legendre,
    diffusion,
    input_weight,
    noise_weight,
    input_bias,
    middle_weight,
    output_weight,
):
    members, lat_rows, lon_count, channels = grid_state.shape
    wave_count = legendre.shape[1]
    far = lax.axis_size("lat") // lanes // 2
    share = wave_count // 2 // lanes
    parts = lat_rows // GROUP
    cuts = 4
    lane = lax.axis_index("lat") % lanes
    core = lax.axis_index("grp") % 2
    entries = share // 2 + 1
    local = core * entries + jnp.arange(entries, dtype=jnp.int32)[None, :]
    owner = (lane - jnp.arange(lanes, dtype=jnp.int32)[:, None]) % lanes * share
    extra = jnp.where(owner == 0, wave_count // 2, owner)
    units = jnp.where(local < share, owner + local, extra)
    blocks = basis_blocks(units, legendre.transpose(1, 0, 2))

    table_t = slot_table(lon_count, wave_count, share, lane, lanes)
    table = table_t.T
    damping = damping_filter(diffusion, wave_count)
    first = jnp.concatenate([input_weight, noise_weight], axis=0)
    params = (first, input_bias[None], middle_weight, output_weight)
    new_state, found = pipeline(
        lanes, far, cuts, grid_state, noise_field, table_t, table, blocks, damping, *params
    )
    fields = [[found[dy][None]] for dy in range(lanes)]
    dist = jnp.zeros((1,), jnp.int32)
    moments = []
    for q in range(parts):
        new_state, stats = columns(
            fields, dist, noise_field, table, *params, members - 1, q, new_state
        )
        moments.append(ensemble_moments(pair_moments(stats, members), members))
    joined = [jnp.concatenate([low, high], axis=2) for low, high in moments]
    ens_mean = jnp.concatenate([j[0] for j in joined], axis=0).astype(F32)
    ens_var = jnp.concatenate([j[1] for j in joined], axis=0).astype(F32)
    return (new_state, ens_mean, ens_var)


def lane_count(mesh):
    line = [getattr(d, "coords", None) for d in mesh.devices.reshape(-1, mesh.shape["lat"])[0]]
    if len(line) < 2 or line[0] is None:
        return 2
    axis = [a != b for a, b in zip(line[0], line[1])].index(True)
    return len({c[axis] for c in line})


def per_device(lanes, *args):
    grid_state, legendre = args[0], args[2]
    members, lat_rows = grid_state.shape[:2]
    units = legendre.shape[1] // 2
    fits = (
        lax.axis_size("lat") % (2 * lanes) == 0
        and units % (4 * lanes) == 0
        and lat_rows % GROUP == 0
        and members > 1
    )
    return hub_plan(lanes, *args) if fits else direct_plan(*args)


def solution(mesh):
    in_specs = (
        P("grp", "lat", None, None),
        P("grp", "lat", None, None),
        P("lat", None, None),
        P(),
        P(),
        P(),
        P(),
        P(),
        P(),
    )
    out_specs = (P("grp", "lat", None, None), P("lat", None, None), P("lat", None, None))
    return jax.shard_map(
        functools.partial(per_device, lane_count(mesh)), mesh=mesh, in_specs=in_specs, out_specs=out_specs, check_vma=False
    )
```

```python
import functools
import math

import jax
import jax.numpy as jnp
from jax import lax
from jax.experimental import pallas as pl
from jax.experimental.pallas import tpu as pltpu
from jax.sharding import PartitionSpec as P


BF16 = jnp.bfloat16
F32 = jnp.float32


def wave_table(lon_count, wave_count):
    lon_ids = jnp.arange(lon_count, dtype=jnp.int32)[:, None]
    wave_ids = jnp.arange(wave_count, dtype=jnp.int32)[None, :]
    phase = (lon_ids * wave_ids % lon_count).astype(jnp.float32) * (2.0 * math.pi / lon_count)
    factor = math.sqrt(2.0 / lon_count)
    joined = jnp.concatenate([jnp.cos(phase), -jnp.sin(phase)], axis=1) * factor
    return joined.astype(jnp.bfloat16)


def damping_filter(diffusion, wave_count):
    degree = jnp.arange(wave_count, dtype=jnp.int32).astype(jnp.float32)
    ratio = degree * (degree + 1.0) / float((wave_count - 1) * wave_count)
    return 1.0 / (1.0 + diffusion[None, :] * (ratio * ratio)[:, None])


def analysis_body(table_ref, grid_ref, out_ref):
    bands, _, rows, width, channels = out_ref.shape
    for row in range(0, rows, 2):
        pair = jnp.concatenate([grid_ref[0, row], grid_ref[0, row + 1]], axis=1)
        waves = jnp.dot(table_ref[...], pair, preferred_element_type=F32).astype(BF16)
        for k in range(2):
            out_ref[:, 0, row + k] = waves[:, k * channels:(k + 1) * channels].reshape(
                bands, width, channels
            )


def analyse(grid_state, table, first, count, bands):
    _, lat_rows, lon_count, channels = grid_state.shape
    width = table.shape[0] // bands
    rows = 6
    return pl.pallas_call(
        analysis_body,
        grid=(count, lat_rows // rows),
        in_specs=[
            pl.BlockSpec(table.shape, lambda b, i: (0, 0)),
            pl.BlockSpec((1, rows, lon_count, channels), lambda b, i: (b + first, i, 0, 0)),
        ],
        out_specs=pl.BlockSpec((bands, 1, rows, width, channels), lambda b, i: (0, b, i, 0, 0)),
        out_shape=jax.ShapeDtypeStruct((bands, count, lat_rows, width, channels), BF16),
        cost_estimate=pl.CostEstimate(
            flops=2 * count * lat_rows * lon_count * channels * table.shape[0],
            bytes_accessed=4 * count * lat_rows * lon_count * channels,
            transcendentals=0,
        ),
    )(table, grid_state)


def spectral_body(parts, in_ref, basis_ref, flipped_ref, damping_ref, *rest):
    outs, (fin, fout) = rest[:parts], rest[parts:]
    bands, _, lat_rows, width, channels = in_ref.shape
    waves = basis_ref.shape[0]
    lats = bands * lat_rows
    span = lat_rows * width
    for s in range(bands):
        fin[pl.ds(s * span, span), :] = in_ref[s, 0].astype(F32).reshape(span, channels)
    damping = jnp.concatenate([damping_ref[...]] * 2, axis=1)
    for m in range(waves):
        values = jnp.concatenate(
            [fin[pl.ds(r * waves + m, lats, stride=width), :] for r in range(2)], axis=1
        ).astype(BF16)
        spectrum = jnp.dot(flipped_ref[m], values, preferred_element_type=F32)
        filtered = (spectrum * damping).astype(BF16)
        grid = jnp.dot(basis_ref[m], filtered, preferred_element_type=F32)
        for r in range(2):
            fout[pl.ds(r * waves + m, lats, stride=width), :] = grid[
                :, r * channels:(r + 1) * channels
            ]
    part_rows = lat_rows // parts
    for q in range(parts):
        for s in range(bands):
            start = (s * lat_rows + q * part_rows) * width
            outs[q][s, 0] = (
                fout[pl.ds(start, part_rows * width), :]
                .reshape(part_rows, width, channels)
                .astype(BF16)
            )


def spectral(received, basis, flipped, damping, parts):
    bands, count, lat_rows, width, channels = received.shape
    part_rows = lat_rows // parts
    whole = lambda a: pl.BlockSpec(a.shape, lambda b: (0,) * a.ndim)
    return pl.pallas_call(
        functools.partial(spectral_body, parts),
        grid=(count,),
        in_specs=[
            pl.BlockSpec((bands, 1, lat_rows, width, channels), lambda b: (0, b, 0, 0, 0)),
            whole(basis),
            whole(flipped),
            whole(damping),
        ],
        out_specs=[
            pl.BlockSpec((bands, 1, part_rows, width, channels), lambda b: (0, b, 0, 0, 0))
        ] * parts,
        out_shape=[
            jax.ShapeDtypeStruct((bands, count, part_rows, width, channels), BF16)
        ] * parts,
        scratch_shapes=[pltpu.VMEM((bands * lat_rows * width, channels), F32)] * 2,
        cost_estimate=pl.CostEstimate(
            flops=8 * count * basis.size * channels,
            bytes_accessed=4 * received.size,
            transcendentals=0,
        ),
    )(received, basis, flipped, damping)


def silu(value):
    half = 0.5 * value
    return half + half * jnp.tanh(half)


def physics_body(groups, *refs):
    fields = refs[:groups]
    noise_ref, table_ref, first_ref, bias_ref, middle_ref, last_ref = refs[groups:groups + 6]
    state_ref, stats_ref = refs[-2:]
    members, _, lon_count, channels = noise_ref.shape
    states = []
    for ref in fields:
        count = ref.shape[1]
        waves = jnp.concatenate(
            [ref[:, k, 0].reshape(-1, channels) for k in range(count)], axis=1
        )
        smoothed = jnp.dot(table_ref[...], waves, preferred_element_type=F32)
        for k in range(count):
            flat = smoothed[:, k * channels:(k + 1) * channels]
            b = len(states)
            joined = jnp.concatenate([flat.astype(BF16), noise_ref[b, 0]], axis=1)
            pre = jnp.dot(joined, first_ref[...], preferred_element_type=F32)
            one = silu(pre + bias_ref[...]).astype(BF16)
            two = silu(jnp.dot(one, middle_ref[...], preferred_element_type=F32)).astype(BF16)
            tendency = jnp.dot(two, last_ref[...], preferred_element_type=F32)
            state = (flat + tendency).astype(BF16)
            state_ref[b, 0] = state
            states.append(state)
    values = [s.astype(F32) for s in states]
    total = functools.reduce(jnp.add, values)
    mean = total * (1.0 / members)
    spread = functools.reduce(jnp.add, [jnp.square(v - mean) for v in values])
    half = lon_count // 2
    for h in range(2):
        stats_ref[h, 0, 0] = total[h * half:(h + 1) * half].astype(BF16)
        stats_ref[h, 1, 0] = spread[h * half:(h + 1) * half].astype(BF16)


def physics(fields, noise, table, first, bias, middle, last, part, previous):
    bands, _, part_rows, width, channels = fields[0].shape
    members, lat_rows, lon_count, noise_channels = noise.shape
    whole = lambda a: pl.BlockSpec(a.shape, lambda i: (0,) * a.ndim)
    at = part * part_rows
    specs = [
        pl.BlockSpec((bands, f.shape[1], 1, width, channels), lambda i: (0, 0, i, 0, 0))
        for f in fields
    ]
    specs.append(
        pl.BlockSpec((members, 1, lon_count, noise_channels), lambda i: (0, i + at, 0, 0))
    )
    params = [table, first, bias, middle, last]
    specs += [whole(a) for a in params]
    operands = [*fields, noise, *params]
    aliases = {}
    if previous is not None:
        aliases = {len(operands): 0}
        operands.append(previous)
        specs.append(pl.BlockSpec(memory_space=pl.ANY))
    columns = members * part_rows * lon_count
    hidden = middle.shape[0]
    return pl.pallas_call(
        functools.partial(physics_body, len(fields)),
        grid=(part_rows,),
        in_specs=specs,
        out_specs=[
            pl.BlockSpec((members, 1, lon_count, channels), lambda i: (0, i + at, 0, 0)),
            pl.BlockSpec((2, 2, 1, lon_count // 2, channels), lambda i: (0, 0, i, 0, 0)),
        ],
        out_shape=[
            jax.ShapeDtypeStruct((members, lat_rows, lon_count, channels), BF16),
            jax.ShapeDtypeStruct((2, 2, part_rows, lon_count // 2, channels), BF16),
        ],
        input_output_aliases=aliases,
        cost_estimate=pl.CostEstimate(
            flops=2 * columns * (first.size + middle.size + last.size + 256 * channels),
            bytes_accessed=8 * columns * channels,
            transcendentals=2 * columns * hidden,
        ),
    )(*operands)


def swap(value, bit):
    groups = lax.axis_size("grp")
    return lax.ppermute(value, "grp", [(g, g ^ bit) for g in range(groups)])


def join(a, b, count):
    a, b = a.astype(F32), b.astype(F32)
    total = a[0] + b[0]
    spread = (a[1] + b[1]) + jnp.square(a[0] - b[0]) * (0.5 / count)
    return total, spread


def pair_moments(stats, members):
    core = lax.axis_index("grp") % 2
    own = lax.dynamic_index_in_dim(stats, core, 0, keepdims=False)
    other = lax.dynamic_index_in_dim(stats, 1 - core, 0, keepdims=False)
    return jnp.stack(join(own, swap(other, 1), members)).astype(BF16)


def ensemble_moments(held, members):
    groups = lax.axis_size("grp")
    core = lax.axis_index("grp") % 2
    bit, count = 2, 2 * members
    while bit < groups:
        held = jnp.stack(join(held.astype(BF16), swap(held.astype(BF16), bit), count))
        bit, count = 2 * bit, 2 * count
    scale = jnp.array([1.0 / count, 1.0 / (count - 1)], F32)
    held = (held * scale[:, None, None, None]).astype(BF16)
    partner = swap(held, 1)
    low = jnp.where(core == 0, held, partner)
    high = jnp.where(core == 0, partner, held)
    return low, high


def direct_plan(
    grid_state,
    noise_field,
    legendre,
    diffusion,
    input_weight,
    noise_weight,
    input_bias,
    middle_weight,
    output_weight,
):
    members, lat_rows, lon_count, _ = grid_state.shape
    wave_count = legendre.shape[1]
    bands = lax.axis_size("lat")
    local_waves = wave_count // bands
    chunk = 2
    parts = 2
    transform = wave_table(lon_count, wave_count)
    table = (
        transform.reshape(lon_count, 2, bands, local_waves)
        .transpose(0, 2, 1, 3)
        .reshape(lon_count, 2 * wave_count)
    )
    table_t = table.T
    exchange = lambda v: lax.all_to_all(v, "lat", split_axis=0, concat_axis=0, tiled=True)
    damping = damping_filter(diffusion, wave_count)

    sent = [
        analyse(grid_state, table_t, b, chunk, bands) for b in range(0, members, chunk)
    ]
    groups = lax.axis_size("grp")
    turned = legendre.transpose(1, 0, 2).reshape(bands, local_waves * lat_rows, wave_count)
    share = local_waves * lat_rows // groups
    own = lax.dynamic_slice_in_dim(turned, lax.axis_index("grp") * share, share, axis=1)
    basis = lax.all_gather(exchange(own), "grp", axis=1, tiled=True)
    basis = basis.reshape(bands, local_waves, lat_rows, wave_count).transpose(1, 0, 2, 3)
    basis = basis.reshape(local_waves, bands * lat_rows, wave_count)
    zonal_ids = lax.axis_index("lat") * local_waves + jnp.arange(local_waves, dtype=jnp.int32)
    total_ids = jnp.arange(wave_count, dtype=jnp.int32)
    triangle = total_ids[None, :] >= zonal_ids[:, None]
    basis = jnp.where(triangle[:, None], basis, jnp.zeros_like(basis))
    flipped = basis.transpose(0, 2, 1)
    received = [exchange(s) for s in sent]
    banded = [spectral(r, basis, flipped, damping, parts) for r in received]

    first = jnp.concatenate([input_weight, noise_weight], axis=0)
    new_state = None
    moments = []
    for q in range(parts):
        fields = [exchange(g[q]) for g in banded]
        if moments:
            fields, moments[-1] = lax.optimization_barrier((fields, moments[-1]))
        new_state, stats = physics(
            fields, noise_field, table, first, input_bias[None], middle_weight,
            output_weight, q, new_state,
        )
        moments.append(ensemble_moments(pair_moments(stats, members), members))
    joined = [jnp.concatenate([low, high], axis=2) for low, high in moments]
    ens_mean = jnp.concatenate([j[0] for j in joined], axis=0).astype(F32)
    ens_var = jnp.concatenate([j[1] for j in joined], axis=0).astype(F32)
    return (new_state, ens_mean, ens_var)


GROUP = 8


def slot_table(lon_count, wave_count, share, lane_y, lanes):
    offset = jnp.arange(lanes, dtype=jnp.int32)[:, None, None, None]
    p = jnp.arange(2, dtype=jnp.int32)[None, :, None, None]
    part = jnp.arange(2, dtype=jnp.int32)[None, None, :, None]
    unit = (lane_y - offset) % lanes * share + jnp.arange(share, dtype=jnp.int32)[None, None, None, :]
    wave = jnp.where(p == 0, unit, wave_count - unit)
    wave = jnp.where(unit == 0, jnp.where(part == 0, 0, wave_count // 2), wave)
    wave, unit, p, part = jnp.broadcast_arrays(wave, unit, p, part)
    quarter = jnp.where(unit == 0, p, part) * lon_count
    lon_ids = jnp.arange(lon_count, dtype=jnp.int32)
    turn = (4 * (wave.reshape(-1, 1) * lon_ids[None, :]) + quarter.reshape(-1, 1)) % (4 * lon_count)
    phase = turn.astype(F32) * (0.5 * math.pi / lon_count)
    return (jnp.cos(phase) * math.sqrt(2.0 / lon_count)).astype(BF16)


WAIT = pl.BlockSpec(memory_space=pl.ANY)
MESH = pl.DeviceIdType.MESH


def pipeline_body(lanes, far, cuts, grid_ref, noise_ref, table_t_ref, turned_ref, diffusion_ref, first_ref, bias_ref,
                  middle_ref, last_ref, state_ref, table_out, *rest):
    fields = rest[:lanes]
    (kept, sent, own, other, back, blocks_ref, basis, flipped, table_ref, damping, rows_in, noise_in,
     rows_out) = rest[lanes:lanes + 13]
    rest = rest[lanes + 13:]
    scratch = rest[:2 * lanes]
    (row_sem, noise_sem, out_sem, field_sem, table_sem, basis_send, basis_recv, kept_send, kept_recv, own_send, own_recv, back_send,
     back_recv) = rest[2 * lanes:]
    members, lat_rows, _, channels = grid_ref.shape
    blocks, share, depth = kept.shape[1:4]
    slots, per, totals, _ = own.shape
    ahead = slots // 2
    wave_count = turned_ref.shape[0]
    pieces = per // 2
    groups = lat_rows // GROUP
    rows = 2 * GROUP
    pitch = scratch[0].shape[0] // share
    chunks = members * cuts
    index, team = lax.axis_index("lat"), lax.axis_index("grp")
    place, lane = index // lanes, index % lanes
    half = place // far
    dist = (1 - half) * (far - 1 - place) + half * (place - far)
    hub_place = far - 1 + half
    opposite = (far - half) * lanes + lane
    core = team % 2
    partner = team + 1 - 2 * core
    hub, leaf = dist == 0, dist > 0
    start = lane * share
    ranges = [pl.ds(q * per, per) for q in range(cuts)]

    def remote(src, dst, send, recv, **target):
        return pltpu.make_async_remote_copy(
            src_ref=src, dst_ref=dst, send_sem=send, recv_sem=recv, device_id=target, device_id_type=MESH
        )

    def hub_lane(dy):
        return hub_place * lanes + (lane + lanes - dy) % lanes

    def source_lane(k):
        return (hub_place + (2 * half - 1) * (k // lanes)) * lanes + (lane + k % lanes) % lanes

    def span(q):
        return (0, pieces + 1) if q == 0 else (pieces * q + 1, pieces)

    def spot(q, j):
        return j // pieces, pieces * q + (q + cuts - 1) // cuts + j % pieces

    def basis_copy(q, dy):
        low, size = span(q)
        at = pl.multiple_of((dist * lanes + dy) * depth, depth)
        return remote(
            blocks_ref.at[dy, pl.ds(low, size)], basis.at[core, pl.ds(low, size), pl.ds(at, depth)],
            basis_send.at[q, dy], basis_recv.at[q, dist * lanes + dy], lat=hub_lane(dy),
        )

    def basis_own(q):
        low, size = span(q)
        return pltpu.make_async_copy(
            blocks_ref.at[0, pl.ds(low, size)], basis.at[core, pl.ds(low, size), pl.ds(0, depth)],
            basis_recv.at[q, 0],
        )

    def send_basis(q):
        for dy in range(1, lanes):
            basis_copy(q, dy).start()

        @pl.when(leaf)
        def _():
            basis_copy(q, 0).start()

        @pl.when(hub)
        def _():
            basis_own(q).start()

    def arrange(q):
        row = lax.broadcasted_iota(jnp.int32, (lat_rows, totals), 1)
        flip = lax.broadcasted_iota(jnp.int32, (totals, totals), 0)
        flip = flip + lax.broadcasted_iota(jnp.int32, (totals, totals), 1) == totals - 1
        flip = flip.astype(F32).astype(BF16)
        low, size = span(q)
        for dy in range(lanes):
            turn = (lane + lanes - dy) % lanes
            for e in range(size):
                unit = turn * share + q * per + core * pieces + e
                if e == pieces:
                    unit = turn * share + wave_count // 2 * (1 - (turn + lanes - 1) // lanes)
                near = turned_ref[unit].astype(F32)
                mirrored = jnp.dot(
                    turned_ref[(wave_count - unit) % wave_count], flip, preferred_element_type=F32
                )
                near = jnp.where(row >= unit, near, 0.0).reshape(groups, 1, GROUP, totals)
                mirrored = jnp.where(row < unit, mirrored, 0.0).reshape(groups, 1, GROUP, totals)
                both = jnp.concatenate([near, mirrored], axis=1).reshape(depth, totals)
                blocks_ref[dy, low + e] = both.astype(BF16)

    def basis_swap(q, low, size):
        part = basis.at[core, pl.ds(low, size)]
        return remote(part, part, basis_send.at[q, lanes], basis_recv.at[q, blocks], grp=partner)

    def basis_ready(q, low, size):
        pltpu.make_async_copy(
            blocks_ref.at[0, pl.ds(low, size)], basis.at[core, pl.ds(low, size), pl.ds(0, depth)],
            basis_recv.at[q, 0],
        ).wait()
        for k in range(1, blocks):
            part = basis.at[core, pl.ds(low, size), pl.ds(k * depth, depth)]
            remote(part, part, basis_send.at[q, 0], basis_recv.at[q, k], lat=opposite).wait_recv()
        basis_swap(q, low, size).start()
        basis_swap(q, low, size).wait_recv()
        for side in range(2):
            for e in range(size):
                flipped[side, low + e] = basis[side, low + e].T

    def lane_copy(b, q, dy):
        return remote(
            sent.at[b, dy - 1, ranges[q]], kept.at[b, dy, ranges[q]], kept_send.at[b, q, dy - 1],
            kept_recv.at[b, q, dy], lat=place * lanes + (lane + lanes - dy) % lanes,
        )

    def kept_copy(b, q, dy):
        k = dist * lanes + dy
        return remote(
            kept.at[b, dy, ranges[q]], kept.at[b, k, ranges[q]], kept_send.at[b, q, lanes - 1 + dy],
            kept_recv.at[b, q, k], lat=hub_lane(0),
        )

    def kept_arrival(b, q, k):
        part = kept.at[b, k, pl.ds(q * per, per)]
        return remote(part, part, kept_send.at[b, q, 0], kept_recv.at[b, q, k], lat=opposite)

    def own_copy(c):
        return remote(own.at[c % slots], other.at[c], own_send.at[c], own_recv.at[c], lat=opposite)

    def back_copy(b, q, k):
        units = pl.ds(q * per, per)
        return remote(
            kept.at[b, k, units], back.at[b, k % lanes, units], back_send.at[b, q, k - 1],
            back_recv.at[b, q, k % lanes], lat=source_lane(k),
        )

    def back_arrival(b, q, dy):
        part = back.at[b, dy, pl.ds(q * per, per)]
        return remote(part, part, back_send.at[b, q, 0], back_recv.at[b, q, dy], lat=opposite)

    def load(ref, n):
        at = pl.multiple_of(n % groups * GROUP, GROUP)
        held, sem = (rows_in, row_sem) if ref is grid_ref else (noise_in, noise_sem)
        return pltpu.make_async_copy(ref.at[n // groups, pl.ds(at, GROUP)], held.at[n % 2], sem.at[n % 2])

    def store(n):
        at = pl.multiple_of(n % groups * GROUP, GROUP)
        return pltpu.make_async_copy(
            rows_out.at[n % 2], state_ref.at[n // groups, pl.ds(at, GROUP)], out_sem.at[n % 2]
        )

    def analyse_group(n, carry):
        b = n // groups
        at = pl.multiple_of(n % groups * rows, rows)

        @pl.when(n + 1 < members * groups)
        def _():
            load(grid_ref, n + 1).start()

        load(grid_ref, n).wait()
        for k in range(0, GROUP, 2):
            pair = jnp.concatenate([rows_in[n % 2, k], rows_in[n % 2, k + 1]], axis=1)
            waves = jnp.dot(table_t_ref[...], pair, preferred_element_type=F32)
            row = 0
            for dy in range(lanes):
                for p in range(2):
                    for part in range(2):
                        for t in range(2):
                            scratch[2 * dy + part][pl.ds(p * GROUP + k + t, share, stride=pitch), :] = (
                                waves[row:row + share, t * channels:(t + 1) * channels]
                            )
                        row += share
        for dy in range(lanes):
            for part in range(2):
                value = scratch[2 * dy + part][...].reshape(share, pitch, channels)[:, :rows].astype(BF16)
                side = slice(part * channels, (part + 1) * channels)
                if dy == 0:
                    kept[b, 0, :, pl.ds(at, rows), side] = value
                else:
                    sent[b, dy - 1, :, pl.ds(at, rows), side] = value
        return carry

    def partial(c):
        b, q = c // cuts, c % cuts

        @pl.when(c == 0)
        def _():
            basis_ready(0, 0, pieces + 1)

        @pl.when((c > 0) & (c < cuts))
        def _():
            basis_ready(c, pieces * c + 1, pieces)

        for k in range(1, blocks):
            kept_arrival(b, q, k).wait_recv()

        @pl.when(c >= slots)
        def _():
            own_copy(c - slots).wait_send()

        def unit(j, carry):
            values = jnp.concatenate([kept[b, k, q * per + j] for k in range(blocks)], axis=0)
            side, e = spot(q, j)
            sums = jnp.dot(flipped[side, e], values, preferred_element_type=F32)
            own[c % slots, j] = sums.astype(BF16)
            return carry

        for j in range(per):
            unit(j, 0)

        @pl.when(q == 0)
        def _():
            values = jnp.concatenate([kept[b, k, 0, :, channels:] for k in range(blocks)], axis=0)
            sums = jnp.dot(flipped[0, pieces], values, preferred_element_type=F32)
            own[c % slots, 0, :, channels:] = sums.astype(BF16)

        own_copy(c).start()

    def synthesise(c):
        b, q = c // cuts, c % cuts
        own_copy(c).wait_recv()
        row = lax.broadcasted_iota(jnp.int32, (totals, channels), 0)

        def damped(j, mark, side):
            total = own[c % slots, j, :, side].astype(F32) + other[c, j, :, side].astype(F32)
            return (total * jnp.where(row < mark, damping[1], damping[0])).astype(BF16)

        def put(i, grid, side):
            back[b, 0, i, :, side] = grid[:depth]
            for k in range(1, blocks):
                kept[b, k, i, :, side] = grid[k * depth:(k + 1) * depth]

        def unit(j, carry):
            mark = start + q * per + j
            value = jnp.concatenate(
                [damped(j, mark, slice(r * channels, (r + 1) * channels)) for r in range(2)], axis=1
            )
            at, e = spot(q, j)
            grid = jnp.dot(basis[at, e], value, preferred_element_type=F32).astype(BF16)
            put(q * per + j, grid, slice(None))
            return carry

        for j in range(per):
            unit(j, 0)

        @pl.when(q == 0)
        def _():
            mark = jnp.where(start == 0, totals // 2, start)
            side = slice(channels, 2 * channels)
            grid = jnp.dot(basis[0, pieces], damped(0, mark, side), preferred_element_type=F32).astype(BF16)
            put(0, grid, side)

        for k in range(1, blocks):
            back_copy(b, q, k).start()

    def column_group(b, g):
        n = b * groups + g
        at = pl.multiple_of(g * rows, rows)

        @pl.when(n + 1 < (members - 1) * groups)
        def _():
            load(noise_ref, n + 1).start()

        @pl.when(g == 0)
        def _():
            for q in range(cuts):
                for dy in range(lanes):
                    if dy > 0:
                        back_arrival(b, q, dy).wait_recv()
                    else:
                        @pl.when(leaf)
                        def _():
                            back_arrival(b, q, dy).wait_recv()

        for dy in range(lanes):
            for part in range(2):
                side = slice(part * channels, (part + 1) * channels)
                value = back[b, dy, :, pl.ds(at, rows), side].astype(F32)
                space = jnp.zeros((share, pitch - rows, channels), F32)
                scratch[2 * dy + part][...] = jnp.concatenate([value, space], axis=1).reshape(-1, channels)
        load(noise_ref, n).wait()

        @pl.when(n >= 2)
        def _():
            store(n - 2).wait()

        def pair(i, carry):
            waves = []
            for t in range(2):
                waves.append(jnp.concatenate([
                    scratch[2 * dy + part][pl.ds(p * GROUP + 2 * i + t, share, stride=pitch), :]
                    for dy in range(lanes) for p in range(2) for part in range(2)
                ], axis=0).astype(BF16))
            smoothed = jnp.dot(table_ref[...], jnp.concatenate(waves, axis=1), preferred_element_type=F32)
            for t in range(2):
                flat = smoothed[:, t * channels:(t + 1) * channels]
                joined = jnp.concatenate([flat.astype(BF16), noise_in[n % 2, 2 * i + t]], axis=1)
                pre = jnp.dot(joined, first_ref[...], preferred_element_type=F32)
                one = silu(pre + bias_ref[...]).astype(BF16)
                two = silu(jnp.dot(one, middle_ref[...], preferred_element_type=F32)).astype(BF16)
                tendency = jnp.dot(two, last_ref[...], preferred_element_type=F32)
                rows_out[n % 2, 2 * i + t] = (flat + tendency).astype(BF16)
            return carry

        lax.fori_loop(0, GROUP // 2, pair, 0)
        store(n).start()

    def analyse_member(b, first):
        lax.fori_loop(b * groups, (b + 1) * groups, analyse_group, 0)
        for q in range(cuts):
            for dy in range(1, lanes):
                lane_copy(b, q, dy).start()
            if first and q == 0:
                for later in range(1, cuts):
                    arrange(later)
            if first and q + 1 < cuts:
                @pl.when(hub)
                def _():
                    send_basis(q + 1)

        @pl.when(leaf)
        def _():
            kept_copy(b, 0, 0).start()
            for q in range(cuts):
                for dy in range(1, lanes):
                    kept_arrival(b, q, dy).wait_recv()
                    kept_copy(b, q, dy).start()
                if q + 1 < cuts:
                    if first:
                        send_basis(q + 1)
                    kept_copy(b, q + 1, 0).start()

    load(grid_ref, 0).start()
    load(noise_ref, 0).start()
    arrange(0)
    send_basis(0)
    analyse_member(0, True)
    table_ref[...] = table_t_ref[...].T
    degree = lax.broadcasted_iota(jnp.int32, (totals, channels), 0)
    for side in range(2):
        n = (degree if side == 0 else totals - 1 - degree).astype(F32)
        ratio = n * (n + 1.0) / float((totals - 1) * totals)
        damping[side] = 1.0 / (1.0 + diffusion_ref[...] * (ratio * ratio))
    table_copy = pltpu.make_async_copy(table_ref, table_out, table_sem)
    table_copy.start()

    def tick(t, carry):
        @pl.when(hub)
        def _():
            @pl.when(t < chunks)
            def _():
                partial(t)

            @pl.when(t >= ahead)
            def _():
                synthesise(t - ahead)

        soon = t // cuts + 1

        @pl.when((t % cuts == 1) & (soon < members))
        def _():
            analyse_member(soon, False)

        late = t - cuts - ahead - 1
        g = (late + 2 * cuts) % cuts

        @pl.when((late >= 0) & (g < groups))
        def _():
            column_group(late // cuts, g)

        return carry

    lax.fori_loop(0, chunks + ahead, tick, 0)

    last = members - 1
    for q in range(cuts):
        for dy in range(lanes):
            if dy > 0:
                back_arrival(last, q, dy).wait_recv()
            else:
                @pl.when(leaf)
                def _():
                    back_arrival(last, q, dy).wait_recv()
    finals = [
        pltpu.make_async_copy(back.at[last, dy], fields[dy].at[0], field_sem.at[dy]) for dy in range(lanes)
    ]
    for dy in range(1, lanes):
        finals[dy].start()
    finals[0].start()
    for n in ((members - 1) * groups - 2, (members - 1) * groups - 1):
        store(n).wait()

    def drain(b, carry):
        for q in range(cuts):
            for dy in range(1, lanes):
                lane_copy(b, q, dy).wait_send()

            @pl.when(leaf)
            def _():
                for dy in range(lanes):
                    kept_copy(b, q, dy).wait_send()

            @pl.when(hub)
            def _():
                for k in range(1, blocks):
                    back_copy(b, q, k).wait_send()
        return carry

    lax.fori_loop(0, members, drain, 0)

    @pl.when(hub)
    def _():
        for q in range(cuts):
            basis_swap(q, *span(q)).wait_send()
        for c in range(chunks - slots, chunks):
            own_copy(c).wait_send()

    @pl.when(leaf)
    def _():
        for q in range(cuts):
            basis_copy(q, 0).wait_send()

    for q in range(cuts):
        for dy in range(1, lanes):
            basis_copy(q, dy).wait_send()
    table_copy.wait()
    for final in finals:
        final.wait()


def pipeline(lanes, far, cuts, grid_state, noise, table_t, turned, diffusion, first, bias, middle, output):
    members, lat_rows, lon_count, channels = grid_state.shape
    wave_count = turned.shape[0]
    share = wave_count // 2 // lanes
    entries = share // 2 + 1
    depth = 2 * lat_rows
    count = far * lanes
    per = share // cuts
    slots = 6
    vmem = pl.BlockSpec(memory_space=pltpu.VMEM)
    dma = pltpu.SemaphoreType.DMA
    return pl.pallas_call(
        functools.partial(pipeline_body, lanes, far, cuts),
        in_specs=[WAIT, WAIT, vmem, vmem, vmem, vmem, vmem, vmem, vmem],
        out_specs=[WAIT] * (2 + lanes),
        out_shape=[
            jax.ShapeDtypeStruct((members - 1, *grid_state.shape[1:]), BF16),
            jax.ShapeDtypeStruct((lon_count, table_t.shape[0]), BF16),
        ] + [jax.ShapeDtypeStruct((1, share, depth, 2 * channels), BF16)] * lanes,
        scratch_shapes=[
            pltpu.VMEM((members, count, share, depth, 2 * channels), BF16),
            pltpu.VMEM((members, lanes - 1, share, depth, 2 * channels), BF16),
            pltpu.VMEM((slots, per, wave_count, 2 * channels), BF16),
            pltpu.VMEM((members * cuts, per, wave_count, 2 * channels), BF16),
            pltpu.VMEM((members, lanes, share, depth, 2 * channels), BF16),
            pltpu.VMEM((lanes, entries, depth, wave_count), BF16),
            pltpu.VMEM((2, entries, count * depth, wave_count), BF16),
            pltpu.VMEM((2, entries, wave_count, count * depth), BF16),
            pltpu.VMEM((lon_count, table_t.shape[0]), BF16),
            pltpu.VMEM((2, wave_count, channels), F32),
        ] + [pltpu.VMEM((2, GROUP, lon_count, channels), BF16)] * 3 + [pltpu.VMEM((share * 3 * GROUP, channels), F32)] * (2 * lanes) + [
            dma((2,)),
            dma((2,)),
            dma((2,)),
            dma((lanes,)),
            dma,
            dma((cuts, lanes + 1)),
            dma((cuts, count + 1)),
            dma((members, cuts, 2 * lanes - 1)),
            dma((members, cuts, count)),
            dma((members * cuts,)),
            dma((members * cuts,)),
            dma((members, cuts, count - 1)),
            dma((members, cuts, lanes)),
        ],
        compiler_params=pltpu.CompilerParams(
            has_side_effects=True, vmem_limit_bytes=64000 * 1024
        ),
    )(grid_state, noise, table_t, turned, diffusion, first, bias, middle, output)


def last_body(lanes, *refs):
    core_ref, fields = refs[0], refs[1:1 + lanes]
    noise_ref, table_ref, first_ref, bias_ref, middle_ref, last_ref, held_ref = refs[1 + lanes:8 + lanes]
    state_ref, mine_ref, give_ref = refs[-2 * lanes - 3:-2 * lanes]
    scratch = refs[-2 * lanes:]
    members, lats, lon_count, channels = state_ref.shape
    _, share, rows, _ = fields[0].shape
    pitch = scratch[0].shape[0] // share
    inner = pl.program_id(0)

    @pl.when(inner == 0)
    def _():
        for dy in range(lanes):
            for part in range(2):
                value = fields[dy][0, :, :, part * channels:(part + 1) * channels].astype(F32)
                space = jnp.zeros((share, pitch - rows, channels), F32)
                scratch[2 * dy + part][...] = jnp.concatenate([value, space], axis=1).reshape(-1, channels)

    waves = []
    for k in range(lats):
        at = inner * lats + k
        waves.append(jnp.concatenate([
            scratch[2 * dy + part][pl.ds(p * rows // 2 + at, share, stride=pitch), :]
            for dy in range(lanes) for p in range(2) for part in range(2)
        ], axis=0).astype(BF16))
    smoothed = jnp.dot(table_ref[...], jnp.concatenate(waves, axis=1), preferred_element_type=F32)
    half = lon_count // 2
    for k in range(lats):
        flat = smoothed[:, k * channels:(k + 1) * channels]
        joined = jnp.concatenate([flat.astype(BF16), noise_ref[0, k]], axis=1)
        pre = jnp.dot(joined, first_ref[...], preferred_element_type=F32)
        one = silu(pre + bias_ref[...]).astype(BF16)
        two = silu(jnp.dot(one, middle_ref[...], preferred_element_type=F32)).astype(BF16)
        tendency = jnp.dot(two, last_ref[...], preferred_element_type=F32)
        state = (flat + tendency).astype(BF16)
        for b in range(members - 1):
            state_ref[b, k] = held_ref[b, k]
        state_ref[members - 1, k] = state
        values = [held_ref[b, k].astype(F32) for b in range(members - 1)] + [state.astype(F32)]
        total = functools.reduce(jnp.add, values)
        mean = total * (1.0 / members)
        spread = functools.reduce(jnp.add, [jnp.square(v - mean) for v in values])
        sums = [total.astype(BF16), spread.astype(BF16)]
        for h in range(2):
            @pl.when(core_ref[0] == h)
            def _():
                for j in range(2):
                    mine_ref[j, k] = sums[j][h * half:(h + 1) * half]
                    give_ref[j, k] = sums[j][(1 - h) * half:(2 - h) * half]


def last_columns(fields, core, noise, table, first, bias, middle, output, states, part, previous, after):
    lanes = len(fields)
    members, _, lon_count, channels = noise.shape
    _, share, _, width = fields[0].shape
    rows = 2 * GROUP
    lats = 2
    inner = GROUP // lats
    half = lon_count // 2
    whole = lambda a: pl.BlockSpec(a.shape, lambda i: (0,) * a.ndim)
    params = [table, first, bias, middle, output]
    operands = [core, *fields, noise, *params, states]
    specs = [pl.BlockSpec(memory_space=pltpu.SMEM)]
    specs += [pl.BlockSpec((1, share, rows, width), lambda i: (0, 0, part, 0))] * lanes
    specs.append(pl.BlockSpec(
        (1, lats, lon_count, channels), lambda i: (members - 1, part * inner + i, 0, 0)
    ))
    specs += [whole(a) for a in params]
    specs.append(pl.BlockSpec(
        (members - 1, lats, lon_count, channels), lambda i: (0, part * inner + i, 0, 0)
    ))
    aliases = {}
    if previous is not None:
        aliases = {len(operands): 0}
        operands.append(previous)
    operands += after
    specs += [WAIT] * (len(operands) - len(specs))
    points = GROUP * lon_count
    hidden = middle.shape[0]
    return pl.pallas_call(
        functools.partial(last_body, lanes),
        grid=(inner,),
        in_specs=specs,
        out_specs=[
            pl.BlockSpec((members, lats, lon_count, channels), lambda i: (0, part * inner + i, 0, 0))
        ] + [pl.BlockSpec((2, lats, half, channels), lambda i: (0, i, 0, 0))] * 2,
        out_shape=[
            jax.ShapeDtypeStruct(noise.shape, BF16)
        ] + [jax.ShapeDtypeStruct((2, GROUP, half, channels), BF16)] * 2,
        input_output_aliases=aliases,
        scratch_shapes=[pltpu.VMEM((share * 3 * GROUP, channels), F32)] * (2 * lanes),
        cost_estimate=pl.CostEstimate(
            flops=2 * points * (first.size + middle.size + output.size + 256 * channels),
            bytes_accessed=16 * points * channels,
            transcendentals=2 * points * hidden,
        ),
    )(*operands)


def blend_body(count, scales, one_ref, two_ref, out_ref):
    total, spread = join(one_ref[...], two_ref[...], count)
    out_ref[0] = (total * scales[0]).astype(BF16)
    out_ref[1] = (spread * scales[1]).astype(BF16)


def blend(one, two, count, scales):
    _, group, half, channels = one.shape
    block = pl.BlockSpec((2, 4, half, channels), lambda i: (0, i, 0, 0))
    return pl.pallas_call(
        functools.partial(blend_body, count, scales),
        grid=(group // 4,),
        in_specs=[block, block],
        out_specs=block,
        out_shape=jax.ShapeDtypeStruct(one.shape, BF16),
        cost_estimate=pl.CostEstimate(
            flops=4 * one.size, bytes_accessed=6 * one.size, transcendentals=0
        ),
    )(one, two)


def place_body(core_ref, mine_ref, partner_ref, *refs):
    outs = refs[-2:]
    half = mine_ref.shape[2]
    for h in range(2):
        @pl.when(core_ref[0] == h)
        def _():
            for j in range(2):
                outs[j][:, h * half:(h + 1) * half] = mine_ref[j].astype(F32)
                outs[j][:, (1 - h) * half:(2 - h) * half] = partner_ref[j].astype(F32)


def place_moments(core, mine, partner, part, lat_rows, previous):
    _, group, half, channels = mine.shape
    shape = (lat_rows, 2 * half, channels)
    block = pl.BlockSpec((2, 4, half, channels), lambda i: (0, i, 0, 0))
    return pl.pallas_call(
        place_body,
        grid=(group // 4,),
        in_specs=[pl.BlockSpec(memory_space=pltpu.SMEM), block, block] + [WAIT] * len(previous),
        out_specs=[
            pl.BlockSpec((4, 2 * half, channels), lambda i: (part * (group // 4) + i, 0, 0))
        ] * 2,
        out_shape=[jax.ShapeDtypeStruct(shape, F32)] * 2,
        input_output_aliases={3 + j: j for j in range(len(previous))},
        cost_estimate=pl.CostEstimate(
            flops=4 * mine.size, bytes_accessed=16 * mine.size, transcendentals=0
        ),
    )(core, mine, partner, *previous)


def hub_plan(
    lanes,
    grid_state,
    noise_field,
    legendre,
    diffusion,
    input_weight,
    noise_weight,
    input_bias,
    middle_weight,
    output_weight,
):
    members, lat_rows, lon_count, _ = grid_state.shape
    wave_count = legendre.shape[1]
    far = lax.axis_size("lat") // lanes // 2
    share = wave_count // 2 // lanes
    parts = lat_rows // GROUP
    cuts = 8
    lane = lax.axis_index("lat") % lanes
    core = lax.axis_index("grp") % 2
    table_t = slot_table(lon_count, wave_count, share, lane, lanes)
    first = jnp.concatenate([input_weight, noise_weight], axis=0)
    params = (first, input_bias[None], middle_weight, output_weight)
    turned = legendre.transpose(1, 0, 2)
    states, table, *fields = pipeline(
        lanes, far, cuts, grid_state, noise_field, table_t, turned, diffusion[None], *params
    )
    groups = lax.axis_size("grp")
    flag = core[None].astype(jnp.int32)
    new_state, after, placed = None, [], []
    for q in range(parts):
        new_state, mine, give = last_columns(
            fields, flag, noise_field, table, *params, states, q, new_state, after
        )
        held = blend(mine, swap(give, 1), members, (1.0, 1.0))
        after = [held]
        bit, count = 2, 2 * members
        while bit < groups:
            other = swap(held, bit)
            final = 2 * bit >= groups
            scales = (0.5 / count, 1.0 / (2 * count - 1)) if final else (1.0, 1.0)
            held = blend(held, other, count, scales)
            bit, count = 2 * bit, 2 * count
        partner = swap(held, 1)
        placed = place_moments(flag, held, partner, q, lat_rows, placed)
    return (new_state, *placed)


def lane_count(mesh):
    line = [getattr(d, "coords", None) for d in mesh.devices.reshape(-1, mesh.shape["lat"])[0]]
    if len(line) < 2 or line[0] is None:
        return 2
    axis = [a != b for a, b in zip(line[0], line[1])].index(True)
    return len({c[axis] for c in line})


def per_device(lanes, *args):
    grid_state, legendre = args[0], args[2]
    members, lat_rows = grid_state.shape[:2]
    units = legendre.shape[1] // 2
    fits = (
        lax.axis_size("lat") % (2 * lanes) == 0
        and units % (16 * lanes) == 0
        and lat_rows % GROUP == 0
        and lat_rows // GROUP < 7
        and members > 1
        and lax.axis_size("grp") > 2
    )
    return hub_plan(lanes, *args) if fits else direct_plan(*args)


def solution(mesh):
    in_specs = (
        P("grp", "lat", None, None),
        P("grp", "lat", None, None),
        P("lat", None, None),
        P(),
        P(),
        P(),
        P(),
        P(),
        P(),
    )
    out_specs = (P("grp", "lat", None, None), P("lat", None, None), P("lat", None, None))

    def body(*args):
        return per_device(lane_count(mesh), *args)

    return jax.shard_map(
        body, mesh=mesh, in_specs=in_specs, out_specs=out_specs, check_vma=False
    )
```

```python
import functools
import math

import jax
import jax.numpy as jnp
from jax import lax
from jax.experimental import pallas as pl
from jax.experimental.pallas import tpu as pltpu
from jax.sharding import PartitionSpec as P


BF16 = jnp.bfloat16
F32 = jnp.float32


def wave_table(lon_count, wave_count):
    lon_ids = jnp.arange(lon_count, dtype=jnp.int32)[:, None]
    wave_ids = jnp.arange(wave_count, dtype=jnp.int32)[None, :]
    phase = (lon_ids * wave_ids % lon_count).astype(jnp.float32) * (2.0 * math.pi / lon_count)
    factor = math.sqrt(2.0 / lon_count)
    joined = jnp.concatenate([jnp.cos(phase), -jnp.sin(phase)], axis=1) * factor
    return joined.astype(jnp.bfloat16)


def damping_filter(diffusion, wave_count):
    degree = jnp.arange(wave_count, dtype=jnp.int32).astype(jnp.float32)
    ratio = degree * (degree + 1.0) / float((wave_count - 1) * wave_count)
    return 1.0 / (1.0 + diffusion[None, :] * (ratio * ratio)[:, None])


def analysis_body(table_ref, grid_ref, out_ref):
    bands, _, rows, width, channels = out_ref.shape
    for row in range(0, rows, 2):
        pair = jnp.concatenate([grid_ref[0, row], grid_ref[0, row + 1]], axis=1)
        waves = jnp.dot(table_ref[...], pair, preferred_element_type=F32).astype(BF16)
        for k in range(2):
            out_ref[:, 0, row + k] = waves[:, k * channels:(k + 1) * channels].reshape(
                bands, width, channels
            )


def analyse(grid_state, table, first, count, bands):
    _, lat_rows, lon_count, channels = grid_state.shape
    width = table.shape[0] // bands
    rows = 6
    return pl.pallas_call(
        analysis_body,
        grid=(count, lat_rows // rows),
        in_specs=[
            pl.BlockSpec(table.shape, lambda b, i: (0, 0)),
            pl.BlockSpec((1, rows, lon_count, channels), lambda b, i: (b + first, i, 0, 0)),
        ],
        out_specs=pl.BlockSpec((bands, 1, rows, width, channels), lambda b, i: (0, b, i, 0, 0)),
        out_shape=jax.ShapeDtypeStruct((bands, count, lat_rows, width, channels), BF16),
        cost_estimate=pl.CostEstimate(
            flops=2 * count * lat_rows * lon_count * channels * table.shape[0],
            bytes_accessed=4 * count * lat_rows * lon_count * channels,
            transcendentals=0,
        ),
    )(table, grid_state)


def spectral_body(parts, in_ref, basis_ref, flipped_ref, damping_ref, *rest):
    outs, (fin, fout) = rest[:parts], rest[parts:]
    bands, _, lat_rows, width, channels = in_ref.shape
    waves = basis_ref.shape[0]
    lats = bands * lat_rows
    span = lat_rows * width
    for s in range(bands):
        fin[pl.ds(s * span, span), :] = in_ref[s, 0].astype(F32).reshape(span, channels)
    damping = jnp.concatenate([damping_ref[...]] * 2, axis=1)
    for m in range(waves):
        values = jnp.concatenate(
            [fin[pl.ds(r * waves + m, lats, stride=width), :] for r in range(2)], axis=1
        ).astype(BF16)
        spectrum = jnp.dot(flipped_ref[m], values, preferred_element_type=F32)
        filtered = (spectrum * damping).astype(BF16)
        grid = jnp.dot(basis_ref[m], filtered, preferred_element_type=F32)
        for r in range(2):
            fout[pl.ds(r * waves + m, lats, stride=width), :] = grid[
                :, r * channels:(r + 1) * channels
            ]
    part_rows = lat_rows // parts
    for q in range(parts):
        for s in range(bands):
            start = (s * lat_rows + q * part_rows) * width
            outs[q][s, 0] = (
                fout[pl.ds(start, part_rows * width), :]
                .reshape(part_rows, width, channels)
                .astype(BF16)
            )


def spectral(received, basis, flipped, damping, parts):
    bands, count, lat_rows, width, channels = received.shape
    part_rows = lat_rows // parts
    whole = lambda a: pl.BlockSpec(a.shape, lambda b: (0,) * a.ndim)
    return pl.pallas_call(
        functools.partial(spectral_body, parts),
        grid=(count,),
        in_specs=[
            pl.BlockSpec((bands, 1, lat_rows, width, channels), lambda b: (0, b, 0, 0, 0)),
            whole(basis),
            whole(flipped),
            whole(damping),
        ],
        out_specs=[
            pl.BlockSpec((bands, 1, part_rows, width, channels), lambda b: (0, b, 0, 0, 0))
        ] * parts,
        out_shape=[
            jax.ShapeDtypeStruct((bands, count, part_rows, width, channels), BF16)
        ] * parts,
        scratch_shapes=[pltpu.VMEM((bands * lat_rows * width, channels), F32)] * 2,
        cost_estimate=pl.CostEstimate(
            flops=8 * count * basis.size * channels,
            bytes_accessed=4 * received.size,
            transcendentals=0,
        ),
    )(received, basis, flipped, damping)


def silu(value):
    half = 0.5 * value
    return half + half * jnp.tanh(half)


def physics_body(groups, *refs):
    fields = refs[:groups]
    noise_ref, table_ref, first_ref, bias_ref, middle_ref, last_ref = refs[groups:groups + 6]
    state_ref, stats_ref = refs[-2:]
    members, _, lon_count, channels = noise_ref.shape
    states = []
    for ref in fields:
        count = ref.shape[1]
        waves = jnp.concatenate(
            [ref[:, k, 0].reshape(-1, channels) for k in range(count)], axis=1
        )
        smoothed = jnp.dot(table_ref[...], waves, preferred_element_type=F32)
        for k in range(count):
            flat = smoothed[:, k * channels:(k + 1) * channels]
            b = len(states)
            joined = jnp.concatenate([flat.astype(BF16), noise_ref[b, 0]], axis=1)
            pre = jnp.dot(joined, first_ref[...], preferred_element_type=F32)
            one = silu(pre + bias_ref[...]).astype(BF16)
            two = silu(jnp.dot(one, middle_ref[...], preferred_element_type=F32)).astype(BF16)
            tendency = jnp.dot(two, last_ref[...], preferred_element_type=F32)
            state = (flat + tendency).astype(BF16)
            state_ref[b, 0] = state
            states.append(state)
    values = [s.astype(F32) for s in states]
    total = functools.reduce(jnp.add, values)
    mean = total * (1.0 / members)
    spread = functools.reduce(jnp.add, [jnp.square(v - mean) for v in values])
    half = lon_count // 2
    for h in range(2):
        stats_ref[h, 0, 0] = total[h * half:(h + 1) * half].astype(BF16)
        stats_ref[h, 1, 0] = spread[h * half:(h + 1) * half].astype(BF16)


def physics(fields, noise, table, first, bias, middle, last, part, previous):
    bands, _, part_rows, width, channels = fields[0].shape
    members, lat_rows, lon_count, noise_channels = noise.shape
    whole = lambda a: pl.BlockSpec(a.shape, lambda i: (0,) * a.ndim)
    at = part * part_rows
    specs = [
        pl.BlockSpec((bands, f.shape[1], 1, width, channels), lambda i: (0, 0, i, 0, 0))
        for f in fields
    ]
    specs.append(
        pl.BlockSpec((members, 1, lon_count, noise_channels), lambda i: (0, i + at, 0, 0))
    )
    params = [table, first, bias, middle, last]
    specs += [whole(a) for a in params]
    operands = [*fields, noise, *params]
    aliases = {}
    if previous is not None:
        aliases = {len(operands): 0}
        operands.append(previous)
        specs.append(pl.BlockSpec(memory_space=pl.ANY))
    columns = members * part_rows * lon_count
    hidden = middle.shape[0]
    return pl.pallas_call(
        functools.partial(physics_body, len(fields)),
        grid=(part_rows,),
        in_specs=specs,
        out_specs=[
            pl.BlockSpec((members, 1, lon_count, channels), lambda i: (0, i + at, 0, 0)),
            pl.BlockSpec((2, 2, 1, lon_count // 2, channels), lambda i: (0, 0, i, 0, 0)),
        ],
        out_shape=[
            jax.ShapeDtypeStruct((members, lat_rows, lon_count, channels), BF16),
            jax.ShapeDtypeStruct((2, 2, part_rows, lon_count // 2, channels), BF16),
        ],
        input_output_aliases=aliases,
        cost_estimate=pl.CostEstimate(
            flops=2 * columns * (first.size + middle.size + last.size + 256 * channels),
            bytes_accessed=8 * columns * channels,
            transcendentals=2 * columns * hidden,
        ),
    )(*operands)


def swap(value, bit):
    groups = lax.axis_size("grp")
    return lax.ppermute(value, "grp", [(g, g ^ bit) for g in range(groups)])


def join(a, b, count):
    a, b = [v.astype(F32) for v in a], [v.astype(F32) for v in b]
    total = a[0] + b[0]
    spread = (a[1] + b[1]) + jnp.square(a[0] - b[0]) * (0.5 / count)
    return total, spread


def pair_moments(stats, members):
    core = lax.axis_index("grp") % 2
    own = lax.dynamic_index_in_dim(stats, core, 0, keepdims=False)
    other = lax.dynamic_index_in_dim(stats, 1 - core, 0, keepdims=False)
    return jnp.stack(join(own, swap(other, 1), members)).astype(BF16)


def ensemble_moments(held, members):
    groups = lax.axis_size("grp")
    core = lax.axis_index("grp") % 2
    bit, count = 2, 2 * members
    while bit < groups:
        held = jnp.stack(join(held.astype(BF16), swap(held.astype(BF16), bit), count))
        bit, count = 2 * bit, 2 * count
    scale = jnp.array([1.0 / count, 1.0 / (count - 1)], F32)
    held = (held * scale[:, None, None, None]).astype(BF16)
    partner = swap(held, 1)
    low = jnp.where(core == 0, held, partner)
    high = jnp.where(core == 0, partner, held)
    return low, high


def direct_plan(
    grid_state,
    noise_field,
    legendre,
    diffusion,
    input_weight,
    noise_weight,
    input_bias,
    middle_weight,
    output_weight,
):
    members, lat_rows, lon_count, _ = grid_state.shape
    wave_count = legendre.shape[1]
    bands = lax.axis_size("lat")
    local_waves = wave_count // bands
    chunk = 2
    parts = 2
    transform = wave_table(lon_count, wave_count)
    table = (
        transform.reshape(lon_count, 2, bands, local_waves)
        .transpose(0, 2, 1, 3)
        .reshape(lon_count, 2 * wave_count)
    )
    table_t = table.T
    exchange = lambda v: lax.all_to_all(v, "lat", split_axis=0, concat_axis=0, tiled=True)
    damping = damping_filter(diffusion, wave_count)

    sent = [
        analyse(grid_state, table_t, b, chunk, bands) for b in range(0, members, chunk)
    ]
    groups = lax.axis_size("grp")
    turned = legendre.transpose(1, 0, 2).reshape(bands, local_waves * lat_rows, wave_count)
    share = local_waves * lat_rows // groups
    own = lax.dynamic_slice_in_dim(turned, lax.axis_index("grp") * share, share, axis=1)
    basis = lax.all_gather(exchange(own), "grp", axis=1, tiled=True)
    basis = basis.reshape(bands, local_waves, lat_rows, wave_count).transpose(1, 0, 2, 3)
    basis = basis.reshape(local_waves, bands * lat_rows, wave_count)
    zonal_ids = lax.axis_index("lat") * local_waves + jnp.arange(local_waves, dtype=jnp.int32)
    total_ids = jnp.arange(wave_count, dtype=jnp.int32)
    triangle = total_ids[None, :] >= zonal_ids[:, None]
    basis = jnp.where(triangle[:, None], basis, jnp.zeros_like(basis))
    flipped = basis.transpose(0, 2, 1)
    received = [exchange(s) for s in sent]
    banded = [spectral(r, basis, flipped, damping, parts) for r in received]

    first = jnp.concatenate([input_weight, noise_weight], axis=0)
    new_state = None
    moments = []
    for q in range(parts):
        fields = [exchange(g[q]) for g in banded]
        if moments:
            fields, moments[-1] = lax.optimization_barrier((fields, moments[-1]))
        new_state, stats = physics(
            fields, noise_field, table, first, input_bias[None], middle_weight,
            output_weight, q, new_state,
        )
        moments.append(ensemble_moments(pair_moments(stats, members), members))
    joined = [jnp.concatenate([low, high], axis=2) for low, high in moments]
    ens_mean = jnp.concatenate([j[0] for j in joined], axis=0).astype(F32)
    ens_var = jnp.concatenate([j[1] for j in joined], axis=0).astype(F32)
    return (new_state, ens_mean, ens_var)


GROUP = 8


def slot_table(lon_count, wave_count, share, lane_y, lanes):
    offset = jnp.arange(lanes, dtype=jnp.int32)[:, None, None, None]
    p = jnp.arange(2, dtype=jnp.int32)[None, :, None, None]
    part = jnp.arange(2, dtype=jnp.int32)[None, None, :, None]
    unit = (lane_y - offset) % lanes * share + jnp.arange(share, dtype=jnp.int32)[None, None, None, :]
    wave = jnp.where(p == 0, unit, wave_count - unit)
    wave = jnp.where(unit == 0, jnp.where(part == 0, 0, wave_count // 2), wave)
    wave, unit, p, part = jnp.broadcast_arrays(wave, unit, p, part)
    quarter = jnp.where(unit == 0, p, part) * lon_count
    lon_ids = jnp.arange(lon_count, dtype=jnp.int32)
    turn = (4 * (wave.reshape(-1, 1) * lon_ids[None, :]) + quarter.reshape(-1, 1)) % (4 * lon_count)
    phase = turn.astype(F32) * (0.5 * math.pi / lon_count)
    return (jnp.cos(phase) * math.sqrt(2.0 / lon_count)).astype(BF16)


WAIT = pl.BlockSpec(memory_space=pl.ANY)
MESH = pl.DeviceIdType.MESH


def pipeline_body(lanes, far, cuts, grid_ref, noise_ref, table_t_ref, turned_ref, diffusion_ref, input_ref, extra_ref,
                  bias_ref, middle_ref, last_ref, state_ref, table_out, first_out, held_out, *rest):
    fields = rest[:lanes]
    (kept, sent, own, other, back, blocks_ref, basis, flipped, table_ref, first_ref, damping, rows_in, noise_in,
     rows_out, held_in, mine, give, taken, held) = rest[lanes:lanes + 19]
    rest = rest[lanes + 19:]
    scratch = rest[:2 * lanes]
    (row_sem, noise_sem, out_sem, field_sem, table_sem, held_sem, give_sem, basis_send, basis_recv, kept_send, kept_recv, own_send, own_recv, back_send,
     back_recv) = rest[2 * lanes:]
    members, lat_rows, lon_count, channels = grid_ref.shape
    blocks, share, depth = kept.shape[1:4]
    slots, per, totals, _ = own.shape
    ahead = slots // 2
    wave_count = turned_ref.shape[0]
    pieces = per // 2
    groups = lat_rows // GROUP
    rows = 2 * GROUP
    pitch = scratch[0].shape[0] // share
    chunks = members * cuts
    index, team = lax.axis_index("lat"), lax.axis_index("grp")
    place, lane = index // lanes, index % lanes
    half = place // far
    dist = (1 - half) * (far - 1 - place) + half * (place - far)
    hub_place = far - 1 + half
    opposite = (far - half) * lanes + lane
    core = team % 2
    partner = team + 1 - 2 * core
    hub, leaf = dist == 0, dist > 0
    start = lane * share
    ranges = [pl.ds(q * per, per) for q in range(cuts)]

    def remote(src, dst, send, recv, **target):
        return pltpu.make_async_remote_copy(
            src_ref=src, dst_ref=dst, send_sem=send, recv_sem=recv, device_id=target, device_id_type=MESH
        )

    def hub_lane(dy):
        return hub_place * lanes + (lane + lanes - dy) % lanes

    def source_lane(k):
        return (hub_place + (2 * half - 1) * (k // lanes)) * lanes + (lane + k % lanes) % lanes

    def span(q):
        return (0, pieces + 1) if q == 0 else (pieces * q + 1, pieces)

    def spot(q, j):
        return j // pieces, pieces * q + (q + cuts - 1) // cuts + j % pieces

    def basis_copy(q, dy):
        low, size = span(q)
        at = pl.multiple_of((dist * lanes + dy) * depth, depth)
        return remote(
            blocks_ref.at[dy, pl.ds(low, size)], basis.at[core, pl.ds(low, size), pl.ds(at, depth)],
            basis_send.at[q, dy], basis_recv.at[q, dist * lanes + dy], lat=hub_lane(dy),
        )

    def basis_own(q):
        low, size = span(q)
        return pltpu.make_async_copy(
            blocks_ref.at[0, pl.ds(low, size)], basis.at[core, pl.ds(low, size), pl.ds(0, depth)],
            basis_recv.at[q, 0],
        )

    def send_basis(q):
        for dy in range(1, lanes):
            basis_copy(q, dy).start()

        @pl.when(leaf)
        def _():
            basis_copy(q, 0).start()

        @pl.when(hub)
        def _():
            basis_own(q).start()

    def arrange(q):
        row = lax.broadcasted_iota(jnp.int32, (lat_rows, totals), 1)
        flip = lax.broadcasted_iota(jnp.int32, (totals, totals), 0)
        flip = flip + lax.broadcasted_iota(jnp.int32, (totals, totals), 1) == totals - 1
        flip = flip.astype(F32).astype(BF16)
        low, size = span(q)
        for dy in range(lanes):
            turn = (lane + lanes - dy) % lanes
            for e in range(size):
                unit = turn * share + q * per + core * pieces + e
                if e == pieces:
                    unit = turn * share + wave_count // 2 * (1 - (turn + lanes - 1) // lanes)
                near = turned_ref[unit].astype(F32)
                mirrored = jnp.dot(
                    turned_ref[(wave_count - unit) % wave_count], flip, preferred_element_type=F32
                )
                near = jnp.where(row >= unit, near, 0.0).reshape(groups, 1, GROUP, totals)
                mirrored = jnp.where(row < unit, mirrored, 0.0).reshape(groups, 1, GROUP, totals)
                both = jnp.concatenate([near, mirrored], axis=1).reshape(depth, totals)
                blocks_ref[dy, low + e] = both.astype(BF16)

    def basis_swap(q, low, size):
        part = basis.at[core, pl.ds(low, size)]
        return remote(part, part, basis_send.at[q, lanes], basis_recv.at[q, blocks], grp=partner)

    def basis_ready(q, low, size):
        pltpu.make_async_copy(
            blocks_ref.at[0, pl.ds(low, size)], basis.at[core, pl.ds(low, size), pl.ds(0, depth)],
            basis_recv.at[q, 0],
        ).wait()
        for k in range(1, blocks):
            part = basis.at[core, pl.ds(low, size), pl.ds(k * depth, depth)]
            remote(part, part, basis_send.at[q, 0], basis_recv.at[q, k], lat=opposite).wait_recv()
        basis_swap(q, low, size).start()
        basis_swap(q, low, size).wait_recv()
        for side in range(2):
            for e in range(size):
                flipped[side, low + e] = basis[side, low + e].T

    def lane_copy(b, q, dy):
        return remote(
            sent.at[b, dy - 1, ranges[q]], kept.at[b, dy, ranges[q]], kept_send.at[b, q, dy - 1],
            kept_recv.at[b, q, dy], lat=place * lanes + (lane + lanes - dy) % lanes,
        )

    def kept_copy(b, q, dy):
        k = dist * lanes + dy
        return remote(
            kept.at[b, dy, ranges[q]], kept.at[b, k, ranges[q]], kept_send.at[b, q, lanes - 1 + dy],
            kept_recv.at[b, q, k], lat=hub_lane(0),
        )

    def kept_arrival(b, q, k):
        part = kept.at[b, k, pl.ds(q * per, per)]
        return remote(part, part, kept_send.at[b, q, 0], kept_recv.at[b, q, k], lat=opposite)

    def own_copy(c):
        return remote(own.at[c % slots], other.at[c], own_send.at[c], own_recv.at[c], lat=opposite)

    def back_copy(b, q, k):
        units = pl.ds(q * per, per)
        return remote(
            kept.at[b, k, units], back.at[b, k % lanes, units], back_send.at[b, q, k - 1],
            back_recv.at[b, q, k % lanes], lat=source_lane(k),
        )

    def back_arrival(b, q, dy):
        part = back.at[b, dy, pl.ds(q * per, per)]
        return remote(part, part, back_send.at[b, q, 0], back_recv.at[b, q, dy], lat=opposite)

    def load(ref, n):
        at = pl.multiple_of(n % groups * GROUP, GROUP)
        held, sem = (rows_in, row_sem) if ref is grid_ref else (noise_in, noise_sem)
        return pltpu.make_async_copy(ref.at[n // groups, pl.ds(at, GROUP)], held.at[n % 2], sem.at[n % 2])

    def store(n):
        at = pl.multiple_of(n % groups * GROUP, GROUP)
        return pltpu.make_async_copy(
            rows_out.at[n % 2], state_ref.at[n // groups, pl.ds(at, GROUP)], out_sem.at[n % 2]
        )

    def greet(**target):
        pl.semaphore_signal(barrier, inc=1, device_id=target, device_id_type=MESH)

    barrier = pltpu.get_barrier_semaphore()
    for step in range(1, lanes):
        greet(lat=place * lanes + (lane + step) % lanes)
    greet(grp=partner)

    @pl.when(leaf)
    def _():
        for step in range(lanes):
            greet(lat=hub_place * lanes + step)

    @pl.when(hub)
    def _():
        greet(lat=opposite)
        for k in range(lanes, blocks):
            greet(lat=source_lane(k))

    def all_here():
        @pl.when(leaf)
        def _():
            pl.semaphore_wait(barrier, 2 * lanes)

        @pl.when(hub)
        def _():
            pl.semaphore_wait(barrier, 1 + blocks)

    def analyse_group(n, carry):
        b = n // groups
        at = pl.multiple_of(n % groups * rows, rows)

        @pl.when(n + 1 < members * groups)
        def _():
            load(grid_ref, n + 1).start()

        load(grid_ref, n).wait()
        for k in range(0, GROUP, 2):
            pair = jnp.concatenate([rows_in[n % 2, k], rows_in[n % 2, k + 1]], axis=1)
            waves = jnp.dot(table_t_ref[...], pair, preferred_element_type=F32)
            row = 0
            for dy in range(lanes):
                for p in range(2):
                    for part in range(2):
                        for t in range(2):
                            scratch[2 * dy + part][pl.ds(p * GROUP + k + t, share, stride=pitch), :] = (
                                waves[row:row + share, t * channels:(t + 1) * channels]
                            )
                        row += share
        for dy in range(lanes):
            for part in range(2):
                value = scratch[2 * dy + part][...].reshape(share, pitch, channels)[:, :rows].astype(BF16)
                side = slice(part * channels, (part + 1) * channels)
                if dy == 0:
                    kept[b, 0, :, pl.ds(at, rows), side] = value
                else:
                    sent[b, dy - 1, :, pl.ds(at, rows), side] = value
        return carry

    def partial(c):
        b, q = c // cuts, c % cuts

        @pl.when(c == 0)
        def _():
            basis_ready(0, 0, pieces + 1)

        @pl.when((c > 0) & (c < cuts))
        def _():
            basis_ready(c, pieces * c + 1, pieces)

        for k in range(1, blocks):
            kept_arrival(b, q, k).wait_recv()

        @pl.when(c >= slots)
        def _():
            own_copy(c - slots).wait_send()

        def unit(j, carry):
            values = jnp.concatenate([kept[b, k, q * per + j] for k in range(blocks)], axis=0)
            side, e = spot(q, j)
            sums = jnp.dot(flipped[side, e], values, preferred_element_type=F32)
            own[c % slots, j] = sums.astype(BF16)
            return carry

        for j in range(per):
            unit(j, 0)

        @pl.when(q == 0)
        def _():
            values = jnp.concatenate([kept[b, k, 0, :, channels:] for k in range(blocks)], axis=0)
            sums = jnp.dot(flipped[0, pieces], values, preferred_element_type=F32)
            own[c % slots, 0, :, channels:] = sums.astype(BF16)

        own_copy(c).start()

    def synthesise(c):
        b, q = c // cuts, c % cuts
        own_copy(c).wait_recv()
        row = lax.broadcasted_iota(jnp.int32, (totals, channels), 0)

        def damped(j, mark, side):
            total = own[c % slots, j, :, side].astype(F32) + other[c, j, :, side].astype(F32)
            return (total * jnp.where(row < mark, damping[1], damping[0])).astype(BF16)

        def put(i, grid, side):
            back[b, 0, i, :, side] = grid[:depth]
            for k in range(1, blocks):
                kept[b, k, i, :, side] = grid[k * depth:(k + 1) * depth]

        def unit(j, carry):
            mark = start + q * per + j
            value = jnp.concatenate(
                [damped(j, mark, slice(r * channels, (r + 1) * channels)) for r in range(2)], axis=1
            )
            at, e = spot(q, j)
            grid = jnp.dot(basis[at, e], value, preferred_element_type=F32).astype(BF16)
            put(q * per + j, grid, slice(None))
            return carry

        for j in range(per):
            unit(j, 0)

        @pl.when(q == 0)
        def _():
            mark = jnp.where(start == 0, totals // 2, start)
            side = slice(channels, 2 * channels)
            grid = jnp.dot(basis[0, pieces], damped(0, mark, side), preferred_element_type=F32).astype(BF16)
            put(0, grid, side)

        for k in range(1, blocks):
            back_copy(b, q, k).start()

    def spread_fields(b, at):
        for dy in range(lanes):
            for part in range(2):
                side = slice(part * channels, (part + 1) * channels)
                value = back[b, dy, :, pl.ds(at, rows), side].astype(F32)
                space = jnp.zeros((share, pitch - rows, channels), F32)
                scratch[2 * dy + part][...] = jnp.concatenate([value, space], axis=1).reshape(-1, channels)

    def column_pair(n, i):
        waves, states = [], []
        for t in range(2):
            waves.append(jnp.concatenate([
                scratch[2 * dy + part][pl.ds(p * GROUP + 2 * i + t, share, stride=pitch), :]
                for dy in range(lanes) for p in range(2) for part in range(2)
            ], axis=0).astype(BF16))
        smoothed = jnp.dot(table_ref[...], jnp.concatenate(waves, axis=1), preferred_element_type=F32)
        for t in range(2):
            flat = smoothed[:, t * channels:(t + 1) * channels]
            joined = jnp.concatenate([flat.astype(BF16), noise_in[n % 2, 2 * i + t]], axis=1)
            pre = jnp.dot(joined, first_ref[...], preferred_element_type=F32)
            one = silu(pre + bias_ref[...]).astype(BF16)
            two = silu(jnp.dot(one, middle_ref[...], preferred_element_type=F32)).astype(BF16)
            tendency = jnp.dot(two, last_ref[...], preferred_element_type=F32)
            state = (flat + tendency).astype(BF16)
            rows_out[n % 2, 2 * i + t] = state
            states.append(state)
        return states

    def column_group(b, g):
        n = b * groups + g
        at = pl.multiple_of(g * rows, rows)

        @pl.when(n <= (members - 1) * groups - 1)
        def _():
            load(noise_ref, n + 1).start()

        @pl.when(g == 0)
        def _():
            for q in range(cuts):
                for dy in range(lanes):
                    if dy > 0:
                        back_arrival(b, q, dy).wait_recv()
                    else:
                        @pl.when(leaf)
                        def _():
                            back_arrival(b, q, dy).wait_recv()

        spread_fields(b, at)
        load(noise_ref, n).wait()

        @pl.when(n >= 2)
        def _():
            store(n - 2).wait()

        def pair(i, carry):
            column_pair(n, i)
            return carry

        lax.fori_loop(0, GROUP // 2, pair, 0)
        store(n).start()

    def analyse_member(b, first):
        lax.fori_loop(b * groups, (b + 1) * groups, analyse_group, 0)
        if first:
            all_here()
            send_basis(0)
        for q in range(cuts):
            for dy in range(1, lanes):
                lane_copy(b, q, dy).start()
            if first and q == 0:
                for later in range(1, cuts):
                    arrange(later)
            if first and q + 1 < cuts:
                @pl.when(hub)
                def _():
                    send_basis(q + 1)

        @pl.when(leaf)
        def _():
            kept_copy(b, 0, 0).start()
            for q in range(cuts):
                for dy in range(1, lanes):
                    kept_arrival(b, q, dy).wait_recv()
                    kept_copy(b, q, dy).start()
                if q + 1 < cuts:
                    if first:
                        send_basis(q + 1)
                    kept_copy(b, q + 1, 0).start()

    load(grid_ref, 0).start()
    load(noise_ref, 0).start()
    arrange(0)
    analyse_member(0, True)
    first_ref[:channels] = input_ref[...]
    first_ref[channels:] = extra_ref[...]
    table_ref[...] = table_t_ref[...].T
    degree = lax.broadcasted_iota(jnp.int32, (totals, channels), 0)
    for side in range(2):
        n = (degree if side == 0 else totals - 1 - degree).astype(F32)
        ratio = n * (n + 1.0) / float((totals - 1) * totals)
        damping[side] = 1.0 / (1.0 + diffusion_ref[...] * (ratio * ratio))
    table_copy = pltpu.make_async_copy(table_ref, table_out, table_sem)
    table_copy.start()
    first_copy = pltpu.make_async_copy(first_ref, first_out, held_sem.at[members])
    first_copy.start()

    def tick(t, carry):
        @pl.when(hub)
        def _():
            @pl.when(t < chunks)
            def _():
                partial(t)

            @pl.when(t >= ahead)
            def _():
                synthesise(t - ahead)

        soon = t // cuts + 1

        @pl.when((t % cuts == 1) & (soon < members))
        def _():
            analyse_member(soon, False)

        late = t - cuts - ahead - 1
        g = (late + 2 * cuts) % cuts

        @pl.when((late >= 0) & (g < groups))
        def _():
            column_group(late // cuts, g)

        return carry

    lax.fori_loop(0, chunks + ahead, tick, 0)

    last = members - 1
    final_group = last * groups
    for n in (final_group - 2, final_group - 1):
        store(n).wait()
    held_copies = [
        pltpu.make_async_copy(state_ref.at[b, pl.ds(0, GROUP)], held_in.at[b], held_sem.at[b]) for b in range(last)
    ]
    for copy in held_copies:
        copy.start()
    for q in range(cuts):
        for dy in range(lanes):
            if dy > 0:
                back_arrival(last, q, dy).wait_recv()
            else:
                @pl.when(leaf)
                def _():
                    back_arrival(last, q, dy).wait_recv()
    finals = [
        pltpu.make_async_copy(back.at[last, dy], fields[dy].at[0], field_sem.at[dy]) for dy in range(lanes)
    ]
    for dy in range(1, lanes):
        finals[dy].start()
    finals[0].start()
    spread_fields(last, 0)
    load(noise_ref, final_group).wait()
    for copy in held_copies:
        copy.wait()

    def moments_pair(i, carry):
        states = column_pair(final_group, i)
        for t in range(2):
            k = 2 * i + t
            values = [held_in[b, k].astype(F32) for b in range(last)] + [states[t].astype(F32)]
            total = functools.reduce(jnp.add, values)
            mean = total * (1.0 / members)
            spread = functools.reduce(jnp.add, [jnp.square(v - mean) for v in values])
            half_lon = lon_count // 2
            for h in range(2):
                @pl.when(core == h)
                def _():
                    for j, value in enumerate((total, spread)):
                        mine[j, k] = value[h * half_lon:(h + 1) * half_lon].astype(BF16)
                        give[j, k] = value[(1 - h) * half_lon:(2 - h) * half_lon].astype(BF16)
        return carry

    lax.fori_loop(0, GROUP // 2, moments_pair, 0)
    store(final_group).start()
    exchange = remote(give, taken, give_sem.at[0], give_sem.at[1], grp=partner)
    exchange.start()
    exchange.wait_recv()
    for k in range(GROUP):
        pair_sums = join(
            [mine[0, k], mine[1, k]], [taken[0, k], taken[1, k]], members
        )
        for j in range(2):
            held[j, k] = pair_sums[j].astype(BF16)
    held_copy = pltpu.make_async_copy(held, held_out, held_sem.at[members + 1])
    held_copy.start()

    def drain(b, carry):
        for q in range(cuts):
            for dy in range(1, lanes):
                lane_copy(b, q, dy).wait_send()

            @pl.when(leaf)
            def _():
                for dy in range(lanes):
                    kept_copy(b, q, dy).wait_send()

            @pl.when(hub)
            def _():
                for k in range(1, blocks):
                    back_copy(b, q, k).wait_send()
        return carry

    lax.fori_loop(0, members, drain, 0)

    @pl.when(hub)
    def _():
        for q in range(cuts):
            basis_swap(q, *span(q)).wait_send()
        for c in range(chunks - slots, chunks):
            own_copy(c).wait_send()

    @pl.when(leaf)
    def _():
        for q in range(cuts):
            basis_copy(q, 0).wait_send()

    for q in range(cuts):
        for dy in range(1, lanes):
            basis_copy(q, dy).wait_send()
    table_copy.wait()
    first_copy.wait()
    for final in finals:
        final.wait()
    exchange.wait_send()
    store(final_group).wait()
    held_copy.wait()


def pipeline(lanes, far, cuts, grid_state, noise, table_t, turned, diffusion, one, two, bias, middle, output):
    members, lat_rows, lon_count, channels = grid_state.shape
    wave_count = turned.shape[0]
    share = wave_count // 2 // lanes
    entries = share // 2 + 1
    depth = 2 * lat_rows
    count = far * lanes
    per = share // cuts
    slots = 6
    sums = (2, GROUP, lon_count // 2, channels)
    vmem = pl.BlockSpec(memory_space=pltpu.VMEM)
    dma = pltpu.SemaphoreType.DMA
    return pl.pallas_call(
        functools.partial(pipeline_body, lanes, far, cuts),
        in_specs=[WAIT, WAIT, vmem, vmem, vmem, vmem, vmem, vmem, vmem, vmem],
        out_specs=[WAIT] * (4 + lanes),
        out_shape=[
            jax.ShapeDtypeStruct(grid_state.shape, BF16),
            jax.ShapeDtypeStruct((lon_count, table_t.shape[0]), BF16),
            jax.ShapeDtypeStruct((2 * channels, middle.shape[0]), BF16),
            jax.ShapeDtypeStruct(sums, BF16),
        ] + [jax.ShapeDtypeStruct((1, share, depth, 2 * channels), BF16)] * lanes,
        scratch_shapes=[
            pltpu.VMEM((members, count, share, depth, 2 * channels), BF16),
            pltpu.VMEM((members, lanes - 1, share, depth, 2 * channels), BF16),
            pltpu.VMEM((slots, per, wave_count, 2 * channels), BF16),
            pltpu.VMEM((members * cuts, per, wave_count, 2 * channels), BF16),
            pltpu.VMEM((members, lanes, share, depth, 2 * channels), BF16),
            pltpu.VMEM((lanes, entries, depth, wave_count), BF16),
            pltpu.VMEM((2, entries, count * depth, wave_count), BF16),
            pltpu.VMEM((2, entries, wave_count, count * depth), BF16),
            pltpu.VMEM((lon_count, table_t.shape[0]), BF16),
            pltpu.VMEM((2 * channels, middle.shape[0]), BF16),
            pltpu.VMEM((2, wave_count, channels), F32),
        ] + [pltpu.VMEM((2, GROUP, lon_count, channels), BF16)] * 3 + [
            pltpu.VMEM((members - 1, GROUP, lon_count, channels), BF16)
        ] + [pltpu.VMEM(sums, BF16)] * 4 + [pltpu.VMEM((share * 3 * GROUP, channels), F32)] * (2 * lanes) + [
            dma((2,)),
            dma((2,)),
            dma((2,)),
            dma((lanes,)),
            dma,
            dma((members + 2,)),
            dma((2,)),
            dma((cuts, lanes + 1)),
            dma((cuts, count + 1)),
            dma((members, cuts, 2 * lanes - 1)),
            dma((members, cuts, count)),
            dma((members * cuts,)),
            dma((members * cuts,)),
            dma((members, cuts, count - 1)),
            dma((members, cuts, lanes)),
        ],
        compiler_params=pltpu.CompilerParams(
            has_side_effects=True, vmem_limit_bytes=64000 * 1024, collective_id=0
        ),
    )(grid_state, noise, table_t, turned, diffusion, one, two, bias, middle, output)


def last_body(lanes, *refs):
    core_ref, fields = refs[0], refs[1:1 + lanes]
    noise_ref, table_ref, first_ref, bias_ref, middle_ref, last_ref, held_ref = refs[1 + lanes:8 + lanes]
    state_ref, mine_ref, give_ref = refs[-2 * lanes - 3:-2 * lanes]
    scratch = refs[-2 * lanes:]
    members, lats, lon_count, channels = state_ref.shape
    _, share, rows, _ = fields[0].shape
    pitch = scratch[0].shape[0] // share
    inner = pl.program_id(0)

    @pl.when(inner == 0)
    def _():
        for dy in range(lanes):
            for part in range(2):
                value = fields[dy][0, :, :, part * channels:(part + 1) * channels].astype(F32)
                space = jnp.zeros((share, pitch - rows, channels), F32)
                scratch[2 * dy + part][...] = jnp.concatenate([value, space], axis=1).reshape(-1, channels)

    waves = []
    for k in range(lats):
        at = inner * lats + k
        waves.append(jnp.concatenate([
            scratch[2 * dy + part][pl.ds(p * rows // 2 + at, share, stride=pitch), :]
            for dy in range(lanes) for p in range(2) for part in range(2)
        ], axis=0).astype(BF16))
    smoothed = jnp.dot(table_ref[...], jnp.concatenate(waves, axis=1), preferred_element_type=F32)
    half = lon_count // 2
    for k in range(lats):
        flat = smoothed[:, k * channels:(k + 1) * channels]
        joined = jnp.concatenate([flat.astype(BF16), noise_ref[0, k]], axis=1)
        pre = jnp.dot(joined, first_ref[...], preferred_element_type=F32)
        one = silu(pre + bias_ref[...]).astype(BF16)
        two = silu(jnp.dot(one, middle_ref[...], preferred_element_type=F32)).astype(BF16)
        tendency = jnp.dot(two, last_ref[...], preferred_element_type=F32)
        state = (flat + tendency).astype(BF16)
        for b in range(members - 1):
            state_ref[b, k] = held_ref[b, k]
        state_ref[members - 1, k] = state
        values = [held_ref[b, k].astype(F32) for b in range(members - 1)] + [state.astype(F32)]
        total = functools.reduce(jnp.add, values)
        mean = total * (1.0 / members)
        spread = functools.reduce(jnp.add, [jnp.square(v - mean) for v in values])
        sums = [total.astype(BF16), spread.astype(BF16)]
        for h in range(2):
            @pl.when(core_ref[0] == h)
            def _():
                for j in range(2):
                    mine_ref[j, k] = sums[j][h * half:(h + 1) * half]
                    give_ref[j, k] = sums[j][(1 - h) * half:(2 - h) * half]


def last_columns(fields, core, noise, table, first, bias, middle, output, states, part, previous, after):
    lanes = len(fields)
    members, _, lon_count, channels = noise.shape
    _, share, _, width = fields[0].shape
    rows = 2 * GROUP
    lats = 2
    inner = GROUP // lats
    half = lon_count // 2
    whole = lambda a: pl.BlockSpec(a.shape, lambda i: (0,) * a.ndim)
    params = [table, first, bias, middle, output]
    operands = [core, *fields, noise, *params, states]
    specs = [pl.BlockSpec(memory_space=pltpu.SMEM)]
    specs += [pl.BlockSpec((1, share, rows, width), lambda i: (0, 0, part, 0))] * lanes
    specs.append(pl.BlockSpec(
        (1, lats, lon_count, channels), lambda i: (members - 1, part * inner + i, 0, 0)
    ))
    specs += [whole(a) for a in params]
    specs.append(pl.BlockSpec(
        (members - 1, lats, lon_count, channels), lambda i: (0, part * inner + i, 0, 0)
    ))
    aliases = {}
    if previous is not None:
        aliases = {len(operands): 0}
        operands.append(previous)
    operands += after
    specs += [WAIT] * (len(operands) - len(specs))
    points = GROUP * lon_count
    hidden = middle.shape[0]
    return pl.pallas_call(
        functools.partial(last_body, lanes),
        grid=(inner,),
        in_specs=specs,
        out_specs=[
            pl.BlockSpec((members, lats, lon_count, channels), lambda i: (0, part * inner + i, 0, 0))
        ] + [pl.BlockSpec((2, lats, half, channels), lambda i: (0, i, 0, 0))] * 2,
        out_shape=[
            jax.ShapeDtypeStruct(noise.shape, BF16)
        ] + [jax.ShapeDtypeStruct((2, GROUP, half, channels), BF16)] * 2,
        input_output_aliases=aliases,
        scratch_shapes=[pltpu.VMEM((share * 3 * GROUP, channels), F32)] * (2 * lanes),
        cost_estimate=pl.CostEstimate(
            flops=2 * points * (first.size + middle.size + output.size + 256 * channels),
            bytes_accessed=16 * points * channels,
            transcendentals=2 * points * hidden,
        ),
    )(*operands)


def carry_body(state_ref, _, out_ref):
    out_ref[...] = state_ref[...]


def carry_states(states, new_state):
    members, _, lon_count, channels = states.shape
    block = pl.BlockSpec((members, GROUP // 2, lon_count, channels), lambda i: (0, i, 0, 0))
    return pl.pallas_call(
        carry_body,
        grid=(2,),
        in_specs=[block, WAIT],
        out_specs=block,
        out_shape=jax.ShapeDtypeStruct(new_state.shape, new_state.dtype),
        input_output_aliases={1: 0},
        cost_estimate=pl.CostEstimate(
            flops=members * GROUP * lon_count * channels,
            bytes_accessed=4 * members * GROUP * lon_count * channels,
            transcendentals=0,
        ),
    )(states, new_state)


def blend_body(count, scales, one_ref, two_ref, out_ref):
    total, spread = join(one_ref[...], two_ref[...], count)
    out_ref[0] = (total * scales[0]).astype(BF16)
    out_ref[1] = (spread * scales[1]).astype(BF16)


def blend(one, two, count, scales):
    _, group, half, channels = one.shape
    block = pl.BlockSpec((2, 4, half, channels), lambda i: (0, i, 0, 0))
    return pl.pallas_call(
        functools.partial(blend_body, count, scales),
        grid=(group // 4,),
        in_specs=[block, block],
        out_specs=block,
        out_shape=jax.ShapeDtypeStruct(one.shape, BF16),
        cost_estimate=pl.CostEstimate(
            flops=4 * one.size, bytes_accessed=6 * one.size, transcendentals=0
        ),
    )(one, two)


def place_body(core_ref, mine_ref, partner_ref, *refs):
    outs = refs[-2:]
    half = mine_ref.shape[2]
    for h in range(2):
        @pl.when(core_ref[0] == h)
        def _():
            for j in range(2):
                outs[j][:, h * half:(h + 1) * half] = mine_ref[j].astype(F32)
                outs[j][:, (1 - h) * half:(2 - h) * half] = partner_ref[j].astype(F32)


def place_moments(core, mine, partner, part, lat_rows, previous):
    _, group, half, channels = mine.shape
    shape = (lat_rows, 2 * half, channels)
    block = pl.BlockSpec((2, 4, half, channels), lambda i: (0, i, 0, 0))
    return pl.pallas_call(
        place_body,
        grid=(group // 4,),
        in_specs=[pl.BlockSpec(memory_space=pltpu.SMEM), block, block] + [WAIT] * len(previous),
        out_specs=[
            pl.BlockSpec((4, 2 * half, channels), lambda i: (part * (group // 4) + i, 0, 0))
        ] * 2,
        out_shape=[jax.ShapeDtypeStruct(shape, F32)] * 2,
        input_output_aliases={3 + j: j for j in range(len(previous))},
        cost_estimate=pl.CostEstimate(
            flops=4 * mine.size, bytes_accessed=16 * mine.size, transcendentals=0
        ),
    )(core, mine, partner, *previous)


def hub_plan(
    lanes,
    grid_state,
    noise_field,
    legendre,
    diffusion,
    input_weight,
    noise_weight,
    input_bias,
    middle_weight,
    output_weight,
):
    members, lat_rows, lon_count, _ = grid_state.shape
    wave_count = legendre.shape[1]
    far = lax.axis_size("lat") // lanes // 2
    share = wave_count // 2 // lanes
    parts = lat_rows // GROUP
    cuts = 8
    lane = lax.axis_index("lat") % lanes
    core = lax.axis_index("grp") % 2
    table_t = slot_table(lon_count, wave_count, share, lane, lanes)
    turned = legendre.transpose(1, 0, 2)
    states, table, first, held, *fields = pipeline(
        lanes, far, cuts, grid_state, noise_field, table_t, turned, diffusion[None], input_weight, noise_weight,
        input_bias[None], middle_weight, output_weight,
    )
    params = (first, input_bias[None], middle_weight, output_weight)
    groups = lax.axis_size("grp")
    flag = core[None].astype(jnp.int32)
    new_state, after, placed = None, [], []
    for q in range(parts):
        if q > 0:
            new_state, mine, give = last_columns(fields, flag, noise_field, table, *params, states, q, new_state, after)
            held = blend(mine, swap(give, 1), members, (1.0, 1.0))
            after = [held]
        bit, count = 2, 2 * members
        while bit < groups:
            other = swap(held, bit)
            final = 2 * bit >= groups
            scales = (0.5 / count, 1.0 / (2 * count - 1)) if final else (1.0, 1.0)
            held = blend(held, other, count, scales)
            bit, count = 2 * bit, 2 * count
        partner = swap(held, 1)
        placed = place_moments(flag, held, partner, q, lat_rows, placed)
    new_state = carry_states(states, new_state)
    return (new_state, *placed)


def lane_count(mesh):
    line = [getattr(d, "coords", None) for d in mesh.devices.reshape(-1, mesh.shape["lat"])[0]]
    if len(line) < 2 or line[0] is None:
        return 2
    axis = [a != b for a, b in zip(line[0], line[1])].index(True)
    return len({c[axis] for c in line})


def per_device(lanes, *args):
    grid_state, legendre = args[0], args[2]
    members, lat_rows = grid_state.shape[:2]
    units = legendre.shape[1] // 2
    fits = (
        lax.axis_size("lat") % (2 * lanes) == 0
        and units % (16 * lanes) == 0
        and lat_rows % GROUP == 0
        and 2 < lat_rows // GROUP < 7
        and members > 1
        and lax.axis_size("grp") > 2
    )
    return hub_plan(lanes, *args) if fits else direct_plan(*args)


def solution(mesh):
    in_specs = (
        P("grp", "lat", None, None),
        P("grp", "lat", None, None),
        P("lat", None, None),
        P(),
        P(),
        P(),
        P(),
        P(),
        P(),
    )
    out_specs = (P("grp", "lat", None, None), P("lat", None, None), P("lat", None, None))

    def body(*args):
        return per_device(lane_count(mesh), *args)

    return jax.shard_map(
        body, mesh=mesh, in_specs=in_specs, out_specs=out_specs, check_vma=False
    )
```

```python
import functools
import math

import jax
import jax.numpy as jnp
from jax import lax
from jax.experimental import pallas as pl
from jax.experimental.pallas import tpu as pltpu
from jax.sharding import PartitionSpec as P


BF16 = jnp.bfloat16
F32 = jnp.float32


def wave_table(lon_count, wave_count):
    lon_ids = jnp.arange(lon_count, dtype=jnp.int32)[:, None]
    wave_ids = jnp.arange(wave_count, dtype=jnp.int32)[None, :]
    phase = (lon_ids * wave_ids % lon_count).astype(jnp.float32) * (2.0 * math.pi / lon_count)
    factor = math.sqrt(2.0 / lon_count)
    joined = jnp.concatenate([jnp.cos(phase), -jnp.sin(phase)], axis=1) * factor
    return joined.astype(jnp.bfloat16)


def damping_filter(diffusion, wave_count):
    degree = jnp.arange(wave_count, dtype=jnp.int32).astype(jnp.float32)
    ratio = degree * (degree + 1.0) / float((wave_count - 1) * wave_count)
    return 1.0 / (1.0 + diffusion[None, :] * (ratio * ratio)[:, None])


def analysis_body(table_ref, grid_ref, out_ref):
    bands, _, rows, width, channels = out_ref.shape
    for row in range(0, rows, 2):
        pair = jnp.concatenate([grid_ref[0, row], grid_ref[0, row + 1]], axis=1)
        waves = jnp.dot(table_ref[...], pair, preferred_element_type=F32).astype(BF16)
        for k in range(2):
            out_ref[:, 0, row + k] = waves[:, k * channels:(k + 1) * channels].reshape(
                bands, width, channels
            )


def analyse(grid_state, table, first, count, bands):
    _, lat_rows, lon_count, channels = grid_state.shape
    width = table.shape[0] // bands
    rows = 6
    return pl.pallas_call(
        analysis_body,
        grid=(count, lat_rows // rows),
        in_specs=[
            pl.BlockSpec(table.shape, lambda b, i: (0, 0)),
            pl.BlockSpec((1, rows, lon_count, channels), lambda b, i: (b + first, i, 0, 0)),
        ],
        out_specs=pl.BlockSpec((bands, 1, rows, width, channels), lambda b, i: (0, b, i, 0, 0)),
        out_shape=jax.ShapeDtypeStruct((bands, count, lat_rows, width, channels), BF16),
        cost_estimate=pl.CostEstimate(
            flops=2 * count * lat_rows * lon_count * channels * table.shape[0],
            bytes_accessed=4 * count * lat_rows * lon_count * channels,
            transcendentals=0,
        ),
    )(table, grid_state)


def spectral_body(parts, in_ref, basis_ref, flipped_ref, damping_ref, *rest):
    outs, (fin, fout) = rest[:parts], rest[parts:]
    bands, _, lat_rows, width, channels = in_ref.shape
    waves = basis_ref.shape[0]
    lats = bands * lat_rows
    span = lat_rows * width
    for s in range(bands):
        fin[pl.ds(s * span, span), :] = in_ref[s, 0].astype(F32).reshape(span, channels)
    damping = jnp.concatenate([damping_ref[...]] * 2, axis=1)
    for m in range(waves):
        values = jnp.concatenate(
            [fin[pl.ds(r * waves + m, lats, stride=width), :] for r in range(2)], axis=1
        ).astype(BF16)
        spectrum = jnp.dot(flipped_ref[m], values, preferred_element_type=F32)
        filtered = (spectrum * damping).astype(BF16)
        grid = jnp.dot(basis_ref[m], filtered, preferred_element_type=F32)
        for r in range(2):
            fout[pl.ds(r * waves + m, lats, stride=width), :] = grid[
                :, r * channels:(r + 1) * channels
            ]
    part_rows = lat_rows // parts
    for q in range(parts):
        for s in range(bands):
            start = (s * lat_rows + q * part_rows) * width
            outs[q][s, 0] = (
                fout[pl.ds(start, part_rows * width), :]
                .reshape(part_rows, width, channels)
                .astype(BF16)
            )


def spectral(received, basis, flipped, damping, parts):
    bands, count, lat_rows, width, channels = received.shape
    part_rows = lat_rows // parts
    whole = lambda a: pl.BlockSpec(a.shape, lambda b: (0,) * a.ndim)
    return pl.pallas_call(
        functools.partial(spectral_body, parts),
        grid=(count,),
        in_specs=[
            pl.BlockSpec((bands, 1, lat_rows, width, channels), lambda b: (0, b, 0, 0, 0)),
            whole(basis),
            whole(flipped),
            whole(damping),
        ],
        out_specs=[
            pl.BlockSpec((bands, 1, part_rows, width, channels), lambda b: (0, b, 0, 0, 0))
        ] * parts,
        out_shape=[
            jax.ShapeDtypeStruct((bands, count, part_rows, width, channels), BF16)
        ] * parts,
        scratch_shapes=[pltpu.VMEM((bands * lat_rows * width, channels), F32)] * 2,
        cost_estimate=pl.CostEstimate(
            flops=8 * count * basis.size * channels,
            bytes_accessed=4 * received.size,
            transcendentals=0,
        ),
    )(received, basis, flipped, damping)


def silu(value):
    half = 0.5 * value
    return half + half * jnp.tanh(half)


def physics_body(groups, *refs):
    fields = refs[:groups]
    noise_ref, table_ref, first_ref, bias_ref, middle_ref, last_ref = refs[groups:groups + 6]
    state_ref, stats_ref = refs[-2:]
    members, _, lon_count, channels = noise_ref.shape
    states = []
    for ref in fields:
        count = ref.shape[1]
        waves = jnp.concatenate(
            [ref[:, k, 0].reshape(-1, channels) for k in range(count)], axis=1
        )
        smoothed = jnp.dot(table_ref[...], waves, preferred_element_type=F32)
        for k in range(count):
            flat = smoothed[:, k * channels:(k + 1) * channels]
            b = len(states)
            joined = jnp.concatenate([flat.astype(BF16), noise_ref[b, 0]], axis=1)
            pre = jnp.dot(joined, first_ref[...], preferred_element_type=F32)
            one = silu(pre + bias_ref[...]).astype(BF16)
            two = silu(jnp.dot(one, middle_ref[...], preferred_element_type=F32)).astype(BF16)
            tendency = jnp.dot(two, last_ref[...], preferred_element_type=F32)
            state = (flat + tendency).astype(BF16)
            state_ref[b, 0] = state
            states.append(state)
    values = [s.astype(F32) for s in states]
    total = functools.reduce(jnp.add, values)
    mean = total * (1.0 / members)
    spread = functools.reduce(jnp.add, [jnp.square(v - mean) for v in values])
    half = lon_count // 2
    for h in range(2):
        stats_ref[h, 0, 0] = total[h * half:(h + 1) * half].astype(BF16)
        stats_ref[h, 1, 0] = spread[h * half:(h + 1) * half].astype(BF16)


def physics(fields, noise, table, first, bias, middle, last, part, previous):
    bands, _, part_rows, width, channels = fields[0].shape
    members, lat_rows, lon_count, noise_channels = noise.shape
    whole = lambda a: pl.BlockSpec(a.shape, lambda i: (0,) * a.ndim)
    at = part * part_rows
    specs = [
        pl.BlockSpec((bands, f.shape[1], 1, width, channels), lambda i: (0, 0, i, 0, 0))
        for f in fields
    ]
    specs.append(
        pl.BlockSpec((members, 1, lon_count, noise_channels), lambda i: (0, i + at, 0, 0))
    )
    params = [table, first, bias, middle, last]
    specs += [whole(a) for a in params]
    operands = [*fields, noise, *params]
    aliases = {}
    if previous is not None:
        aliases = {len(operands): 0}
        operands.append(previous)
        specs.append(pl.BlockSpec(memory_space=pl.ANY))
    columns = members * part_rows * lon_count
    hidden = middle.shape[0]
    return pl.pallas_call(
        functools.partial(physics_body, len(fields)),
        grid=(part_rows,),
        in_specs=specs,
        out_specs=[
            pl.BlockSpec((members, 1, lon_count, channels), lambda i: (0, i + at, 0, 0)),
            pl.BlockSpec((2, 2, 1, lon_count // 2, channels), lambda i: (0, 0, i, 0, 0)),
        ],
        out_shape=[
            jax.ShapeDtypeStruct((members, lat_rows, lon_count, channels), BF16),
            jax.ShapeDtypeStruct((2, 2, part_rows, lon_count // 2, channels), BF16),
        ],
        input_output_aliases=aliases,
        cost_estimate=pl.CostEstimate(
            flops=2 * columns * (first.size + middle.size + last.size + 256 * channels),
            bytes_accessed=8 * columns * channels,
            transcendentals=2 * columns * hidden,
        ),
    )(*operands)


def swap(value, bit):
    groups = lax.axis_size("grp")
    return lax.ppermute(value, "grp", [(g, g ^ bit) for g in range(groups)])


def join(a, b, count):
    a, b = [v.astype(F32) for v in a], [v.astype(F32) for v in b]
    total = a[0] + b[0]
    spread = (a[1] + b[1]) + jnp.square(a[0] - b[0]) * (0.5 / count)
    return total, spread


def pair_moments(stats, members):
    core = lax.axis_index("grp") % 2
    own = lax.dynamic_index_in_dim(stats, core, 0, keepdims=False)
    other = lax.dynamic_index_in_dim(stats, 1 - core, 0, keepdims=False)
    return jnp.stack(join(own, swap(other, 1), members)).astype(BF16)


def ensemble_moments(held, members):
    groups = lax.axis_size("grp")
    core = lax.axis_index("grp") % 2
    bit, count = 2, 2 * members
    while bit < groups:
        held = jnp.stack(join(held.astype(BF16), swap(held.astype(BF16), bit), count))
        bit, count = 2 * bit, 2 * count
    scale = jnp.array([1.0 / count, 1.0 / (count - 1)], F32)
    held = (held * scale[:, None, None, None]).astype(BF16)
    partner = swap(held, 1)
    low = jnp.where(core == 0, held, partner)
    high = jnp.where(core == 0, partner, held)
    return low, high


def direct_plan(
    grid_state,
    noise_field,
    legendre,
    diffusion,
    input_weight,
    noise_weight,
    input_bias,
    middle_weight,
    output_weight,
):
    members, lat_rows, lon_count, _ = grid_state.shape
    wave_count = legendre.shape[1]
    bands = lax.axis_size("lat")
    local_waves = wave_count // bands
    chunk = 2
    parts = 2
    transform = wave_table(lon_count, wave_count)
    table = (
        transform.reshape(lon_count, 2, bands, local_waves)
        .transpose(0, 2, 1, 3)
        .reshape(lon_count, 2 * wave_count)
    )
    table_t = table.T
    exchange = lambda v: lax.all_to_all(v, "lat", split_axis=0, concat_axis=0, tiled=True)
    damping = damping_filter(diffusion, wave_count)

    sent = [
        analyse(grid_state, table_t, b, chunk, bands) for b in range(0, members, chunk)
    ]
    groups = lax.axis_size("grp")
    turned = legendre.transpose(1, 0, 2).reshape(bands, local_waves * lat_rows, wave_count)
    share = local_waves * lat_rows // groups
    own = lax.dynamic_slice_in_dim(turned, lax.axis_index("grp") * share, share, axis=1)
    basis = lax.all_gather(exchange(own), "grp", axis=1, tiled=True)
    basis = basis.reshape(bands, local_waves, lat_rows, wave_count).transpose(1, 0, 2, 3)
    basis = basis.reshape(local_waves, bands * lat_rows, wave_count)
    zonal_ids = lax.axis_index("lat") * local_waves + jnp.arange(local_waves, dtype=jnp.int32)
    total_ids = jnp.arange(wave_count, dtype=jnp.int32)
    triangle = total_ids[None, :] >= zonal_ids[:, None]
    basis = jnp.where(triangle[:, None], basis, jnp.zeros_like(basis))
    flipped = basis.transpose(0, 2, 1)
    received = [exchange(s) for s in sent]
    banded = [spectral(r, basis, flipped, damping, parts) for r in received]

    first = jnp.concatenate([input_weight, noise_weight], axis=0)
    new_state = None
    moments = []
    for q in range(parts):
        fields = [exchange(g[q]) for g in banded]
        if moments:
            fields, moments[-1] = lax.optimization_barrier((fields, moments[-1]))
        new_state, stats = physics(
            fields, noise_field, table, first, input_bias[None], middle_weight,
            output_weight, q, new_state,
        )
        moments.append(ensemble_moments(pair_moments(stats, members), members))
    joined = [jnp.concatenate([low, high], axis=2) for low, high in moments]
    ens_mean = jnp.concatenate([j[0] for j in joined], axis=0).astype(F32)
    ens_var = jnp.concatenate([j[1] for j in joined], axis=0).astype(F32)
    return (new_state, ens_mean, ens_var)


GROUP = 8


def slot_table(lon_count, wave_count, share, lane_y, lanes):
    offset = jnp.arange(lanes, dtype=jnp.int32)[:, None, None, None]
    p = jnp.arange(2, dtype=jnp.int32)[None, :, None, None]
    part = jnp.arange(2, dtype=jnp.int32)[None, None, :, None]
    unit = (lane_y - offset) % lanes * share + jnp.arange(share, dtype=jnp.int32)[None, None, None, :]
    wave = jnp.where(p == 0, unit, wave_count - unit)
    wave = jnp.where(unit == 0, jnp.where(part == 0, 0, wave_count // 2), wave)
    wave, unit, p, part = jnp.broadcast_arrays(wave, unit, p, part)
    quarter = jnp.where(unit == 0, p, part) * lon_count
    lon_ids = jnp.arange(lon_count, dtype=jnp.int32)
    turn = (4 * (wave.reshape(-1, 1) * lon_ids[None, :]) + quarter.reshape(-1, 1)) % (4 * lon_count)
    phase = turn.astype(F32) * (0.5 * math.pi / lon_count)
    return (jnp.cos(phase) * math.sqrt(2.0 / lon_count)).astype(BF16)


WAIT = pl.BlockSpec(memory_space=pl.ANY)
MESH = pl.DeviceIdType.MESH


def pipeline_body(lanes, far, cuts, grid_ref, noise_ref, table_t_ref, legendre_ref, diffusion_ref, input_ref, extra_ref,
                  bias_ref, middle_ref, last_ref, state_ref, table_out, first_out, held_out, *rest):
    fields = rest[:lanes]
    (kept, sent, own, other, back, blocks_ref, basis, flipped, table_ref, first_ref, damping, rows_in, noise_in,
     rows_out, held_in, mine, give, taken, held, turned) = rest[lanes:lanes + 20]
    rest = rest[lanes + 20:]
    scratch = rest[:2 * lanes]
    (row_sem, noise_sem, out_sem, field_sem, table_sem, held_sem, give_sem, basis_send, basis_recv, kept_send, kept_recv, own_send, own_recv, back_send,
     back_recv, piece_send, piece_recv) = rest[2 * lanes:]
    members, lat_rows, lon_count, channels = grid_ref.shape
    blocks, share, depth = kept.shape[1:4]
    slots, per, totals, _ = own.shape
    ahead = slots // 2
    wave_count = legendre_ref.shape[1]
    pieces = per // 2
    groups = lat_rows // GROUP
    rows = 2 * GROUP
    pitch = scratch[0].shape[0] // share
    chunks = members * cuts
    index, team = lax.axis_index("lat"), lax.axis_index("grp")
    place, lane = index // lanes, index % lanes
    half = place // far
    dist = (1 - half) * (far - 1 - place) + half * (place - far)
    hub_place = far - 1 + half
    opposite = (far - half) * lanes + lane
    core = team % 2
    partner = team + 1 - 2 * core
    hub, leaf = dist == 0, dist > 0
    start = lane * share
    ranges = [pl.ds(q * per, per) for q in range(cuts)]

    def remote(src, dst, send, recv, **target):
        return pltpu.make_async_remote_copy(
            src_ref=src, dst_ref=dst, send_sem=send, recv_sem=recv, device_id=target, device_id_type=MESH
        )

    def hub_lane(dy):
        return hub_place * lanes + (lane + lanes - dy) % lanes

    def source_lane(k):
        return (hub_place + (2 * half - 1) * (k // lanes)) * lanes + (lane + k % lanes) % lanes

    def span(q):
        return (0, pieces + 1) if q == 0 else (pieces * q + 1, pieces)

    def spot(q, j):
        return j // pieces, pieces * q + (q + cuts - 1) // cuts + j % pieces

    def basis_copy(q, dy):
        low, size = span(q)
        at = pl.multiple_of((dist * lanes + dy) * depth, depth)
        return remote(
            blocks_ref.at[dy, pl.ds(low, size)], basis.at[core, pl.ds(low, size), pl.ds(at, depth)],
            basis_send.at[q, dy], basis_recv.at[q, dist * lanes + dy], lat=hub_lane(dy),
        )

    def basis_own(q):
        low, size = span(q)
        return pltpu.make_async_copy(
            blocks_ref.at[0, pl.ds(low, size)], basis.at[core, pl.ds(low, size), pl.ds(0, depth)],
            basis_recv.at[q, 0],
        )

    def send_basis(q):
        for dy in range(1, lanes):
            basis_copy(q, dy).start()

        @pl.when(leaf)
        def _():
            basis_copy(q, 0).start()

        @pl.when(hub)
        def _():
            basis_own(q).start()

    def waves_of(wave):
        return turned[pl.ds(pl.multiple_of(wave * lat_rows, GROUP), lat_rows), :]

    def arrange(q):
        row = lax.broadcasted_iota(jnp.int32, (lat_rows, totals), 1)
        flip = lax.broadcasted_iota(jnp.int32, (totals, totals), 0)
        flip = flip + lax.broadcasted_iota(jnp.int32, (totals, totals), 1) == totals - 1
        flip = flip.astype(F32).astype(BF16)
        low, size = span(q)
        for dy in range(lanes):
            turn = (lane + lanes - dy) % lanes
            for e in range(size):
                unit = turn * share + q * per + core * pieces + e
                if e == pieces:
                    unit = turn * share + wave_count // 2 * (1 - (turn + lanes - 1) // lanes)
                near = waves_of(unit)
                mirrored = jnp.dot(
                    waves_of((wave_count - unit) % wave_count).astype(BF16), flip, preferred_element_type=F32
                )
                near = jnp.where(row >= unit, near, 0.0).reshape(groups, 1, GROUP, totals)
                mirrored = jnp.where(row < unit, mirrored, 0.0).reshape(groups, 1, GROUP, totals)
                both = jnp.concatenate([near, mirrored], axis=1).reshape(depth, totals)
                blocks_ref[dy, low + e] = both.astype(BF16)

    def basis_swap(q, low, size):
        part = basis.at[core, pl.ds(low, size)]
        return remote(part, part, basis_send.at[q, lanes], basis_recv.at[q, blocks], grp=partner)

    def basis_ready(q, low, size):
        pltpu.make_async_copy(
            blocks_ref.at[0, pl.ds(low, size)], basis.at[core, pl.ds(low, size), pl.ds(0, depth)],
            basis_recv.at[q, 0],
        ).wait()
        for k in range(1, blocks):
            part = basis.at[core, pl.ds(low, size), pl.ds(k * depth, depth)]
            remote(part, part, basis_send.at[q, 0], basis_recv.at[q, k], lat=opposite).wait_recv()
        basis_swap(q, low, size).start()
        basis_swap(q, low, size).wait_recv()
        for side in range(2):
            for e in range(size):
                flipped[side, low + e] = basis[side, low + e].T

    def lane_copy(b, q, dy):
        return remote(
            sent.at[b, dy - 1, ranges[q]], kept.at[b, dy, ranges[q]], kept_send.at[b, q, dy - 1],
            kept_recv.at[b, q, dy], lat=place * lanes + (lane + lanes - dy) % lanes,
        )

    def kept_copy(b, q, dy):
        k = dist * lanes + dy
        return remote(
            kept.at[b, dy, ranges[q]], kept.at[b, k, ranges[q]], kept_send.at[b, q, lanes - 1 + dy],
            kept_recv.at[b, q, k], lat=hub_lane(0),
        )

    def kept_arrival(b, q, k):
        part = kept.at[b, k, pl.ds(q * per, per)]
        return remote(part, part, kept_send.at[b, q, 0], kept_recv.at[b, q, k], lat=opposite)

    def own_copy(c):
        return remote(own.at[c % slots], other.at[c], own_send.at[c], own_recv.at[c], lat=opposite)

    def back_copy(b, q, k):
        units = pl.ds(q * per, per)
        return remote(
            kept.at[b, k, units], back.at[b, k % lanes, units], back_send.at[b, q, k - 1],
            back_recv.at[b, q, k % lanes], lat=source_lane(k),
        )

    def back_arrival(b, q, dy):
        part = back.at[b, dy, pl.ds(q * per, per)]
        return remote(part, part, back_send.at[b, q, 0], back_recv.at[b, q, dy], lat=opposite)

    def piece_copy(k, g):
        b, q = members - 1, cuts - 1
        units, lats = pl.ds(q * per, per), pl.ds(g * rows, rows)
        return remote(
            kept.at[b, k, units, lats], back.at[b, k % lanes, units, lats],
            back_send.at[b, q, k - 1] if g == 0 else piece_send.at[k - 1, g - 1],
            back_recv.at[b, q, k % lanes] if g == 0 else piece_recv.at[k % lanes, g - 1], lat=source_lane(k),
        )

    def piece_arrival(dy, g):
        b, q = members - 1, cuts - 1
        part = back.at[b, dy, pl.ds(q * per, per), pl.ds(g * rows, rows)]
        recv = back_recv.at[b, q, dy] if g == 0 else piece_recv.at[dy, g - 1]
        return remote(part, part, back_send.at[b, q, 0], recv, lat=opposite)

    def load(ref, n):
        at = pl.multiple_of(n % groups * GROUP, GROUP)
        held, sem = (rows_in, row_sem) if ref is grid_ref else (noise_in, noise_sem)
        return pltpu.make_async_copy(ref.at[n // groups, pl.ds(at, GROUP)], held.at[n % 2], sem.at[n % 2])

    def store(n):
        at = pl.multiple_of(n % groups * GROUP, GROUP)
        return pltpu.make_async_copy(
            rows_out.at[n % 2], state_ref.at[n // groups, pl.ds(at, GROUP)], out_sem.at[n % 2]
        )

    def greet(**target):
        pl.semaphore_signal(barrier, inc=1, device_id=target, device_id_type=MESH)

    barrier = pltpu.get_barrier_semaphore()
    for step in range(1, lanes):
        greet(lat=place * lanes + (lane + step) % lanes)
    greet(grp=partner)

    @pl.when(leaf)
    def _():
        for step in range(lanes):
            greet(lat=hub_place * lanes + step)

    @pl.when(hub)
    def _():
        greet(lat=opposite)
        for k in range(lanes, blocks):
            greet(lat=source_lane(k))

    def all_here():
        @pl.when(leaf)
        def _():
            pl.semaphore_wait(barrier, 2 * lanes)

        @pl.when(hub)
        def _():
            pl.semaphore_wait(barrier, 1 + blocks)

    def analyse_group(n, carry):
        b = n // groups
        at = pl.multiple_of(n % groups * rows, rows)

        @pl.when(n + 1 < members * groups)
        def _():
            load(grid_ref, n + 1).start()

        load(grid_ref, n).wait()
        for k in range(0, GROUP, 2):
            pair = jnp.concatenate([rows_in[n % 2, k], rows_in[n % 2, k + 1]], axis=1)
            waves = jnp.dot(table_t_ref[...], pair, preferred_element_type=F32)
            row = 0
            for dy in range(lanes):
                for p in range(2):
                    for part in range(2):
                        for t in range(2):
                            scratch[2 * dy + part][pl.ds(p * GROUP + k + t, share, stride=pitch), :] = (
                                waves[row:row + share, t * channels:(t + 1) * channels]
                            )
                        row += share
        for dy in range(lanes):
            for part in range(2):
                value = scratch[2 * dy + part][...].reshape(share, pitch, channels)[:, :rows].astype(BF16)
                side = slice(part * channels, (part + 1) * channels)
                if dy == 0:
                    kept[b, 0, :, pl.ds(at, rows), side] = value
                else:
                    sent[b, dy - 1, :, pl.ds(at, rows), side] = value
        return carry

    def partial(c):
        b, q = c // cuts, c % cuts

        @pl.when(c == 0)
        def _():
            basis_ready(0, 0, pieces + 1)

        @pl.when((c > 0) & (c < cuts))
        def _():
            basis_ready(c, pieces * c + 1, pieces)

        for k in range(1, blocks):
            kept_arrival(b, q, k).wait_recv()

        @pl.when(c >= slots)
        def _():
            own_copy(c - slots).wait_send()

        def unit(j, carry):
            values = jnp.concatenate([kept[b, k, q * per + j] for k in range(blocks)], axis=0)
            side, e = spot(q, j)
            sums = jnp.dot(flipped[side, e], values, preferred_element_type=F32)
            own[c % slots, j] = sums.astype(BF16)
            return carry

        for j in range(per):
            unit(j, 0)

        @pl.when(q == 0)
        def _():
            values = jnp.concatenate([kept[b, k, 0, :, channels:] for k in range(blocks)], axis=0)
            sums = jnp.dot(flipped[0, pieces], values, preferred_element_type=F32)
            own[c % slots, 0, :, channels:] = sums.astype(BF16)

        own_copy(c).start()

    def synthesise(c):
        b, q = c // cuts, c % cuts
        own_copy(c).wait_recv()
        row = lax.broadcasted_iota(jnp.int32, (totals, channels), 0)

        def damped(j, mark, side):
            total = own[c % slots, j, :, side].astype(F32) + other[c, j, :, side].astype(F32)
            return (total * jnp.where(row < mark, damping[1], damping[0])).astype(BF16)

        def put(i, grid, side):
            back[b, 0, i, :, side] = grid[:depth]
            for k in range(1, blocks):
                kept[b, k, i, :, side] = grid[k * depth:(k + 1) * depth]

        def unit(j, carry):
            mark = start + q * per + j
            value = jnp.concatenate(
                [damped(j, mark, slice(r * channels, (r + 1) * channels)) for r in range(2)], axis=1
            )
            at, e = spot(q, j)
            grid = jnp.dot(basis[at, e], value, preferred_element_type=F32).astype(BF16)
            put(q * per + j, grid, slice(None))
            return carry

        for j in range(per):
            unit(j, 0)

        @pl.when(q == 0)
        def _():
            mark = jnp.where(start == 0, totals // 2, start)
            side = slice(channels, 2 * channels)
            grid = jnp.dot(basis[0, pieces], damped(0, mark, side), preferred_element_type=F32).astype(BF16)
            put(0, grid, side)

        @pl.when(c < chunks - 1)
        def _():
            for k in range(1, blocks):
                back_copy(b, q, k).start()

        @pl.when(c == chunks - 1)
        def _():
            for g in range(groups):
                for k in range(1, blocks):
                    piece_copy(k, g).start()

    def spread_fields(b, at):
        for dy in range(lanes):
            for part in range(2):
                side = slice(part * channels, (part + 1) * channels)
                value = back[b, dy, :, pl.ds(at, rows), side].astype(F32)
                space = jnp.zeros((share, pitch - rows, channels), F32)
                scratch[2 * dy + part][...] = jnp.concatenate([value, space], axis=1).reshape(-1, channels)

    def column_pair(n, i):
        waves, states = [], []
        for t in range(2):
            waves.append(jnp.concatenate([
                scratch[2 * dy + part][pl.ds(p * GROUP + 2 * i + t, share, stride=pitch), :]
                for dy in range(lanes) for p in range(2) for part in range(2)
            ], axis=0).astype(BF16))
        smoothed = jnp.dot(table_ref[...], jnp.concatenate(waves, axis=1), preferred_element_type=F32)
        for t in range(2):
            flat = smoothed[:, t * channels:(t + 1) * channels]
            joined = jnp.concatenate([flat.astype(BF16), noise_in[n % 2, 2 * i + t]], axis=1)
            pre = jnp.dot(joined, first_ref[...], preferred_element_type=F32)
            one = silu(pre + bias_ref[...]).astype(BF16)
            two = silu(jnp.dot(one, middle_ref[...], preferred_element_type=F32)).astype(BF16)
            tendency = jnp.dot(two, last_ref[...], preferred_element_type=F32)
            state = (flat + tendency).astype(BF16)
            rows_out[n % 2, 2 * i + t] = state
            states.append(state)
        return states

    def column_group(b, g):
        n = b * groups + g
        at = pl.multiple_of(g * rows, rows)

        @pl.when(n <= (members - 1) * groups - 1)
        def _():
            load(noise_ref, n + 1).start()

        @pl.when(g == 0)
        def _():
            for q in range(cuts):
                for dy in range(lanes):
                    if dy > 0:
                        back_arrival(b, q, dy).wait_recv()
                    else:
                        @pl.when(leaf)
                        def _():
                            back_arrival(b, q, dy).wait_recv()

        spread_fields(b, at)
        load(noise_ref, n).wait()

        @pl.when(n >= 2)
        def _():
            store(n - 2).wait()

        def pair(i, carry):
            column_pair(n, i)
            return carry

        lax.fori_loop(0, GROUP // 2, pair, 0)
        store(n).start()

    def analyse_member(b, first):
        lax.fori_loop(b * groups, (b + 1) * groups, analyse_group, 0)
        if first:
            all_here()
            send_basis(0)
        for q in range(cuts):
            for dy in range(1, lanes):
                lane_copy(b, q, dy).start()
            if first and q == 0:
                for later in range(1, cuts):
                    arrange(later)
            if first and q + 1 < cuts:
                @pl.when(hub)
                def _():
                    send_basis(q + 1)

        @pl.when(leaf)
        def _():
            kept_copy(b, 0, 0).start()
            for q in range(cuts):
                for dy in range(1, lanes):
                    kept_arrival(b, q, dy).wait_recv()
                    kept_copy(b, q, dy).start()
                if q + 1 < cuts:
                    if first:
                        send_basis(q + 1)
                    kept_copy(b, q + 1, 0).start()

    load(grid_ref, 0).start()
    load(noise_ref, 0).start()
    for k in range(lat_rows):
        turned[pl.ds(k, wave_count, stride=lat_rows), :] = legendre_ref[k].astype(F32)
    arrange(0)
    analyse_member(0, True)
    first_ref[:channels] = input_ref[...]
    first_ref[channels:] = extra_ref[...]
    table_ref[...] = table_t_ref[...].T
    degree = lax.broadcasted_iota(jnp.int32, (totals, channels), 0)
    for side in range(2):
        n = (degree if side == 0 else totals - 1 - degree).astype(F32)
        ratio = n * (n + 1.0) / float((totals - 1) * totals)
        damping[side] = 1.0 / (1.0 + diffusion_ref[...] * (ratio * ratio))
    table_copy = pltpu.make_async_copy(table_ref, table_out, table_sem)
    table_copy.start()
    first_copy = pltpu.make_async_copy(first_ref, first_out, held_sem.at[members])
    first_copy.start()

    def tick(t, carry):
        @pl.when(hub)
        def _():
            @pl.when(t < chunks)
            def _():
                partial(t)

            @pl.when(t >= ahead)
            def _():
                synthesise(t - ahead)

        soon = t // cuts + 1

        @pl.when((t % cuts == 1) & (soon < members))
        def _():
            analyse_member(soon, False)

        late = t - cuts - ahead - 1
        g = (late + 2 * cuts) % cuts

        @pl.when((late >= 0) & (g < groups))
        def _():
            column_group(late // cuts, g)

        return carry

    lax.fori_loop(0, chunks + ahead, tick, 0)

    last = members - 1
    final_group = last * groups
    for n in (final_group - 2, final_group - 1):
        store(n).wait()
    held_copies = [
        pltpu.make_async_copy(state_ref.at[b, pl.ds(0, GROUP)], held_in.at[b], held_sem.at[b]) for b in range(last)
    ]
    for copy in held_copies:
        copy.start()

    def drain(b, carry):
        for q in range(cuts):
            for dy in range(1, lanes):
                lane_copy(b, q, dy).wait_send()

            @pl.when(leaf)
            def _():
                for dy in range(lanes):
                    kept_copy(b, q, dy).wait_send()

            @pl.when(hub & (b < last) if q == cuts - 1 else hub)
            def _():
                for k in range(1, blocks):
                    back_copy(b, q, k).wait_send()
        return carry

    lax.fori_loop(0, members, drain, 0)

    @pl.when(hub)
    def _():
        for q in range(cuts):
            basis_swap(q, *span(q)).wait_send()
        for c in range(chunks - slots, chunks):
            own_copy(c).wait_send()

    @pl.when(leaf)
    def _():
        for q in range(cuts):
            basis_copy(q, 0).wait_send()

    for q in range(cuts):
        for dy in range(1, lanes):
            basis_copy(q, dy).wait_send()

    def arrived(dy, g):
        if g == 0:
            for q in range(cuts - 1):
                back_arrival(last, q, dy).wait_recv()
        piece_arrival(dy, g).wait_recv()

    def all_arrived(g):
        for dy in range(1, lanes):
            arrived(dy, g)

        @pl.when(leaf)
        def _():
            arrived(0, g)

    all_arrived(0)
    finals = [
        pltpu.make_async_copy(back.at[last, dy], fields[dy].at[0], field_sem.at[dy]) for dy in range(lanes)
    ]
    spread_fields(last, 0)
    load(noise_ref, final_group).wait()
    for copy in held_copies:
        copy.wait()

    def moments_pair(i, carry):
        states = column_pair(final_group, i)
        for t in range(2):
            k = 2 * i + t
            values = [held_in[b, k].astype(F32) for b in range(last)] + [states[t].astype(F32)]
            total = functools.reduce(jnp.add, values)
            mean = total * (1.0 / members)
            spread = functools.reduce(jnp.add, [jnp.square(v - mean) for v in values])
            half_lon = lon_count // 2
            for h in range(2):
                @pl.when(core == h)
                def _():
                    for j, value in enumerate((total, spread)):
                        mine[j, k] = value[h * half_lon:(h + 1) * half_lon].astype(BF16)
                        give[j, k] = value[(1 - h) * half_lon:(2 - h) * half_lon].astype(BF16)
        return carry

    lax.fori_loop(0, GROUP // 2, moments_pair, 0)
    store(final_group).start()
    exchange = remote(give, taken, give_sem.at[0], give_sem.at[1], grp=partner)
    exchange.start()
    for g in range(1, groups):
        all_arrived(g)
    for final in finals:
        final.start()
    exchange.wait_recv()
    for k in range(GROUP):
        pair_sums = join(
            [mine[0, k], mine[1, k]], [taken[0, k], taken[1, k]], members
        )
        for j in range(2):
            held[j, k] = pair_sums[j].astype(BF16)
    held_copy = pltpu.make_async_copy(held, held_out, held_sem.at[members + 1])
    held_copy.start()

    @pl.when(hub)
    def _():
        for g in range(groups):
            for k in range(1, blocks):
                piece_copy(k, g).wait_send()

    table_copy.wait()
    first_copy.wait()
    for final in finals:
        final.wait()
    exchange.wait_send()
    store(final_group).wait()
    held_copy.wait()


def pipeline(lanes, far, cuts, grid_state, noise, table_t, legendre, diffusion, one, two, bias, middle, output):
    members, lat_rows, lon_count, channels = grid_state.shape
    wave_count = legendre.shape[1]
    share = wave_count // 2 // lanes
    entries = share // 2 + 1
    depth = 2 * lat_rows
    groups = lat_rows // GROUP
    count = far * lanes
    per = share // cuts
    slots = 6
    sums = (2, GROUP, lon_count // 2, channels)
    vmem = pl.BlockSpec(memory_space=pltpu.VMEM)
    dma = pltpu.SemaphoreType.DMA
    return pl.pallas_call(
        functools.partial(pipeline_body, lanes, far, cuts),
        in_specs=[WAIT, WAIT, vmem, vmem, vmem, vmem, vmem, vmem, vmem, vmem],
        out_specs=[WAIT] * (4 + lanes),
        out_shape=[
            jax.ShapeDtypeStruct(grid_state.shape, BF16),
            jax.ShapeDtypeStruct((lon_count, table_t.shape[0]), BF16),
            jax.ShapeDtypeStruct((2 * channels, middle.shape[0]), BF16),
            jax.ShapeDtypeStruct(sums, BF16),
        ] + [jax.ShapeDtypeStruct((1, share, depth, 2 * channels), BF16)] * lanes,
        scratch_shapes=[
            pltpu.VMEM((members, count, share, depth, 2 * channels), BF16),
            pltpu.VMEM((members, lanes - 1, share, depth, 2 * channels), BF16),
            pltpu.VMEM((slots, per, wave_count, 2 * channels), BF16),
            pltpu.VMEM((members * cuts, per, wave_count, 2 * channels), BF16),
            pltpu.VMEM((members, lanes, share, depth, 2 * channels), BF16),
            pltpu.VMEM((lanes, entries, depth, wave_count), BF16),
            pltpu.VMEM((2, entries, count * depth, wave_count), BF16),
            pltpu.VMEM((2, entries, wave_count, count * depth), BF16),
            pltpu.VMEM((lon_count, table_t.shape[0]), BF16),
            pltpu.VMEM((2 * channels, middle.shape[0]), BF16),
            pltpu.VMEM((2, wave_count, channels), F32),
        ] + [pltpu.VMEM((2, GROUP, lon_count, channels), BF16)] * 3 + [
            pltpu.VMEM((members - 1, GROUP, lon_count, channels), BF16)
        ] + [pltpu.VMEM(sums, BF16)] * 4 + [pltpu.VMEM((wave_count * lat_rows, wave_count), F32)] + [pltpu.VMEM((share * 3 * GROUP, channels), F32)] * (2 * lanes) + [
            dma((2,)),
            dma((2,)),
            dma((2,)),
            dma((lanes,)),
            dma,
            dma((members + 2,)),
            dma((2,)),
            dma((cuts, lanes + 1)),
            dma((cuts, count + 1)),
            dma((members, cuts, 2 * lanes - 1)),
            dma((members, cuts, count)),
            dma((members * cuts,)),
            dma((members * cuts,)),
            dma((members, cuts, count - 1)),
            dma((members, cuts, lanes)),
            dma((count - 1, groups - 1)),
            dma((lanes, groups - 1)),
        ],
        compiler_params=pltpu.CompilerParams(
            has_side_effects=True, vmem_limit_bytes=64000 * 1024, collective_id=0
        ),
    )(grid_state, noise, table_t, legendre, diffusion, one, two, bias, middle, output)


def last_body(lanes, *refs):
    core_ref, fields = refs[0], refs[1:1 + lanes]
    noise_ref, table_ref, first_ref, bias_ref, middle_ref, last_ref, held_ref = refs[1 + lanes:8 + lanes]
    state_ref, mine_ref, give_ref = refs[-2 * lanes - 3:-2 * lanes]
    scratch = refs[-2 * lanes:]
    members, lats, lon_count, channels = state_ref.shape
    _, share, rows, _ = fields[0].shape
    pitch = scratch[0].shape[0] // share
    inner = pl.program_id(0)

    @pl.when(inner == 0)
    def _():
        for dy in range(lanes):
            for part in range(2):
                value = fields[dy][0, :, :, part * channels:(part + 1) * channels].astype(F32)
                space = jnp.zeros((share, pitch - rows, channels), F32)
                scratch[2 * dy + part][...] = jnp.concatenate([value, space], axis=1).reshape(-1, channels)

    waves = []
    for k in range(lats):
        at = inner * lats + k
        waves.append(jnp.concatenate([
            scratch[2 * dy + part][pl.ds(p * rows // 2 + at, share, stride=pitch), :]
            for dy in range(lanes) for p in range(2) for part in range(2)
        ], axis=0).astype(BF16))
    smoothed = jnp.dot(table_ref[...], jnp.concatenate(waves, axis=1), preferred_element_type=F32)
    half = lon_count // 2
    for k in range(lats):
        flat = smoothed[:, k * channels:(k + 1) * channels]
        joined = jnp.concatenate([flat.astype(BF16), noise_ref[0, k]], axis=1)
        pre = jnp.dot(joined, first_ref[...], preferred_element_type=F32)
        one = silu(pre + bias_ref[...]).astype(BF16)
        two = silu(jnp.dot(one, middle_ref[...], preferred_element_type=F32)).astype(BF16)
        tendency = jnp.dot(two, last_ref[...], preferred_element_type=F32)
        state = (flat + tendency).astype(BF16)
        for b in range(members - 1):
            state_ref[b, k] = held_ref[b, k]
        state_ref[members - 1, k] = state
        values = [held_ref[b, k].astype(F32) for b in range(members - 1)] + [state.astype(F32)]
        total = functools.reduce(jnp.add, values)
        mean = total * (1.0 / members)
        spread = functools.reduce(jnp.add, [jnp.square(v - mean) for v in values])
        sums = [total.astype(BF16), spread.astype(BF16)]
        for h in range(2):
            @pl.when(core_ref[0] == h)
            def _():
                for j in range(2):
                    mine_ref[j, k] = sums[j][h * half:(h + 1) * half]
                    give_ref[j, k] = sums[j][(1 - h) * half:(2 - h) * half]


def last_columns(fields, core, noise, table, first, bias, middle, output, states, part, previous, after):
    lanes = len(fields)
    members, _, lon_count, channels = noise.shape
    _, share, _, width = fields[0].shape
    rows = 2 * GROUP
    lats = 2
    inner = GROUP // lats
    half = lon_count // 2
    whole = lambda a: pl.BlockSpec(a.shape, lambda i: (0,) * a.ndim)
    params = [table, first, bias, middle, output]
    operands = [core, *fields, noise, *params, states]
    specs = [pl.BlockSpec(memory_space=pltpu.SMEM)]
    specs += [pl.BlockSpec((1, share, rows, width), lambda i: (0, 0, part, 0))] * lanes
    specs.append(pl.BlockSpec(
        (1, lats, lon_count, channels), lambda i: (members - 1, part * inner + i, 0, 0)
    ))
    specs += [whole(a) for a in params]
    specs.append(pl.BlockSpec(
        (members - 1, lats, lon_count, channels), lambda i: (0, part * inner + i, 0, 0)
    ))
    aliases = {}
    if previous is not None:
        aliases = {len(operands): 0}
        operands.append(previous)
    operands += after
    specs += [WAIT] * (len(operands) - len(specs))
    points = GROUP * lon_count
    hidden = middle.shape[0]
    return pl.pallas_call(
        functools.partial(last_body, lanes),
        grid=(inner,),
        in_specs=specs,
        out_specs=[
            pl.BlockSpec((members, lats, lon_count, channels), lambda i: (0, part * inner + i, 0, 0))
        ] + [pl.BlockSpec((2, lats, half, channels), lambda i: (0, i, 0, 0))] * 2,
        out_shape=[
            jax.ShapeDtypeStruct(noise.shape, BF16)
        ] + [jax.ShapeDtypeStruct((2, GROUP, half, channels), BF16)] * 2,
        input_output_aliases=aliases,
        scratch_shapes=[pltpu.VMEM((share * 3 * GROUP, channels), F32)] * (2 * lanes),
        cost_estimate=pl.CostEstimate(
            flops=2 * points * (first.size + middle.size + output.size + 256 * channels),
            bytes_accessed=16 * points * channels,
            transcendentals=2 * points * hidden,
        ),
    )(*operands)


def carry_body(state_ref, _, out_ref):
    out_ref[...] = state_ref[...]


def carry_states(states, new_state):
    members, _, lon_count, channels = states.shape
    block = pl.BlockSpec((members, GROUP // 2, lon_count, channels), lambda i: (0, i, 0, 0))
    return pl.pallas_call(
        carry_body,
        grid=(2,),
        in_specs=[block, WAIT],
        out_specs=block,
        out_shape=jax.ShapeDtypeStruct(new_state.shape, new_state.dtype),
        input_output_aliases={1: 0},
        cost_estimate=pl.CostEstimate(
            flops=members * GROUP * lon_count * channels,
            bytes_accessed=4 * members * GROUP * lon_count * channels,
            transcendentals=0,
        ),
    )(states, new_state)


def blend_body(count, scales, one_ref, two_ref, out_ref):
    total, spread = join(one_ref[...], two_ref[...], count)
    out_ref[0] = (total * scales[0]).astype(BF16)
    out_ref[1] = (spread * scales[1]).astype(BF16)


def blend(one, two, count, scales):
    _, group, half, channels = one.shape
    block = pl.BlockSpec((2, 4, half, channels), lambda i: (0, i, 0, 0))
    return pl.pallas_call(
        functools.partial(blend_body, count, scales),
        grid=(group // 4,),
        in_specs=[block, block],
        out_specs=block,
        out_shape=jax.ShapeDtypeStruct(one.shape, BF16),
        compiler_params=pltpu.CompilerParams(vmem_limit_bytes=64000 * 1024),
        cost_estimate=pl.CostEstimate(
            flops=4 * one.size, bytes_accessed=6 * one.size, transcendentals=0
        ),
    )(one, two)


def place_body(count, core_ref, mine_ref, other_ref, beside_ref, crossed_ref, *refs):
    outs = refs[-2:]
    half = mine_ref.shape[2]
    scales = (0.5 / count, 1.0 / (2 * count - 1))
    own = join(mine_ref[...], other_ref[...], count)
    partner = join(beside_ref[...], crossed_ref[...], count)
    for h in range(2):
        @pl.when(core_ref[0] == h)
        def _():
            for j in range(2):
                outs[j][:, h * half:(h + 1) * half] = own[j] * scales[j]
                outs[j][:, (1 - h) * half:(2 - h) * half] = partner[j] * scales[j]


def place_moments(core, sums, count, part, lat_rows, previous):
    _, group, half, channels = sums[0].shape
    shape = (lat_rows, 2 * half, channels)
    block = pl.BlockSpec((2, 4, half, channels), lambda i: (0, i, 0, 0))
    return pl.pallas_call(
        functools.partial(place_body, count),
        grid=(group // 4,),
        in_specs=[pl.BlockSpec(memory_space=pltpu.SMEM)] + [block] * 4 + [WAIT] * len(previous),
        out_specs=[
            pl.BlockSpec((4, 2 * half, channels), lambda i: (part * (group // 4) + i, 0, 0))
        ] * 2,
        out_shape=[jax.ShapeDtypeStruct(shape, F32)] * 2,
        input_output_aliases={5 + j: j for j in range(len(previous))},
        compiler_params=pltpu.CompilerParams(vmem_limit_bytes=64000 * 1024),
        cost_estimate=pl.CostEstimate(
            flops=16 * sums[0].size, bytes_accessed=24 * sums[0].size, transcendentals=0
        ),
    )(core, *sums, *previous)


def hub_plan(
    lanes,
    grid_state,
    noise_field,
    legendre,
    diffusion,
    input_weight,
    noise_weight,
    input_bias,
    middle_weight,
    output_weight,
):
    members, lat_rows, lon_count, _ = grid_state.shape
    wave_count = legendre.shape[1]
    far = lax.axis_size("lat") // lanes // 2
    share = wave_count // 2 // lanes
    parts = lat_rows // GROUP
    cuts = 8
    lane = lax.axis_index("lat") % lanes
    core = lax.axis_index("grp") % 2
    table_t = slot_table(lon_count, wave_count, share, lane, lanes)
    states, table, first, held, *fields = pipeline(
        lanes, far, cuts, grid_state, noise_field, table_t, legendre, diffusion[None], input_weight, noise_weight,
        input_bias[None], middle_weight, output_weight,
    )
    params = (first, input_bias[None], middle_weight, output_weight)
    groups = lax.axis_size("grp")
    flag = core[None].astype(jnp.int32)
    new_state, after, placed = None, [], []
    for q in range(parts):
        if q > 0:
            new_state, mine, give = last_columns(fields, flag, noise_field, table, *params, states, q, new_state, after)
            given = swap(give, 1)
            held = blend(mine, given, members, (1.0, 1.0))
            after = [held]
        bit, count = 2, 2 * members
        while 2 * bit < groups:
            held = blend(held, swap(held, bit), count, (1.0, 1.0))
            bit, count = 2 * bit, 2 * count
        beside = swap(held, 1)
        other = swap(held, bit)
        crossed = swap(other, 1)
        placed = place_moments(flag, (held, other, beside, crossed), count, q, lat_rows, placed)
    new_state = carry_states(states, new_state)
    return (new_state, *placed)


def lane_count(mesh):
    line = [getattr(d, "coords", None) for d in mesh.devices.reshape(-1, mesh.shape["lat"])[0]]
    if len(line) < 2 or line[0] is None:
        return 2
    axis = [a != b for a, b in zip(line[0], line[1])].index(True)
    return len({c[axis] for c in line})


def per_device(lanes, *args):
    grid_state, legendre = args[0], args[2]
    members, lat_rows = grid_state.shape[:2]
    units = legendre.shape[1] // 2
    fits = (
        lax.axis_size("lat") % (2 * lanes) == 0
        and units % (16 * lanes) == 0
        and lat_rows % GROUP == 0
        and 2 < lat_rows // GROUP < 7
        and members > 1
        and lax.axis_size("grp") > 2
    )
    return hub_plan(lanes, *args) if fits else direct_plan(*args)


def solution(mesh):
    in_specs = (
        P("grp", "lat", None, None),
        P("grp", "lat", None, None),
        P("lat", None, None),
        P(),
        P(),
        P(),
        P(),
        P(),
        P(),
    )
    out_specs = (P("grp", "lat", None, None), P("lat", None, None), P("lat", None, None))

    def body(*args):
        return per_device(lane_count(mesh), *args)

    return jax.shard_map(
        body, mesh=mesh, in_specs=in_specs, out_specs=out_specs, check_vma=False
    )
```
